256 devices in a mesh: gx: 16 (over z_hi, x), gy: 4 (over y), gz: 4 (over z_lo, core).
Axes of the slice: x: 4, y: 4, z: 8 (z_hi: 4, z_lo: 2; z = z_hi * 2 + z_lo), core: 2. Of those that a mesh axis runs over, the one named last changes fastest.
Arguments:
- ambient_motion_array: float32 [3, 128, 256, 512], P(None, 'gx', 'gy', 'gz'), may hold values from -6 to 6
- ambient_scalar_trio: float32 [3, 128, 256, 512], P(None, 'gx', 'gy', 'gz'), may hold values from 0.2 to 1
- droplet_local_position: float32 [3, 262144], P(None, ('gx', 'gy', 'gz')), may hold values from -0.5 to 0.5
- droplet_motion_array: float32 [3, 262144], P(None, ('gx', 'gy', 'gz')), may hold values from -6 to 6
- droplet_heat_level: float32 [262144], P(('gx', 'gy', 'gz')), may hold values from 0.3 to 0.9
- droplet_size_quadratic: float32 [262144], P(('gx', 'gy', 'gz')), may hold values from 0.25 to 4
- local_i_position: int32 [262144], P(('gx', 'gy', 'gz')), may hold values from 0 to 7
- local_j_position: int32 [262144], P(('gx', 'gy', 'gz')), may hold values from 0 to 63
- local_k_position: int32 [262144], P(('gx', 'gy', 'gz')), may hold values from 0 to 127
- active_group_tally: int32 [256], P(('gx', 'gy', 'gz')), may hold values from 1 to 8, as said below
Outputs:
- gas_source: float32 [5, 128, 256, 512], P(None, 'gx', 'gy', 'gz')
- parcel_state: float32 [5, 262144], P(None, ('gx', 'gy', 'gz'))
The draws below stay inside these ranges and needn't reach their ends.
Inputs may be any that keep to these rules, and one draw needn't show every extreme that they name: `active_group_tally`: tiles of a brick are live from the first one on; in every draw some brick has all 8 tiles live.
All inputs are finite; a program needn't handle non-finite values.
Results may differ from the reference program's by a relative error of at most 0.0003.
Values sent between devices are 32-bit elements; how exact they have to be, the bound alone decides.
A program may use at most 128 MiB of HBM per device.

```python
import math
import jax
import jax.numpy as jnp
from jax import lax

CX = 8
CY = 64
CZ = 128
TILE = 128
TILE_CAP = 8
PAR_DEV = 1024
BRICKS = 256
GRID_EXTENT_I = 128
GRID_EXTENT_J = 256
GRID_EXTENT_K = 512
SPRAY_CAPACITY_N = 262144
N_GY = 4
N_GZ = 4


def draw_active_group_tally(key, part):
    key_base, key_core, key_pick = jax.random.split(key, 3)
    lowest = max(1, TILE_CAP // 4)
    highest = max(lowest + 1, TILE_CAP // 2 + 1)
    base_tiles = jax.random.randint(key_base, (BRICKS,), lowest, highest)
    dense_brick = jax.random.randint(key_core, (BRICKS,), 0, 8) == 0
    chosen = jax.random.randint(key_pick, (), 0, BRICKS)
    dense_brick = dense_brick | (jnp.arange(BRICKS) == chosen)
    return jnp.where(dense_brick, TILE_CAP, base_tiles).astype(jnp.int32)


def plant(array, stream_key, low, top_value):
    dims = array.shape
    spot = [jax.random.randint(jax.random.fold_in(stream_key, axis), (), 0, dims[axis]) for axis in range(len(dims))]
    array = array.at[tuple(spot)].set(low)
    longest = dims.index(max(dims))
    spot[longest] = (spot[longest] + 1) % dims[longest]
    return array.at[tuple(spot)].set(top_value)


def block_scale(stream_key, shape, cuts, smallest, top_value):
    gain = 1.0
    for position, parts in cuts:
        heights = jax.random.uniform(jax.random.fold_in(jax.random.fold_in(stream_key, 6), position), (parts,), jnp.float32, smallest / len(cuts), top_value / len(cuts))
        gain = gain * jnp.repeat(jnp.exp(heights), shape[position] // parts).reshape((-1,) + (1,) * (len(shape) - 1 - position))
    return gain


def normal_values(stream_key, dims, deviation, limit, pieces=(), held_as=jnp.bfloat16):
    entries = jax.random.normal(stream_key, dims, jnp.float32) * deviation
    if len(pieces) > 0:
        entries = block_scale(stream_key, dims, pieces, -0.22, 0.18) * entries
    return jnp.clip(entries, min=-limit, max=limit).astype(held_as)


def setup_inputs(seed: int = 0) -> dict:
    key_of = jax.random.split(jax.random.key(seed), 11)
    ambient_motion_array = normal_values(key_of[0], (3, GRID_EXTENT_I, GRID_EXTENT_J, GRID_EXTENT_K), 1.0, 6.0, ((1, 16), (2, 4), (3, 4)), jnp.float32)
    ambient_scalar_trio = jnp.clip(0.2 + 0.8 * jax.random.uniform(key_of[1], (3, GRID_EXTENT_I, GRID_EXTENT_J, GRID_EXTENT_K), jnp.float32) ** block_scale(key_of[1], (3, GRID_EXTENT_I, GRID_EXTENT_J, GRID_EXTENT_K), ((1, 16), (2, 4), (3, 4)), -0.2, 0.2), 0.2, 1.0)
    droplet_local_position = jnp.clip(jax.random.uniform(key_of[2], (3, SPRAY_CAPACITY_N), jnp.float32, -0.5, 0.5) * block_scale(key_of[2], (3, SPRAY_CAPACITY_N), ((1, 256),), -0.4, 0.0), -0.5, 0.5)
    droplet_motion_array = normal_values(key_of[3], (3, SPRAY_CAPACITY_N), 1.0, 6.0, ((1, 256),), jnp.float32)
    droplet_heat_level = jnp.clip(0.3 + 0.59999996 * jax.random.uniform(key_of[4], (SPRAY_CAPACITY_N,), jnp.float32) ** block_scale(key_of[4], (SPRAY_CAPACITY_N,), ((0, 256),), -0.2, 0.2), 0.3, 0.9)
    droplet_size_quadratic = jnp.clip(jnp.exp(math.log(4.0) - 2.7725887 * jax.random.uniform(key_of[5], (SPRAY_CAPACITY_N,), jnp.float32) ** block_scale(key_of[5], (SPRAY_CAPACITY_N,), ((0, 256),), -0.2, 0.2)), 0.25, 4.0)
    local_i_position = plant(jax.random.randint(key_of[6], (SPRAY_CAPACITY_N,), 0, CX), jax.random.fold_in(key_of[6], 1), 0, CX - 1).astype(jnp.int32)
    local_j_position = plant(jax.random.randint(key_of[7], (SPRAY_CAPACITY_N,), 0, CY), jax.random.fold_in(key_of[7], 1), 0, CY - 1).astype(jnp.int32)
    local_k_position = plant(jax.random.randint(key_of[8], (SPRAY_CAPACITY_N,), 0, CZ), jax.random.fold_in(key_of[8], 1), 0, CZ - 1).astype(jnp.int32)
    active_group_tally = draw_active_group_tally(jax.random.fold_in(key_of[10], 71), 0)
    return {"ambient_motion_array": ambient_motion_array, "ambient_scalar_trio": ambient_scalar_trio, "droplet_local_position": droplet_local_position, "droplet_motion_array": droplet_motion_array, "droplet_heat_level": droplet_heat_level, "droplet_size_quadratic": droplet_size_quadratic, "local_i_position": local_i_position, "local_j_position": local_j_position, "local_k_position": local_k_position, "active_group_tally": active_group_tally}


step_time = 0.25
evap_rate = 1.0
heat_rate = 2.0
boiling_energy_drain = 0.3

def tent_weights(offset_values):
    shifts = jnp.arange(3, dtype=jnp.float32) - 1.0
    return jnp.maximum(0.0, 1.0 - jnp.abs(offset_values[:, None, :] - shifts[None, :, None]))

def integrate_droplets(sampled_ambient_quantities, sampled_motion, sampled_heat_level, diam_quadratic_entry):
    ambient_motion = sampled_ambient_quantities[0:3]
    ambient_heat_level = sampled_ambient_quantities[3]
    ambient_moisture = sampled_ambient_quantities[4]
    ambient_rho_level = sampled_ambient_quantities[5]
    drag_ratio = step_time / (0.5 * diam_quadratic_entry)
    revised_speed = (sampled_motion + drag_ratio * ambient_motion) / (1.0 + drag_ratio)
    blob_weight_kilos = diam_quadratic_entry * jnp.sqrt(diam_quadratic_entry)
    vapour_equilibrium_share = jnp.exp(4.0 * (sampled_heat_level - 1.0))
    decay_multiplier = step_time * evap_rate * ambient_rho_level * (vapour_equilibrium_share - ambient_moisture)
    next_width_power = diam_quadratic_entry - decay_multiplier
    revised_weight = next_width_power * jnp.sqrt(next_width_power)
    conduction_intensity = step_time * heat_rate * ambient_rho_level / diam_quadratic_entry
    fresh_heat_level = (sampled_heat_level + conduction_intensity * ambient_heat_level) / (1.0 + conduction_intensity) - boiling_energy_drain * decay_multiplier / diam_quadratic_entry
    momentum_energy_deposits = jnp.concatenate([blob_weight_kilos[None] * (sampled_motion - revised_speed), (blob_weight_kilos * (sampled_heat_level - fresh_heat_level))[None], (blob_weight_kilos - revised_weight)[None]], axis=0)
    fresh_droplet_entry = jnp.concatenate([revised_speed, fresh_heat_level[None], next_width_power[None]], axis=0)
    return (fresh_droplet_entry, momentum_energy_deposits)

def reference(ambient_motion_array, ambient_scalar_trio, droplet_local_position, droplet_motion_array, droplet_heat_level, droplet_size_quadratic, local_i_position, local_j_position, local_k_position, active_group_tally):
    maximum_droplets_held = droplet_heat_level.shape[0]
    slot_id = jnp.arange(maximum_droplets_held, dtype=jnp.int32)
    brick_id = slot_id // PAR_DEV
    live_slot = slot_id % PAR_DEV // TILE < active_group_tally[brick_id]
    glob_x = brick_id // (N_GY * N_GZ) * CX + local_i_position
    glob_y = brick_id // N_GZ % N_GY * CY + local_j_position
    glob_z = brick_id % N_GZ * CZ + local_k_position
    quantity_bundle = jnp.concatenate([ambient_motion_array, ambient_scalar_trio], axis=0).reshape(6, -1)
    tent_table = tent_weights(droplet_local_position)
    vertex_weightings = jnp.arange(27, dtype=jnp.int32)
    cell_total = GRID_EXTENT_I * GRID_EXTENT_J * GRID_EXTENT_K

    def locate(stencil):
        pos_x = glob_x + stencil // 9 - 1
        pos_y = glob_y + stencil // 3 % 3 - 1
        pos_z = glob_z + stencil % 3 - 1
        inside = (pos_x >= 0) & (pos_x < GRID_EXTENT_I) & (pos_y >= 0) & (pos_y < GRID_EXTENT_J) & (pos_z >= 0) & (pos_z < GRID_EXTENT_K)
        flat_idx = (jnp.clip(pos_x, 0, GRID_EXTENT_I - 1) * GRID_EXTENT_J + jnp.clip(pos_y, 0, GRID_EXTENT_J - 1)) * GRID_EXTENT_K + jnp.clip(pos_z, 0, GRID_EXTENT_K - 1)
        weight = tent_table[0, stencil // 9] * tent_table[1, stencil // 3 % 3] * tent_table[2, stencil % 3]
        weight = jnp.where(inside, weight, 0.0)
        return (flat_idx.astype(jnp.int32), weight, inside)

    def sample_routine(running, stencil):
        flat_idx, weight, inside = locate(stencil)
        return (running + weight[None] * quantity_bundle[:, flat_idx], None)
    sampled_ambient_quantities = lax.scan(sample_routine, jnp.zeros((6, maximum_droplets_held), jnp.float32), vertex_weightings)[0]
    fresh_droplet_entry, momentum_energy_deposits = integrate_droplets(sampled_ambient_quantities, droplet_motion_array, droplet_heat_level, droplet_size_quadratic)
    momentum_energy_deposits = jnp.where(live_slot[None], momentum_energy_deposits, 0.0)

    def deposit_step(running, stencil):
        flat_idx, weight, inside = locate(stencil)
        target = jnp.where(inside, flat_idx, cell_total).astype(jnp.int32)
        return (running.at[:, target].add(weight[None] * momentum_energy_deposits, mode='drop'), None)
    deposit = lax.scan(deposit_step, jnp.zeros((5, cell_total), jnp.float32), vertex_weightings)[0]
    forwarded_carry = jnp.concatenate([droplet_motion_array, droplet_heat_level[None], droplet_size_quadratic[None]], axis=0)
    parcel_state = jnp.where(live_slot[None], fresh_droplet_entry, forwarded_carry)
    return (deposit.reshape(5, GRID_EXTENT_I, GRID_EXTENT_J, GRID_EXTENT_K), parcel_state)
```

```python
import functools

import jax
import jax.numpy as jnp
from jax import lax
from jax.experimental import pallas as pl
from jax.experimental.pallas import tpu as pltpu
from jax.sharding import PartitionSpec as P

TILE = 128
NF = 6
NS = 5
CI, CJ, CK = 8, 64, 128
OWN = CI * CJ
XB = OWN
YB = OWN + 128
COLS = OWN + 256
ROWS = NF * CK + 16
MESH = pl.DeviceIdType.MESH
F32 = jnp.float32
BF16 = jnp.bfloat16

step_time = 0.25
evap_rate = 1.0
heat_rate = 2.0
boiling_energy_drain = 0.3


def split(x):
    hi = x.astype(BF16)
    return hi, (x - hi.astype(F32)).astype(BF16)


def tent(offset):
    return jnp.maximum(0.0, 1.0 - jnp.abs(offset))


def iota(shape, dim):
    return lax.broadcasted_iota(jnp.int32, shape, dim)


def kernel(
    sizes,
    vel,
    scal,
    pos,
    mot,
    heat,
    diam,
    li,
    lj,
    lk,
    tally,
    out,
    state,
    fields,
    a_hi,
    a_lo,
    s_hi,
    s_lo,
    t_hi,
    t_lo,
    picked,
    wi,
    lines,
    line_ends,
    gathered,
    xb,
    yb,
    y_out,
    z_out,
    z_in,
    xz_out,
    xz_in,
    xy_out,
    xy_in,
    dx_out,
    dx_in,
    dy,
    dy_in,
    dz_out,
    dz_in,
    dxe_out,
    dxe_in,
    local_sem,
    send_sem,
    recv_sem,
):
    n = pos.shape[1]
    me = {axis: lax.axis_index(axis) for axis in sizes}
    ends = {axis: size - 1 for axis, size in sizes.items()}

    def copy(src, dst, number, side, axis, peer):
        return pltpu.make_async_remote_copy(
            src_ref=src,
            dst_ref=dst,
            send_sem=send_sem.at[2 * number + side],
            recv_sem=recv_sem.at[2 * number + side],
            device_id={axis: peer},
            device_id_type=MESH,
        )

    def send(number, axis, up, land0, down, land1):
        @pl.when(me[axis] < ends[axis])
        def _():
            copy(up, land0, number, 0, axis, me[axis] + 1).start()

        @pl.when(me[axis] > 0)
        def _():
            copy(down, land1, number, 1, axis, me[axis] - 1).start()

    def arrive(number, axis, up, land0, down, land1):
        @pl.when(me[axis] > 0)
        def _():
            copy(up, land0, number, 0, axis, me[axis] - 1).wait_recv()

        @pl.when(me[axis] < ends[axis])
        def _():
            copy(down, land1, number, 1, axis, me[axis] + 1).wait_recv()

    def sent(number, axis, up, land0, down, land1):
        @pl.when(me[axis] < ends[axis])
        def _():
            copy(up, land0, number, 0, axis, me[axis] + 1).wait_send()

        @pl.when(me[axis] > 0)
        def _():
            copy(down, land1, number, 1, axis, me[axis] - 1).wait_send()

    def blank(axis, land0, land1):
        @pl.when(me[axis] == 0)
        def _():
            land0[...] = jnp.zeros(land0.shape, F32)

        @pl.when(me[axis] == ends[axis])
        def _():
            land1[...] = jnp.zeros(land1.shape, F32)

    x_vel = (0, "gx", vel.at[:, CI - 1], xb.at[0:3, 0:CJ], vel.at[:, 0], xb.at[0:3, CJ:128])
    x_scal = (1, "gx", scal.at[:, CI - 1], xb.at[3:6, 0:CJ], scal.at[:, 0], xb.at[3:6, CJ:128])
    y_rows = (2, "gy", y_out.at[1], yb.at[:, 0:8], y_out.at[0], yb.at[:, 16:24])
    z_cols = (3, "gz", z_out.at[1], z_in.at[0:8], z_out.at[0], z_in.at[8:16])
    xz_cols = (4, "gx", xz_out.at[1], xz_in.at[0], xz_out.at[0], xz_in.at[1])
    xy_rows = (5, "gx", xy_out.at[1], xy_in.at[0], xy_out.at[0], xy_in.at[1])
    d_x = (6, "gx", dx_out.at[1], dx_in.at[0], dx_out.at[0], dx_in.at[1])
    d_z = (7, "gz", dz_out.at[8:16], dz_in.at[0:8], dz_out.at[0:8], dz_in.at[8:16])
    d_y = (8, "gy", dy.at[16:32], dy_in.at[0], dy.at[0:16], dy_in.at[1])
    d_xe = (9, "gx", dxe_out.at[1], dxe_in.at[0], dxe_out.at[0], dxe_in.at[1])
    transfers = (x_vel, x_scal, y_rows, z_cols, xz_cols, xy_rows, d_x, d_z, d_y, d_xe)

    load_vel = pltpu.make_async_copy(vel, fields.at[0:3], local_sem.at[0])
    load_scal = pltpu.make_async_copy(scal, fields.at[3:6], local_sem.at[1])
    load_vel.start()
    load_scal.start()

    barrier = pltpu.get_barrier_semaphore()
    for axis in sizes:

        @pl.when(me[axis] > 0)
        def _():
            pl.semaphore_signal(
                barrier, inc=1, device_id={axis: me[axis] - 1}, device_id_type=MESH
            )

        @pl.when(me[axis] < ends[axis])
        def _():
            pl.semaphore_signal(
                barrier, inc=1, device_id={axis: me[axis] + 1}, device_id_type=MESH
            )

    for number, axis, up, land0, down, land1 in transfers:
        blank(axis, land0, land1)
    yb[:, 8:16] = jnp.zeros((NF, 8, CK), F32)
    yb[:, 24:128] = jnp.zeros((NF, 104, CK), F32)
    dz_in[16:128] = jnp.zeros((112, COLS), F32)
    xy_out[...] = jnp.zeros(xy_out.shape, F32)

    peers = 0
    for axis in sizes:
        peers = peers + jnp.minimum(me[axis], 1) + jnp.minimum(ends[axis] - me[axis], 1)
    pl.semaphore_wait(barrier, peers)

    send(*x_vel)
    send(*x_scal)
    load_vel.wait()
    load_scal.wait()

    for f in range(NF):
        for i in range(CI):
            y_out[0, f, i : i + 1, :] = fields[f, i, 0:1, :]
            y_out[1, f, i : i + 1, :] = fields[f, i, CJ - 1 : CJ, :]
    send(*y_rows)

    z_out[...] = jnp.zeros(z_out.shape, F32)
    for f in range(NF):
        for b in range(OWN // 128):
            block = fields[f, 2 * b : 2 * b + 2].reshape(128, CK).T
            z_out[0, f : f + 1, b * 128 : b * 128 + 128] = block[0:1]
            z_out[1, f : f + 1, b * 128 : b * 128 + 128] = block[CK - 1 : CK]
            hi, lo = split(block)
            a_hi[f * CK : f * CK + CK, b * 128 : b * 128 + 128] = hi
            a_lo[f * CK : f * CK + CK, b * 128 : b * 128 + 128] = lo

    arrive(*y_rows)
    for f in range(NF):
        block = yb[f].T
        z_out[0, f : f + 1, YB:COLS] = block[0:1]
        z_out[1, f : f + 1, YB:COLS] = block[CK - 1 : CK]
    send(*z_cols)
    for side, i in ((0, 0), (1, CI - 1)):
        for part in range(2):
            for f in range(NF):
                row = yb[f, 16 * part + i : 16 * part + i + 1, :]
                xy_out[side, 8 * part + f : 8 * part + f + 1, :] = row
    send(*xy_rows)

    where_i = li[...].reshape(1, n).astype(F32)
    where_j = lj[...].reshape(1, n).astype(F32)
    where_k = lk[...].reshape(1, n).astype(F32)
    row16 = iota((16, n), 0)
    plane = jnp.where(row16 == 8, -1, jnp.where(row16 == 9, CI, row16)).astype(F32)
    spread = tent(pos[0:1, :] - (plane - where_i))
    wi[...] = jnp.where(row16 < 10, spread, 0.0)
    wj = tent(pos[1:2, :] - (iota((CJ, n), 0).astype(F32) - where_j))
    wj_ends = (tent(pos[1:2, :] - (-1.0 - where_j)), tent(pos[1:2, :] - (float(CJ) - where_j)))
    lines[...] = tent(pos[2:3, :] - (iota((CK, n), 0).astype(F32) - where_k))
    line_ends[0:1, :] = tent(pos[2:3, :] - (-1.0 - where_k))
    line_ends[1:2, :] = tent(pos[2:3, :] - (float(CK) - where_k))
    for i in range(10):
        hi, lo = split(wi[i : i + 1, :] * wj)
        s_hi[i * CJ : i * CJ + CJ, :] = hi
        s_lo[i * CJ : i * CJ + CJ, :] = lo
    for part in range(2):
        hi, lo = split(wi[...] * wj_ends[part])
        s_hi[YB + 16 * part : YB + 16 * part + 16, :] = hi
        s_lo[YB + 16 * part : YB + 16 * part + 16, :] = lo
    s_hi[YB + 32 : COLS, :] = jnp.zeros((96, n), BF16)
    s_lo[YB + 32 : COLS, :] = jnp.zeros((96, n), BF16)

    arrive(*z_cols)
    for part in range(2):
        xz_out[0, 8 * part : 8 * part + 8, 0:128] = z_in[8 * part : 8 * part + 8, 0:128]
        xz_out[1, 8 * part : 8 * part + 8, 0:128] = z_in[8 * part : 8 * part + 8, OWN - 128 : OWN]
        for side in range(2):
            xz_out[side, 8 * part : 8 * part + 8, 128:256] = z_in[8 * part : 8 * part + 8, YB:COLS]
    send(*xz_cols)
    hi, lo = split(z_in[:, 0:OWN])
    a_hi[NF * CK : ROWS, 0:OWN] = hi
    a_lo[NF * CK : ROWS, 0:OWN] = lo

    def pick(columns, chunk):
        left = jnp.concatenate([a_hi[:, columns], a_hi[:, columns], a_lo[:, columns]], axis=1)
        right = jnp.concatenate(
            [s_hi[columns, chunk], s_lo[columns, chunk], s_hi[columns, chunk]], axis=0
        )
        return jnp.dot(left, right, preferred_element_type=F32)

    chunks = [slice(c * 256, c * 256 + 256) for c in range(n // 256)]
    for chunk in chunks:
        picked[:, chunk] = pick(slice(0, OWN), chunk)

    arrive(*xy_rows)
    for part in range(2):
        for f in range(NF):
            for side in range(2):
                row = xy_in[side, 8 * part + f : 8 * part + f + 1, :]
                yb[f, 16 * part + 8 + side : 16 * part + 9 + side, :] = row
    arrive(*xz_cols)
    lane = iota((16, 128), 1)
    x_part = jnp.where(
        lane < CJ,
        pltpu.roll(xz_in[0, :, 0:128], 64, 1),
        pltpu.roll(xz_in[1, :, 0:128], 64, 1),
    )
    lane16 = lane % 16
    y_part = jnp.where(
        lane16 == 8,
        pltpu.roll(xz_in[0, :, 128:256], 1, 1),
        jnp.where(lane16 == 9, pltpu.roll(xz_in[1, :, 128:256], 9, 1), z_in[:, YB:COLS]),
    )
    for column, part in ((XB, x_part), (YB, y_part)):
        hi, lo = split(part)
        a_hi[NF * CK : ROWS, column : column + 128] = hi
        a_lo[NF * CK : ROWS, column : column + 128] = lo
    for f in range(NF):
        hi, lo = split(yb[f].T)
        a_hi[f * CK : f * CK + CK, YB:COLS] = hi
        a_lo[f * CK : f * CK + CK, YB:COLS] = lo
    arrive(*x_vel)
    arrive(*x_scal)
    for f in range(NF):
        hi, lo = split(xb[f].T)
        a_hi[f * CK : f * CK + CK, XB:YB] = hi
        a_lo[f * CK : f * CK + CK, XB:YB] = lo

    for chunk in chunks:
        value = picked[:, chunk] + pick(slice(OWN, COLS), chunk)
        for f in range(NF):
            total = jnp.sum(value[f * CK : f * CK + CK] * lines[:, chunk], axis=0, keepdims=True)
            for part in range(2):
                row = NF * CK + 8 * part + f
                total = total + value[row : row + 1] * line_ends[part : part + 1, chunk]
            gathered[f : f + 1, chunk] = total

    motion = mot[...]
    warmth = heat[...].reshape(1, n)
    q = diam[...].reshape(1, n)
    gas = gathered[0:3, :]
    gas_heat, moisture, rho = gathered[3:4, :], gathered[4:5, :], gathered[5:6, :]
    drag = step_time / (0.5 * q)
    new_motion = (motion + drag * gas) / (1.0 + drag)
    mass = q * jnp.sqrt(q)
    vapour = jnp.exp(4.0 * (warmth - 1.0))
    decay = step_time * evap_rate * rho * (vapour - moisture)
    new_q = q - decay
    new_mass = new_q * jnp.sqrt(new_q)
    conduction = step_time * heat_rate * rho / q
    new_heat = (warmth + conduction * gas_heat) / (1.0 + conduction) - (
        boiling_energy_drain * decay / q
    )
    live = iota((1, n), 1) // TILE < tally[0]
    state[0:3, :] = jnp.where(live, new_motion, motion)
    state[3:4, :] = jnp.where(live, new_heat, warmth)
    state[4:5, :] = jnp.where(live, new_q, q)
    mass = jnp.where(live, mass, 0.0)
    terms = [mass * (motion[c : c + 1] - new_motion[c : c + 1]) for c in range(3)]
    terms.append(mass * (warmth - new_heat))
    terms.append(jnp.where(live, mass - new_mass, 0.0))

    for c in range(NS):
        hi, lo = split(terms[c] * lines[...])
        t_hi[c * CK : c * CK + CK, :] = hi
        t_lo[c * CK : c * CK + CK, :] = lo
    packed = jnp.concatenate(terms + [jnp.zeros((3, n), F32)], axis=0)
    tail = jnp.concatenate([packed * line_ends[0:1, :], packed * line_ends[1:2, :]], axis=0)
    hi, lo = split(tail)
    t_hi[NS * CK : NS * CK + 16, :] = hi
    t_lo[NS * CK : NS * CK + 16, :] = lo
    t_hi[NS * CK + 16 : COLS, :] = jnp.zeros((112, n), BF16)
    t_lo[NS * CK + 16 : COLS, :] = jnp.zeros((112, n), BF16)

    def spill(line, column):
        left = jnp.concatenate([s_hi[line, :], s_lo[line, :], s_hi[line, :]], axis=1)
        right = jnp.concatenate([t_hi[column, :], t_hi[column, :], t_lo[column, :]], axis=1)
        return lax.dot_general(
            left, right, (((1,), (1,)), ((), ())), preferred_element_type=F32
        )

    def put_z(block, column):
        dz_out[:, column : column + 128] = block.T[0:16]

    rim = slice(OWN, COLS)
    for w in range(3):
        value = spill(rim, slice(w * 256, w * 256 + 256))
        for h in range(2):
            c = 2 * w + h
            half = value[:, h * 128 : h * 128 + 128]
            if c < NS:
                dx_out[0, :, c * CK : c * CK + CK] = half[0:64]
                dx_out[1, :, c * CK : c * CK + CK] = half[64:128]
                dy[:, c * CK : c * CK + CK] = half[128:160]
            else:
                put_z(half[0:128], XB)
                put_z(half[128:256], YB)
    send(*d_x)

    for w in (2, 0, 1):
        value = spill(slice(0, OWN), slice(w * 256, w * 256 + 256))
        for h in range(2):
            c = 2 * w + h
            half = value[:, h * 128 : h * 128 + 128]
            if c < NS:
                out[c] = half.reshape(CI, CJ, CK)
            else:
                for b in range(OWN // 128):
                    put_z(half[b * 128 : b * 128 + 128], b * 128)
        if w == 2:
            send(*d_z)

    lane128 = iota((128, 128), 1)

    def ends_of(columns, c):
        return jnp.where(
            lane128 == 0,
            columns[:, c : c + 1],
            jnp.where(lane128 == CK - 1, columns[:, 8 + c : 9 + c], 0.0),
        )

    arrive(*d_z)
    y_cols = dz_in[:, YB:COLS].T
    for c in range(NS):
        at = slice(c * CK, c * CK + CK)
        dy[:, at] = dy[:, at] + ends_of(y_cols, c)[0:32]
    send(*d_y)
    for b in range(OWN // 128):
        columns = dz_in[:, b * 128 : b * 128 + 128].T
        for c in range(NS):
            add = ends_of(columns, c).reshape(2, CJ, CK)
            out[c, 2 * b : 2 * b + 2] = out[c, 2 * b : 2 * b + 2] + add

    arrive(*d_y)
    for side in range(2):
        dxe_out[side, 0:16, :] = dz_in[0:16, XB:YB]
        dxe_out[side, 16:32, :] = jnp.zeros((16, CK), F32)
        for part in range(2):
            for c in range(NS):
                row = dy_in[part, 8 + side : 9 + side, c * CK : c * CK + CK]
                dxe_out[side, 16 + 8 * part + c : 17 + 8 * part + c, :] = row
    send(*d_xe)
    for part in range(2):
        j = 0 if part == 0 else CJ - 1
        for c in range(NS):
            for i in range(CI):
                out[c, i, j : j + 1, :] = (
                    out[c, i, j : j + 1, :] + dy_in[part, i : i + 1, c * CK : c * CK + CK]
                )

    arrive(*d_xe)
    for side in range(2):
        i = 0 if side == 0 else CI - 1
        for part in range(2):
            j = 0 if part == 0 else CJ - 1
            for c in range(NS):
                row = 16 + 8 * part + c
                out[c, i, j : j + 1, :] = out[c, i, j : j + 1, :] + dxe_in[side, row : row + 1, :]
    x_cols = jnp.where(
        lane < CJ,
        pltpu.roll(dxe_in[0, 0:16, :], 64, 1),
        pltpu.roll(dxe_in[1, 0:16, :], 64, 1),
    )
    x_cols = jnp.concatenate([x_cols, jnp.zeros((112, 128), F32)], axis=0).T
    for c in range(NS):
        add = ends_of(x_cols, c)
        out[c, 0] = out[c, 0] + add[0:CJ]
        out[c, CI - 1] = out[c, CI - 1] + add[CJ:128]

    arrive(*d_x)
    for side in range(2):
        i = 0 if side == 0 else CI - 1
        for c in range(NS):
            out[c, i] = out[c, i] + dx_in[side, :, c * CK : c * CK + CK]

    for transfer in transfers:
        sent(*transfer)


def local(sizes, vel, scal, pos, mot, heat, diam, li, lj, lk, tally):
    n = heat.shape[0]
    vmem = pl.BlockSpec(memory_space=pltpu.VMEM)
    hbm = pl.BlockSpec(memory_space=pl.ANY)
    return pl.pallas_call(
        functools.partial(kernel, sizes),
        out_shape=(
            jax.ShapeDtypeStruct((NS, CI, CJ, CK), F32),
            jax.ShapeDtypeStruct((NS, n), F32),
        ),
        in_specs=[hbm, hbm] + [vmem] * 7 + [pl.BlockSpec(memory_space=pltpu.SMEM)],
        out_specs=(vmem, vmem),
        scratch_shapes=[
            pltpu.VMEM((NF, CI, CJ, CK), F32),
            pltpu.VMEM((ROWS, COLS), BF16),
            pltpu.VMEM((ROWS, COLS), BF16),
            pltpu.VMEM((COLS, n), BF16),
            pltpu.VMEM((COLS, n), BF16),
            pltpu.VMEM((COLS, n), BF16),
            pltpu.VMEM((COLS, n), BF16),
            pltpu.VMEM((ROWS, n), F32),
            pltpu.VMEM((16, n), F32),
            pltpu.VMEM((CK, n), F32),
            pltpu.VMEM((8, n), F32),
            pltpu.VMEM((8, n), F32),
            pltpu.VMEM((NF, 128, CK), F32),
            pltpu.VMEM((NF, 128, CK), F32),
            pltpu.VMEM((2, NF, 8, CK), F32),
            pltpu.VMEM((2, 8, COLS), F32),
            pltpu.VMEM((16, COLS), F32),
            pltpu.VMEM((2, 16, 256), F32),
            pltpu.VMEM((2, 16, 256), F32),
            pltpu.VMEM((2, 16, CK), F32),
            pltpu.VMEM((2, 16, CK), F32),
            pltpu.VMEM((2, CJ, NS * CK), F32),
            pltpu.VMEM((2, CJ, NS * CK), F32),
            pltpu.VMEM((32, NS * CK), F32),
            pltpu.VMEM((2, 16, NS * CK), F32),
            pltpu.VMEM((16, COLS), F32),
            pltpu.VMEM((128, COLS), F32),
            pltpu.VMEM((2, 32, CK), F32),
            pltpu.VMEM((2, 32, CK), F32),
            pltpu.SemaphoreType.DMA((2,)),
            pltpu.SemaphoreType.DMA((20,)),
            pltpu.SemaphoreType.DMA((20,)),
        ],
        compiler_params=pltpu.CompilerParams(
            collective_id=0, has_side_effects=True, vmem_limit_bytes=60 * 1024 * 1024
        ),
    )(vel, scal, pos, mot, heat, diam, li, lj, lk, tally)


def solution(mesh):
    sizes = {axis: mesh.shape[axis] for axis in ("gx", "gy", "gz")}
    flat = P(("gx", "gy", "gz"))
    wide = P(None, ("gx", "gy", "gz"))
    grid = P(None, "gx", "gy", "gz")
    return jax.shard_map(
        functools.partial(local, sizes),
        mesh=mesh,
        in_specs=(grid, grid, wide, wide) + (flat,) * 6,
        out_specs=(grid, wide),
        check_vma=False,
    )
```

```python
import functools

import jax
import jax.numpy as jnp
from jax import lax
from jax.experimental import pallas as pl
from jax.experimental.pallas import tpu as pltpu
from jax.sharding import PartitionSpec as P

TILE = 128
NF = 6
NS = 5
CI, CJ, CK = 8, 64, 128
OWN = CI * CJ
COLS = OWN + 128
ROWS = NF * CK + 16
MESH = pl.DeviceIdType.MESH
F32 = jnp.float32
BF16 = jnp.bfloat16

step_time = 0.25
evap_rate = 1.0
heat_rate = 2.0
boiling_energy_drain = 0.3


def split(x):
    hi = x.astype(BF16)
    return hi, (x - hi.astype(F32)).astype(BF16)


def tent(offset):
    return jnp.maximum(0.0, 1.0 - jnp.abs(offset))


def iota(shape, dim):
    return lax.broadcasted_iota(jnp.int32, shape, dim)


def kernel(
    sizes,
    vel,
    scal,
    pos_hbm,
    mot_hbm,
    heat_hbm,
    diam_hbm,
    li_hbm,
    lj_hbm,
    lk_hbm,
    tally,
    out,
    state,
    fields,
    pos,
    mot,
    heat,
    diam,
    li,
    lj,
    lk,
    mine,
    theirs,
    a_hi,
    a_lo,
    s_hi,
    s_lo,
    t_hi,
    t_lo,
    e_lhs,
    l_hi,
    l_lo,
    u_hi,
    u_lo,
    ws,
    ws_ends,
    wi,
    lines,
    line_ends,
    gathered,
    part_out,
    part_in,
    terms_out,
    terms_in,
    yb,
    y_out,
    z_out,
    z_in,
    yz_in,
    dy,
    dy_in,
    dz_out,
    dz_in,
    dyz_in,
    local_sem,
    send_sem,
    recv_sem,
):
    n = pos.shape[1]
    axes = tuple(sizes)
    me = {axis: lax.axis_index(axis) for axis in axes}
    ends = {axis: size - 1 for axis, size in sizes.items()}

    def there(steps):
        found = None
        for axis, step in steps:
            one = me[axis] < ends[axis] if step > 0 else me[axis] > 0
            found = one if found is None else jnp.logical_and(found, one)
        return found

    def peer(steps):
        return {axis: me[axis] + step for axis, step in steps}

    def back(steps):
        return tuple((axis, -step) for axis, step in steps)

    numbers = iter(range(64))

    def both(axis, up, land0, down, land1):
        return (
            (next(numbers), ((axis, 1),), up, land0),
            (next(numbers), ((axis, -1),), down, land1),
        )

    def corners(source, land):
        found = []
        for y in (1, -1):
            for z in (1, -1):
                sides = (0 if y > 0 else 1, 0 if z > 0 else 1)
                steps = (("gy", y), ("gz", z))
                found.append((next(numbers), steps, source(1 - sides[1]), land.at[sides]))
        return tuple(found)

    def copy(transfer, steps):
        number, _, source, land = transfer
        return pltpu.make_async_remote_copy(
            src_ref=source,
            dst_ref=land,
            send_sem=send_sem.at[number],
            recv_sem=recv_sem.at[number],
            device_id=peer(steps),
            device_id_type=MESH,
        )

    def send(group):
        for transfer in group:
            pl.when(there(transfer[1]))(lambda t=transfer: copy(t, t[1]).start())

    def arrive(group):
        for transfer in group:
            steps = back(transfer[1])
            pl.when(there(steps))(lambda t=transfer, s=steps: copy(t, s).wait_recv())

    def sent(group):
        for transfer in group:
            pl.when(there(transfer[1]))(lambda t=transfer: copy(t, t[1]).wait_send())

    def blank(group):
        for _, steps, _, land in group:

            @pl.when(jnp.logical_not(there(back(steps))))
            def _():
                land[...] = jnp.zeros(land.shape, F32)

    g_pos = both("gx", mine, theirs.at[0], mine, theirs.at[1])
    g_y = both("gy", y_out.at[1], yb.at[:, 0:8], y_out.at[0], yb.at[:, 16:24])
    g_z = both("gz", z_out.at[1], z_in.at[0:8], z_out.at[0], z_in.at[8:16])
    g_yz = corners(lambda side: z_out.at[side], yz_in)
    g_part = both("gx", part_out.at[1], part_in.at[0], part_out.at[0], part_in.at[1])
    d_terms = both("gx", terms_out, terms_in.at[0], terms_out, terms_in.at[1])
    d_z = both(
        "gz",
        dz_out.at[8:16, 0:OWN],
        dz_in.at[0:8],
        dz_out.at[0:8, 0:OWN],
        dz_in.at[8:16],
    )
    d_y = both("gy", dy.at[16:24], dy_in.at[0], dy.at[0:8], dy_in.at[1])
    d_yz = corners(lambda side: dz_out.at[8 * side : 8 * side + 8, OWN:COLS], dyz_in)
    groups = (g_pos, g_y, g_z, g_yz, g_part, d_terms, d_z, d_y, d_yz)

    loads = []
    for number, (source, land) in enumerate(
        (
            (pos_hbm, pos),
            (li_hbm, li),
            (lj_hbm, lj),
            (lk_hbm, lk),
            (vel, fields.at[0:3]),
            (scal, fields.at[3:6]),
            (mot_hbm, mot),
            (heat_hbm, heat),
            (diam_hbm, diam),
        )
    ):
        loads.append(pltpu.make_async_copy(source, land, local_sem.at[number]))
        loads[-1].start()

    barrier = pltpu.get_barrier_semaphore()
    for _, steps, _, _ in g_pos + g_y + g_z + g_yz:
        pl.when(there(steps))(
            lambda s=steps: pl.semaphore_signal(
                barrier, inc=1, device_id=peer(s), device_id_type=MESH
            )
        )

    for group in groups:
        blank(group)
    yb[:, 8:16] = jnp.zeros((NF, 8, CK), F32)
    yb[:, 24:128] = jnp.zeros((NF, 104, CK), F32)
    z_out[...] = jnp.zeros(z_out.shape, F32)
    part_out[:, 6:8] = jnp.zeros((2, 2, n), F32)
    for x in range(2):
        l_hi[x, CK : 2 * CK] = jnp.zeros((CK, n), BF16)
        l_lo[x, CK : 2 * CK] = jnp.zeros((CK, n), BF16)
    s_hi[OWN + 32 : COLS] = jnp.zeros((96, n), BF16)
    s_lo[OWN + 32 : COLS] = jnp.zeros((96, n), BF16)
    t_hi[NS * CK + 16 :] = jnp.zeros((112, n), BF16)
    t_lo[NS * CK + 16 :] = jnp.zeros((112, n), BF16)

    for load in loads[0:4]:
        load.wait()
    mine[0:3] = pos[...]
    for axis, cell in enumerate((li, lj, lk)):
        mine[3 + axis : 4 + axis] = cell[...].reshape(1, n).astype(F32)
    mine[6:8] = jnp.zeros((2, n), F32)

    near = {axis: jnp.minimum(me[axis], 1) + jnp.minimum(ends[axis] - me[axis], 1) for axis in axes}
    pl.semaphore_wait(barrier, near["gx"] + near["gy"] + near["gz"] + near["gy"] * near["gz"])
    send(g_pos)

    for load in loads[4:]:
        load.wait()
    for f in range(NF):
        for i in range(CI):
            y_out[0, f, i : i + 1, :] = fields[f, i, 0:1, :]
            y_out[1, f, i : i + 1, :] = fields[f, i, CJ - 1 : CJ, :]
    send(g_y)

    for f in range(NF):
        for b in range(OWN // 128):
            block = fields[f, 2 * b : 2 * b + 2].reshape(128, CK).T
            z_out[0, f : f + 1, b * 128 : b * 128 + 128] = block[0:1]
            z_out[1, f : f + 1, b * 128 : b * 128 + 128] = block[CK - 1 : CK]
            hi, lo = split(block)
            a_hi[f * CK : f * CK + CK, b * 128 : b * 128 + 128] = hi
            a_lo[f * CK : f * CK + CK, b * 128 : b * 128 + 128] = lo
    send(g_z)
    send(g_yz)

    def ramp(rows):
        return iota((rows, n), 0).astype(F32)

    row16 = iota((16, n), 0)
    spread = tent(mine[0:1] - (ramp(16) - mine[3:4]))
    wi[...] = jnp.where(row16 < CI, spread, 0.0)
    wj = tent(mine[1:2] - (ramp(CJ) - mine[4:5]))
    wj_ends = (tent(mine[1:2] - (-1.0 - mine[4:5])), tent(mine[1:2] - (float(CJ) - mine[4:5])))
    lines[...] = tent(mine[2:3] - (ramp(CK) - mine[5:6]))
    line_ends[0:1] = tent(mine[2:3] - (-1.0 - mine[5:6]))
    line_ends[1:2] = tent(mine[2:3] - (float(CK) - mine[5:6]))
    for i in range(CI):
        hi, lo = split(wi[i : i + 1] * wj)
        s_hi[i * CJ : i * CJ + CJ] = hi
        s_lo[i * CJ : i * CJ + CJ] = lo
    for y in range(2):
        hi, lo = split(wi[...] * wj_ends[y])
        s_hi[OWN + 16 * y : OWN + 16 * y + 16] = hi
        s_lo[OWN + 16 * y : OWN + 16 * y + 16] = lo

    lane16 = iota((16, 128), 1)
    arrive(g_y)
    for f in range(NF):
        hi, lo = split(yb[f].T)
        a_hi[f * CK : f * CK + CK, OWN:COLS] = hi
        a_lo[f * CK : f * CK + CK, OWN:COLS] = lo
    arrive(g_z)
    hi, lo = split(z_in[...])
    a_hi[NF * CK : ROWS, 0:OWN] = hi
    a_lo[NF * CK : ROWS, 0:OWN] = lo
    arrive(g_yz)
    corner = jnp.zeros((16, 128), F32)
    for y in range(2):
        for i in range(CI):
            at = i * CJ + (CJ - 1 if y == 0 else 0)
            first = at // 128 * 128
            block = jnp.concatenate([yz_in[y, z, :, first : first + 128] for z in range(2)], axis=0)
            to = 16 * y + i
            moved = pltpu.roll(block, (to - at) % 128, 1)
            corner = jnp.where(lane16 == to, moved, corner)
    hi, lo = split(corner)
    a_hi[NF * CK : ROWS, OWN:COLS] = hi
    a_lo[NF * CK : ROWS, OWN:COLS] = lo

    def z_block(value):
        hi, lo = split(value)
        hi, lo = hi.astype(F32), lo.astype(F32)
        return (hi + pltpu.roll(hi, 16, 1) + pltpu.roll(lo, 32, 1)).astype(BF16)

    def put_plane(x, at, rows, value, ends_value):
        hi, lo = split(value)
        e_lhs[x, at : at + rows, 0:128] = hi
        e_lhs[x, at : at + rows, 128:256] = hi
        e_lhs[x, at : at + rows, 256:384] = lo
        e_lhs[x, at : at + rows, 384:512] = z_block(ends_value)

    lane64 = iota((CJ, 128), 1)
    lane8 = iota((8, 128), 1)
    for x in range(2):
        i = 0 if x == 0 else CI - 1
        first = i * CJ // 128 * 128
        columns = jnp.concatenate(
            [z_in[:, first : first + 128], jnp.zeros((112, 128), F32)], axis=0
        ).T
        columns = columns[0:CJ] if x == 0 else columns[CJ:128]
        for f in range(NF):
            moved = columns if f == 0 else pltpu.roll(columns, 128 - f, 1)
            moved = jnp.where((lane64 == 0) | (lane64 == 8), moved, 0.0)
            put_plane(x, f * CJ, CJ, fields[f, i], moved)
        values, moves = [], []
        for y in range(2):
            values += [yb[f, 16 * y + i : 16 * y + i + 1, :] for f in range(NF)]
            values.append(jnp.zeros((2, CK), F32))
            at = i * CJ + (CJ - 1 if y == 0 else 0)
            first = at // 128 * 128
            total = jnp.zeros((8, 128), F32)
            for z in range(2):
                block = pltpu.roll(yz_in[y, z, :, first : first + 128], (8 * z - at) % 128, 1)
                total = jnp.where(lane8 == 8 * z, block, total)
            moves.append(total)
        put_plane(
            x, NF * CJ, 16, jnp.concatenate(values, axis=0), jnp.concatenate(moves, axis=0)
        )

    chunks = [slice(c * 256, c * 256 + 256) for c in range(n // 256)]

    def gather(chunk):
        left = jnp.concatenate([a_hi[...], a_hi[...], a_lo[...]], axis=1)
        right = jnp.concatenate([s_hi[:, chunk], s_lo[:, chunk], s_hi[:, chunk]], axis=0)
        value = jnp.dot(left, right, preferred_element_type=F32)
        for f in range(NF):
            total = jnp.sum(value[f * CK : f * CK + CK] * lines[:, chunk], axis=0, keepdims=True)
            for z in range(2):
                row = NF * CK + 8 * z + f
                total = total + value[row : row + 1] * line_ends[z : z + 1, chunk]
            gathered[f : f + 1, chunk] = total

    for chunk in chunks[:2]:
        gather(chunk)

    arrive(g_pos)
    for x in range(2):
        p = theirs.at[x]
        reach = tent(p[0:1] - ((float(CI) if x == 0 else -1.0) - p[3:4]))
        ws[x] = reach * tent(p[1:2] - (ramp(CJ) - p[4:5]))
        ws_ends[x, 0:1] = reach * tent(p[1:2] - (-1.0 - p[4:5]))
        ws_ends[x, 1:2] = reach * tent(p[1:2] - (float(CJ) - p[4:5]))
        hi, lo = split(tent(p[2:3] - (ramp(CK) - p[5:6])))
        l_hi[x, 0:CK] = hi
        l_lo[x, 0:CK] = lo
        low = tent(p[2:3] - (-1.0 - p[5:6]))
        high = tent(p[2:3] - (float(CK) - p[5:6]))
        hi, lo = split(jnp.where(row16 == 0, low, jnp.where(row16 == 8, high, 0.0)))
        l_hi[x, CK : CK + 16] = hi
        l_lo[x, CK : CK + 16] = lo
    for x in range(2):
        for chunk in chunks:
            top, low = l_hi[x, 0:CK, chunk], l_lo[x, 0:CK, chunk]
            top_z, low_z = l_hi[x, CK : CK + 16, chunk], l_lo[x, CK : CK + 16, chunk]
            right = jnp.concatenate(
                [top, low, top, top_z, low_z, top_z, jnp.zeros((80, 256), BF16)], axis=0
            )
            value = jnp.dot(e_lhs[x], right, preferred_element_type=F32)
            last = NF * CJ
            total = value[last : last + 8] * ws_ends[x, 0:1, chunk]
            total = total + value[last + 8 : last + 16] * ws_ends[x, 1:2, chunk]
            weight = ws[x, :, chunk]
            for f in range(NF):
                row = jnp.sum(value[f * CJ : f * CJ + CJ] * weight, axis=0, keepdims=True)
                part_out[x, f : f + 1, chunk] = row + total[f : f + 1]
    send(g_part)

    for chunk in chunks[2:]:
        gather(chunk)

    motion = mot[...]
    warmth = heat[...].reshape(1, n)
    q = diam[...].reshape(1, n)
    live = iota((1, n), 1) // TILE < tally[0]
    arrive(g_part)
    got = gathered[0:NF] + part_in[0, 0:NF] + part_in[1, 0:NF]
    gas = got[0:3]
    gas_heat, moisture, rho = got[3:4], got[4:5], got[5:6]
    drag = step_time / (0.5 * q)
    new_motion = (motion + drag * gas) / (1.0 + drag)
    mass = q * jnp.sqrt(q)
    vapour = jnp.exp(4.0 * (warmth - 1.0))
    decay = step_time * evap_rate * rho * (vapour - moisture)
    new_q = q - decay
    new_mass = new_q * jnp.sqrt(new_q)
    conduction = step_time * heat_rate * rho / q
    new_heat = (warmth + conduction * gas_heat) / (1.0 + conduction) - (
        boiling_energy_drain * decay / q
    )
    state[0:3] = jnp.where(live, new_motion, motion)
    state[3:4] = jnp.where(live, new_heat, warmth)
    state[4:5] = jnp.where(live, new_q, q)
    terms_out[0:3] = jnp.where(live, mass * (motion - new_motion), 0.0)
    terms_out[3:4] = jnp.where(live, mass * (warmth - new_heat), 0.0)
    terms_out[4:5] = jnp.where(live, mass - new_mass, 0.0)
    terms_out[5:8] = jnp.zeros((3, n), F32)
    send(d_terms)

    for c in range(NS):
        hi, lo = split(terms_out[c : c + 1] * lines[...])
        t_hi[c * CK : c * CK + CK] = hi
        t_lo[c * CK : c * CK + CK] = lo
    tail = jnp.concatenate(
        [terms_out[...] * line_ends[0:1], terms_out[...] * line_ends[1:2]], axis=0
    )
    hi, lo = split(tail)
    t_hi[NS * CK : NS * CK + 16] = hi
    t_lo[NS * CK : NS * CK + 16] = lo

    def cross(left, right):
        return lax.dot_general(
            left, right, (((1,), (1,)), ((), ())), preferred_element_type=F32
        )

    lines_used = slice(0, OWN + 32)
    for w in range(3):
        column = slice(w * 256, w * 256 + 256)
        left = jnp.concatenate(
            [s_hi[lines_used], s_lo[lines_used], s_hi[lines_used]], axis=1
        )
        right = jnp.concatenate([t_hi[column], t_hi[column], t_lo[column]], axis=1)
        value = cross(left, right)
        for h in range(2):
            c = 2 * w + h
            half = value[:, h * 128 : h * 128 + 128]
            if c < NS:
                out[c] = half[0:OWN].reshape(CI, CJ, CK)
                dy[:, c * CK : c * CK + CK] = half[OWN : OWN + 32]
            else:
                for b in range(OWN // 128):
                    dz_out[:, b * 128 : b * 128 + 128] = half[b * 128 : b * 128 + 128].T[0:16]
                rest = jnp.concatenate([half[OWN : OWN + 32], jnp.zeros((96, 128), F32)], axis=0)
                dz_out[:, OWN:COLS] = rest.T[0:16]

    arrive(d_terms)
    lane1 = iota((1, 128), 1)
    for x in range(2):
        i = 0 if x == 0 else CI - 1
        weight = ws[x]
        for c in range(NS):
            hi, lo = split(terms_in[x, c : c + 1] * weight)
            u_hi[c * CJ : c * CJ + CJ] = hi
            u_lo[c * CJ : c * CJ + CJ] = lo
        last = NS * CJ
        for y in range(2):
            hi, lo = split(
                jnp.concatenate(
                    [terms_in[x] * ws_ends[x, y : y + 1], jnp.zeros((8, n), F32)], axis=0
                )
            )
            u_hi[last + 16 * y : last + 16 * y + 16] = hi
            u_lo[last + 16 * y : last + 16 * y + 16] = lo
        left = jnp.concatenate([u_hi[...], u_hi[...], u_lo[...]], axis=1)
        right = jnp.concatenate([l_hi[x], l_lo[x], l_hi[x]], axis=1)
        value = cross(left, right)
        for c in range(NS):
            out[c, i] = out[c, i] + value[c * CJ : c * CJ + CJ, 0:CK]
            for y in range(2):
                row = 16 * y + i
                at = slice(c * CK, c * CK + CK)
                line = last + 16 * y + c
                dy[row : row + 1, at] = dy[row : row + 1, at] + value[line : line + 1, 0:CK]
        first = i * CJ // 128 * 128
        keep = lane1 < CJ if x == 0 else lane1 >= CJ
        for b in range(3):
            block = value[b * 128 : min(b * 128 + 128, last + 32), CK : 2 * CK]
            if b == 2:
                block = jnp.concatenate([block, jnp.zeros((32, 128), F32)], axis=0)
            block = block.T
            for c in range(2 * b, min(2 * b + 2, NS)):
                for z in range(2):
                    row = block[8 * z : 8 * z + 1]
                    if c % 2 != x:
                        row = pltpu.roll(row, CJ, 1)
                    at = 8 * z + c
                    old = dz_out[at : at + 1, first : first + 128]
                    dz_out[at : at + 1, first : first + 128] = old + jnp.where(keep, row, 0.0)
        for y in range(2):
            block = value[last + 16 * y : last + 16 * y + 8, CK : 2 * CK]
            to = 16 * y + i
            for z in range(2):
                moved = pltpu.roll(block, (to - 8 * z) % 128, 1)
                old = dz_out[8 * z : 8 * z + 8, OWN:COLS]
                dz_out[8 * z : 8 * z + 8, OWN:COLS] = old + jnp.where(lane8 == to, moved, 0.0)
    send(d_z)
    send(d_yz)
    send(d_y)

    arrive(d_yz)
    arrive(d_z)
    lane128 = iota((128, 128), 1)
    for b in range(OWN // 128):
        block = dz_in[:, b * 128 : b * 128 + 128]
        for i in (2 * b, 2 * b + 1):
            for y in range(2):
                to = i * CJ % 128 + (0 if y == 0 else CJ - 1)
                at = (16 if y == 0 else 0) + i
                moved = jnp.concatenate([dyz_in[y, 0], dyz_in[y, 1]], axis=0)
                moved = pltpu.roll(moved, (to - at) % 128, 1)
                block = block + jnp.where(lane16 == to, moved, 0.0)
        columns = jnp.concatenate([block, jnp.zeros((112, 128), F32)], axis=0).T
        for c in range(NS):
            add = jnp.where(
                lane128 == 0,
                columns[:, c : c + 1],
                jnp.where(lane128 == CK - 1, columns[:, 8 + c : 9 + c], 0.0),
            ).reshape(2, CJ, CK)
            out[c, 2 * b : 2 * b + 2] = out[c, 2 * b : 2 * b + 2] + add
    arrive(d_y)
    for y in range(2):
        j = 0 if y == 0 else CJ - 1
        for c in range(NS):
            for i in range(CI):
                out[c, i, j : j + 1, :] = (
                    out[c, i, j : j + 1, :] + dy_in[y, i : i + 1, c * CK : c * CK + CK]
                )

    for group in groups:
        sent(group)


def local(sizes, vel, scal, pos, mot, heat, diam, li, lj, lk, tally):
    n = heat.shape[0]
    vmem = pl.BlockSpec(memory_space=pltpu.VMEM)
    hbm = pl.BlockSpec(memory_space=pltpu.HBM)
    planes = NF * CJ + 16
    return pl.pallas_call(
        functools.partial(kernel, sizes),
        out_shape=(
            jax.ShapeDtypeStruct((NS, CI, CJ, CK), F32),
            jax.ShapeDtypeStruct((NS, n), F32),
        ),
        in_specs=[hbm] * 9 + [pl.BlockSpec(memory_space=pltpu.SMEM)],
        out_specs=(vmem, vmem),
        scratch_shapes=[
            pltpu.VMEM((NF, CI, CJ, CK), F32),
            pltpu.VMEM((3, n), F32),
            pltpu.VMEM((3, n), F32),
            pltpu.VMEM((n,), F32),
            pltpu.VMEM((n,), F32),
            pltpu.VMEM((n,), jnp.int32),
            pltpu.VMEM((n,), jnp.int32),
            pltpu.VMEM((n,), jnp.int32),
            pltpu.VMEM((8, n), F32),
            pltpu.VMEM((2, 8, n), F32),
            pltpu.VMEM((ROWS, COLS), BF16),
            pltpu.VMEM((ROWS, COLS), BF16),
            pltpu.VMEM((COLS, n), BF16),
            pltpu.VMEM((COLS, n), BF16),
            pltpu.VMEM((768, n), BF16),
            pltpu.VMEM((768, n), BF16),
            pltpu.VMEM((2, planes, 512), BF16),
            pltpu.VMEM((2, 2 * CK, n), BF16),
            pltpu.VMEM((2, 2 * CK, n), BF16),
            pltpu.VMEM((NS * CJ + 32, n), BF16),
            pltpu.VMEM((NS * CJ + 32, n), BF16),
            pltpu.VMEM((2, CJ, n), F32),
            pltpu.VMEM((2, 8, n), F32),
            pltpu.VMEM((16, n), F32),
            pltpu.VMEM((CK, n), F32),
            pltpu.VMEM((8, n), F32),
            pltpu.VMEM((8, n), F32),
            pltpu.VMEM((2, 8, n), F32),
            pltpu.VMEM((2, 8, n), F32),
            pltpu.VMEM((8, n), F32),
            pltpu.VMEM((2, 8, n), F32),
            pltpu.VMEM((NF, 128, CK), F32),
            pltpu.VMEM((2, NF, 8, CK), F32),
            pltpu.VMEM((2, 8, OWN), F32),
            pltpu.VMEM((16, OWN), F32),
            pltpu.VMEM((2, 2, 8, OWN), F32),
            pltpu.VMEM((32, NS * CK), F32),
            pltpu.VMEM((2, 8, NS * CK), F32),
            pltpu.VMEM((16, COLS), F32),
            pltpu.VMEM((16, OWN), F32),
            pltpu.VMEM((2, 2, 8, 128), F32),
            pltpu.SemaphoreType.DMA((9,)),
            pltpu.SemaphoreType.DMA((22,)),
            pltpu.SemaphoreType.DMA((22,)),
        ],
        compiler_params=pltpu.CompilerParams(
            collective_id=0, has_side_effects=True, vmem_limit_bytes=32 * 1024 * 1024
        ),
    )(vel, scal, pos, mot, heat, diam, li, lj, lk, tally)


def solution(mesh):
    sizes = {axis: mesh.shape[axis] for axis in ("gx", "gy", "gz")}
    flat = P(("gx", "gy", "gz"))
    wide = P(None, ("gx", "gy", "gz"))
    grid = P(None, "gx", "gy", "gz")
    return jax.shard_map(
        functools.partial(local, sizes),
        mesh=mesh,
        in_specs=(grid, grid, wide, wide) + (flat,) * 6,
        out_specs=(grid, wide),
        check_vma=False,
    )
```

```python
import functools

import jax
import jax.numpy as jnp
from jax import lax
from jax.experimental import pallas as pl
from jax.experimental.pallas import tpu as pltpu
from jax.sharding import PartitionSpec as P

TILE = 128
NF = 6
NS = 5
CI, CJ, CK = 8, 64, 128
OWN = CI * CJ
COLS = OWN + 128
ROWS = NF * CK + 16
MESH = pl.DeviceIdType.MESH
F32 = jnp.float32
BF16 = jnp.bfloat16

step_time = 0.25
evap_rate = 1.0
heat_rate = 2.0
boiling_energy_drain = 0.3


def split(x):
    hi = x.astype(BF16)
    return hi, (x - hi.astype(F32)).astype(BF16)


def tent(offset):
    return jnp.maximum(0.0, 1.0 - jnp.abs(offset))


def iota(shape, dim):
    return lax.broadcasted_iota(jnp.int32, shape, dim)


def kernel(
    sizes,
    vel,
    scal,
    pos_hbm,
    mot_hbm,
    heat_hbm,
    diam_hbm,
    li_hbm,
    lj_hbm,
    lk_hbm,
    tally,
    out,
    state,
    fields,
    pos,
    mot,
    heat,
    diam,
    li,
    lj,
    lk,
    mine,
    theirs,
    a_hi,
    a_lo,
    s_hi,
    s_lo,
    t_hi,
    t_lo,
    e_lhs,
    l_hi,
    l_lo,
    u_hi,
    u_lo,
    ws,
    ws_ends,
    wi,
    lines,
    line_ends,
    gathered,
    part_out,
    part_in,
    terms_out,
    terms_in,
    yb,
    y_out,
    z_out,
    z_in,
    yz_in,
    dy,
    dy_in,
    dz_out,
    dz_in,
    dyz_in,
    local_sem,
    send_sem,
    recv_sem,
):
    n = pos.shape[1]
    axes = tuple(sizes)
    me = {axis: lax.axis_index(axis) for axis in axes}
    ends = {axis: size - 1 for axis, size in sizes.items()}

    def there(steps):
        found = None
        for axis, step in steps:
            one = me[axis] < ends[axis] if step > 0 else me[axis] > 0
            found = one if found is None else jnp.logical_and(found, one)
        return found

    def peer(steps):
        return {axis: me[axis] + step for axis, step in steps}

    def back(steps):
        return tuple((axis, -step) for axis, step in steps)

    numbers = iter(range(64))

    def both(axis, up, land0, down, land1):
        return (
            (next(numbers), ((axis, 1),), up, land0),
            (next(numbers), ((axis, -1),), down, land1),
        )

    def corners(source, land):
        found = []
        for y in (1, -1):
            for z in (1, -1):
                sides = (0 if y > 0 else 1, 0 if z > 0 else 1)
                steps = (("gy", y), ("gz", z))
                found.append((next(numbers), steps, source(1 - sides[1]), land.at[sides]))
        return tuple(found)

    def copy(transfer, steps):
        number, _, source, land = transfer
        return pltpu.make_async_remote_copy(
            src_ref=source,
            dst_ref=land,
            send_sem=send_sem.at[number],
            recv_sem=recv_sem.at[number],
            device_id=peer(steps),
            device_id_type=MESH,
        )

    def send(group):
        for transfer in group:
            pl.when(there(transfer[1]))(lambda t=transfer: copy(t, t[1]).start())

    def arrive(group):
        for transfer in group:
            steps = back(transfer[1])
            pl.when(there(steps))(lambda t=transfer, s=steps: copy(t, s).wait_recv())

    def sent(group):
        for transfer in group:
            pl.when(there(transfer[1]))(lambda t=transfer: copy(t, t[1]).wait_send())

    def blank(group):
        for _, steps, _, land in group:

            @pl.when(jnp.logical_not(there(back(steps))))
            def _():
                land[...] = jnp.zeros(land.shape, F32)

    g_pos = both("gx", mine, theirs.at[0], mine, theirs.at[1])
    g_y = both("gy", y_out.at[1], yb.at[:, 0:8], y_out.at[0], yb.at[:, 16:24])
    g_z = both("gz", z_out.at[1], z_in.at[0:8], z_out.at[0], z_in.at[8:16])
    g_yz = corners(lambda side: z_out.at[side], yz_in)
    g_part = both("gx", part_out.at[1], part_in.at[0], part_out.at[0], part_in.at[1])
    d_terms = both("gx", terms_out, terms_in.at[0], terms_out, terms_in.at[1])
    d_z = both(
        "gz",
        dz_out.at[8:16, 0:OWN],
        dz_in.at[0:8],
        dz_out.at[0:8, 0:OWN],
        dz_in.at[8:16],
    )
    d_y = both("gy", dy.at[16:24], dy_in.at[0], dy.at[0:8], dy_in.at[1])
    d_yz = corners(lambda side: dz_out.at[8 * side : 8 * side + 8, OWN:COLS], dyz_in)
    groups = (g_pos, g_y, g_z, g_yz, g_part, d_terms, d_z, d_y, d_yz)

    loads = []
    for number, (source, land) in enumerate(
        (
            (pos_hbm, pos),
            (li_hbm, li),
            (lj_hbm, lj),
            (lk_hbm, lk),
            (vel, fields.at[0:3]),
            (scal, fields.at[3:6]),
            (mot_hbm, mot),
            (heat_hbm, heat),
            (diam_hbm, diam),
        )
    ):
        loads.append(pltpu.make_async_copy(source, land, local_sem.at[number]))
        loads[-1].start()

    barrier = pltpu.get_barrier_semaphore()
    for _, steps, _, _ in g_pos + g_y + g_z + g_yz:
        pl.when(there(steps))(
            lambda s=steps: pl.semaphore_signal(
                barrier, inc=1, device_id=peer(s), device_id_type=MESH
            )
        )

    for group in groups:
        blank(group)
    yb[:, 8:16] = jnp.zeros((NF, 8, CK), F32)
    yb[:, 24:128] = jnp.zeros((NF, 104, CK), F32)
    z_out[...] = jnp.zeros(z_out.shape, F32)
    part_out[:, 6:8] = jnp.zeros((2, 2, n), F32)
    for x in range(2):
        l_hi[x, CK : 2 * CK] = jnp.zeros((CK, n), BF16)
        l_lo[x, CK : 2 * CK] = jnp.zeros((CK, n), BF16)
    s_hi[OWN + 32 : COLS] = jnp.zeros((96, n), BF16)
    s_lo[OWN + 32 : COLS] = jnp.zeros((96, n), BF16)
    t_hi[NS * CK + 16 :] = jnp.zeros((112, n), BF16)
    t_lo[NS * CK + 16 :] = jnp.zeros((112, n), BF16)

    for load in loads[0:4]:
        load.wait()
    mine[0:3] = pos[...]
    for axis, cell in enumerate((li, lj, lk)):
        mine[3 + axis : 4 + axis] = cell[...].reshape(1, n).astype(F32)
    mine[6:8] = jnp.zeros((2, n), F32)

    near = {axis: jnp.minimum(me[axis], 1) + jnp.minimum(ends[axis] - me[axis], 1) for axis in axes}
    pl.semaphore_wait(barrier, near["gx"] + near["gy"] + near["gz"] + near["gy"] * near["gz"])
    send(g_pos)

    for load in loads[4:]:
        load.wait()
    for f in range(NF):
        for i in range(CI):
            y_out[0, f, i : i + 1, :] = fields[f, i, 0:1, :]
            y_out[1, f, i : i + 1, :] = fields[f, i, CJ - 1 : CJ, :]
    send(g_y)

    for f in range(NF):
        for b in range(OWN // 128):
            block = fields[f, 2 * b : 2 * b + 2].reshape(128, CK).T
            z_out[0, f : f + 1, b * 128 : b * 128 + 128] = block[0:1]
            z_out[1, f : f + 1, b * 128 : b * 128 + 128] = block[CK - 1 : CK]
            hi, lo = split(block)
            a_hi[f * CK : f * CK + CK, b * 128 : b * 128 + 128] = hi
            a_lo[f * CK : f * CK + CK, b * 128 : b * 128 + 128] = lo
    send(g_z)
    send(g_yz)

    def ramp(rows):
        return iota((rows, n), 0).astype(F32)

    row16 = iota((16, n), 0)
    spread = tent(mine[0:1] - (ramp(16) - mine[3:4]))
    wi[...] = jnp.where(row16 < CI, spread, 0.0)
    wj = tent(mine[1:2] - (ramp(CJ) - mine[4:5]))
    wj_ends = (tent(mine[1:2] - (-1.0 - mine[4:5])), tent(mine[1:2] - (float(CJ) - mine[4:5])))
    lines[...] = tent(mine[2:3] - (ramp(CK) - mine[5:6]))
    line_ends[0:1] = tent(mine[2:3] - (-1.0 - mine[5:6]))
    line_ends[1:2] = tent(mine[2:3] - (float(CK) - mine[5:6]))
    for i in range(CI):
        hi, lo = split(wi[i : i + 1] * wj)
        s_hi[i * CJ : i * CJ + CJ] = hi
        s_lo[i * CJ : i * CJ + CJ] = lo
    for y in range(2):
        hi, lo = split(wi[...] * wj_ends[y])
        s_hi[OWN + 16 * y : OWN + 16 * y + 16] = hi
        s_lo[OWN + 16 * y : OWN + 16 * y + 16] = lo

    lane16 = iota((16, 128), 1)
    arrive(g_y)
    for f in range(NF):
        hi, lo = split(yb[f].T)
        a_hi[f * CK : f * CK + CK, OWN:COLS] = hi
        a_lo[f * CK : f * CK + CK, OWN:COLS] = lo
    arrive(g_z)
    hi, lo = split(z_in[...])
    a_hi[NF * CK : ROWS, 0:OWN] = hi
    a_lo[NF * CK : ROWS, 0:OWN] = lo
    arrive(g_yz)
    corner = jnp.zeros((16, 128), F32)
    for y in range(2):
        for i in range(CI):
            at = i * CJ + (CJ - 1 if y == 0 else 0)
            first = at // 128 * 128
            block = jnp.concatenate([yz_in[y, z, :, first : first + 128] for z in range(2)], axis=0)
            to = 16 * y + i
            moved = pltpu.roll(block, (to - at) % 128, 1)
            corner = jnp.where(lane16 == to, moved, corner)
    hi, lo = split(corner)
    a_hi[NF * CK : ROWS, OWN:COLS] = hi
    a_lo[NF * CK : ROWS, OWN:COLS] = lo

    def z_block(value):
        hi, lo = split(value)
        hi, lo = hi.astype(F32), lo.astype(F32)
        return (hi + pltpu.roll(hi, 16, 1) + pltpu.roll(lo, 32, 1)).astype(BF16)

    def put_plane(x, at, rows, value, ends_value):
        hi, lo = split(value)
        e_lhs[x, at : at + rows, 0:128] = hi
        e_lhs[x, at : at + rows, 128:256] = hi
        e_lhs[x, at : at + rows, 256:384] = lo
        e_lhs[x, at : at + rows, 384:512] = z_block(ends_value)

    lane64 = iota((CJ, 128), 1)
    lane8 = iota((8, 128), 1)
    for x in range(2):
        i = 0 if x == 0 else CI - 1
        first = i * CJ // 128 * 128
        columns = jnp.concatenate(
            [z_in[:, first : first + 128], jnp.zeros((112, 128), F32)], axis=0
        ).T
        columns = columns[0:CJ] if x == 0 else columns[CJ:128]
        for f in range(NF):
            moved = columns if f == 0 else pltpu.roll(columns, 128 - f, 1)
            moved = jnp.where((lane64 == 0) | (lane64 == 8), moved, 0.0)
            put_plane(x, f * CJ, CJ, fields[f, i], moved)
        values, moves = [], []
        for y in range(2):
            values += [yb[f, 16 * y + i : 16 * y + i + 1, :] for f in range(NF)]
            values.append(jnp.zeros((2, CK), F32))
            at = i * CJ + (CJ - 1 if y == 0 else 0)
            first = at // 128 * 128
            total = jnp.zeros((8, 128), F32)
            for z in range(2):
                block = pltpu.roll(yz_in[y, z, :, first : first + 128], (8 * z - at) % 128, 1)
                total = jnp.where(lane8 == 8 * z, block, total)
            moves.append(total)
        put_plane(
            x, NF * CJ, 16, jnp.concatenate(values, axis=0), jnp.concatenate(moves, axis=0)
        )

    chunks = [slice(c * 256, c * 256 + 256) for c in range(n // 256)]

    def gather(chunk):
        left = jnp.concatenate([a_hi[...], a_hi[...], a_lo[...]], axis=1)
        right = jnp.concatenate([s_hi[:, chunk], s_lo[:, chunk], s_hi[:, chunk]], axis=0)
        value = jnp.dot(left, right, preferred_element_type=F32)
        for f in range(NF):
            total = jnp.sum(value[f * CK : f * CK + CK] * lines[:, chunk], axis=0, keepdims=True)
            for z in range(2):
                row = NF * CK + 8 * z + f
                total = total + value[row : row + 1] * line_ends[z : z + 1, chunk]
            gathered[f : f + 1, chunk] = total

    for chunk in chunks[:2]:
        gather(chunk)

    arrive(g_pos)
    for x in range(2):
        p = theirs.at[x]
        reach = tent(p[0:1] - ((float(CI) if x == 0 else -1.0) - p[3:4]))
        ws[x] = reach * tent(p[1:2] - (ramp(CJ) - p[4:5]))
        ws_ends[x, 0:1] = reach * tent(p[1:2] - (-1.0 - p[4:5]))
        ws_ends[x, 1:2] = reach * tent(p[1:2] - (float(CJ) - p[4:5]))
        hi, lo = split(tent(p[2:3] - (ramp(CK) - p[5:6])))
        l_hi[x, 0:CK] = hi
        l_lo[x, 0:CK] = lo
        low = tent(p[2:3] - (-1.0 - p[5:6]))
        high = tent(p[2:3] - (float(CK) - p[5:6]))
        hi, lo = split(jnp.where(row16 == 0, low, jnp.where(row16 == 8, high, 0.0)))
        l_hi[x, CK : CK + 16] = hi
        l_lo[x, CK : CK + 16] = lo
    for x in range(2):
        for chunk in chunks:
            top, low = l_hi[x, 0:CK, chunk], l_lo[x, 0:CK, chunk]
            top_z, low_z = l_hi[x, CK : CK + 16, chunk], l_lo[x, CK : CK + 16, chunk]
            right = jnp.concatenate(
                [top, low, top, top_z, low_z, top_z, jnp.zeros((80, 256), BF16)], axis=0
            )
            value = jnp.dot(e_lhs[x], right, preferred_element_type=F32)
            last = NF * CJ
            total = value[last : last + 8] * ws_ends[x, 0:1, chunk]
            total = total + value[last + 8 : last + 16] * ws_ends[x, 1:2, chunk]
            weight = ws[x, :, chunk]
            for f in range(NF):
                row = jnp.sum(value[f * CJ : f * CJ + CJ] * weight, axis=0, keepdims=True)
                part_out[x, f : f + 1, chunk] = row + total[f : f + 1]
    send(g_part)

    for chunk in chunks[2:]:
        gather(chunk)

    motion = mot[...]
    warmth = heat[...].reshape(1, n)
    q = diam[...].reshape(1, n)
    live = iota((1, n), 1) // TILE < tally[0]
    arrive(g_part)
    got = gathered[0:NF] + part_in[0, 0:NF] + part_in[1, 0:NF]
    gas = got[0:3]
    gas_heat, moisture, rho = got[3:4], got[4:5], got[5:6]
    drag = step_time / (0.5 * q)
    new_motion = (motion + drag * gas) / (1.0 + drag)
    mass = q * jnp.sqrt(q)
    vapour = jnp.exp(4.0 * (warmth - 1.0))
    decay = step_time * evap_rate * rho * (vapour - moisture)
    new_q = q - decay
    new_mass = new_q * jnp.sqrt(new_q)
    conduction = step_time * heat_rate * rho / q
    new_heat = (warmth + conduction * gas_heat) / (1.0 + conduction) - (
        boiling_energy_drain * decay / q
    )
    state[0:3] = jnp.where(live, new_motion, motion)
    state[3:4] = jnp.where(live, new_heat, warmth)
    state[4:5] = jnp.where(live, new_q, q)
    terms_out[0:3] = jnp.where(live, mass * (motion - new_motion), 0.0)
    terms_out[3:4] = jnp.where(live, mass * (warmth - new_heat), 0.0)
    terms_out[4:5] = jnp.where(live, mass - new_mass, 0.0)
    terms_out[5:8] = jnp.zeros((3, n), F32)
    send(d_terms)

    for c in range(NS):
        hi, lo = split(terms_out[c : c + 1] * lines[...])
        t_hi[c * CK : c * CK + CK] = hi
        t_lo[c * CK : c * CK + CK] = lo
    tail = jnp.concatenate(
        [terms_out[...] * line_ends[0:1], terms_out[...] * line_ends[1:2]], axis=0
    )
    hi, lo = split(tail)
    t_hi[NS * CK : NS * CK + 16] = hi
    t_lo[NS * CK : NS * CK + 16] = lo

    def cross(left, right):
        return lax.dot_general(
            left, right, (((1,), (1,)), ((), ())), preferred_element_type=F32
        )

    lines_used = slice(0, OWN + 32)
    for w in range(3):
        column = slice(w * 256, w * 256 + 256)
        left = jnp.concatenate(
            [s_hi[lines_used], s_lo[lines_used], s_hi[lines_used]], axis=1
        )
        right = jnp.concatenate([t_hi[column], t_hi[column], t_lo[column]], axis=1)
        value = cross(left, right)
        for h in range(2):
            c = 2 * w + h
            half = value[:, h * 128 : h * 128 + 128]
            if c < NS:
                out[c] = half[0:OWN].reshape(CI, CJ, CK)
                dy[:, c * CK : c * CK + CK] = half[OWN : OWN + 32]
            else:
                for b in range(OWN // 128):
                    dz_out[:, b * 128 : b * 128 + 128] = half[b * 128 : b * 128 + 128].T[0:16]
                rest = jnp.concatenate([half[OWN : OWN + 32], jnp.zeros((96, 128), F32)], axis=0)
                dz_out[:, OWN:COLS] = rest.T[0:16]

    arrive(d_terms)
    lane1 = iota((1, 128), 1)
    for x in range(2):
        i = 0 if x == 0 else CI - 1
        weight = ws[x]
        for c in range(NS):
            hi, lo = split(terms_in[x, c : c + 1] * weight)
            u_hi[c * CJ : c * CJ + CJ] = hi
            u_lo[c * CJ : c * CJ + CJ] = lo
        last = NS * CJ
        for y in range(2):
            hi, lo = split(
                jnp.concatenate(
                    [terms_in[x] * ws_ends[x, y : y + 1], jnp.zeros((8, n), F32)], axis=0
                )
            )
            u_hi[last + 16 * y : last + 16 * y + 16] = hi
            u_lo[last + 16 * y : last + 16 * y + 16] = lo
        left = jnp.concatenate([u_hi[...], u_hi[...], u_lo[...]], axis=1)
        right = jnp.concatenate([l_hi[x], l_lo[x], l_hi[x]], axis=1)
        value = cross(left, right)
        for c in range(NS):
            out[c, i] = out[c, i] + value[c * CJ : c * CJ + CJ, 0:CK]
            for y in range(2):
                row = 16 * y + i
                at = slice(c * CK, c * CK + CK)
                line = last + 16 * y + c
                dy[row : row + 1, at] = dy[row : row + 1, at] + value[line : line + 1, 0:CK]
        first = i * CJ // 128 * 128
        keep = lane1 < CJ if x == 0 else lane1 >= CJ
        for b in range(3):
            block = value[b * 128 : min(b * 128 + 128, last + 32), CK : 2 * CK]
            if b == 2:
                block = jnp.concatenate([block, jnp.zeros((32, 128), F32)], axis=0)
            block = block.T
            for c in range(2 * b, min(2 * b + 2, NS)):
                for z in range(2):
                    row = block[8 * z : 8 * z + 1]
                    if c % 2 != x:
                        row = pltpu.roll(row, CJ, 1)
                    at = 8 * z + c
                    old = dz_out[at : at + 1, first : first + 128]
                    dz_out[at : at + 1, first : first + 128] = old + jnp.where(keep, row, 0.0)
        for y in range(2):
            block = value[last + 16 * y : last + 16 * y + 8, CK : 2 * CK]
            to = 16 * y + i
            for z in range(2):
                moved = pltpu.roll(block, (to - 8 * z) % 128, 1)
                old = dz_out[8 * z : 8 * z + 8, OWN:COLS]
                dz_out[8 * z : 8 * z + 8, OWN:COLS] = old + jnp.where(lane8 == to, moved, 0.0)
    send(d_z)
    send(d_yz)
    send(d_y)

    arrive(d_yz)
    arrive(d_z)
    lane128 = iota((128, 128), 1)
    for b in range(OWN // 128):
        block = dz_in[:, b * 128 : b * 128 + 128]
        for i in (2 * b, 2 * b + 1):
            for y in range(2):
                to = i * CJ % 128 + (0 if y == 0 else CJ - 1)
                at = (16 if y == 0 else 0) + i
                moved = jnp.concatenate([dyz_in[y, 0], dyz_in[y, 1]], axis=0)
                moved = pltpu.roll(moved, (to - at) % 128, 1)
                block = block + jnp.where(lane16 == to, moved, 0.0)
        columns = jnp.concatenate([block, jnp.zeros((112, 128), F32)], axis=0).T
        for c in range(NS):
            add = jnp.where(
                lane128 == 0,
                columns[:, c : c + 1],
                jnp.where(lane128 == CK - 1, columns[:, 8 + c : 9 + c], 0.0),
            ).reshape(2, CJ, CK)
            out[c, 2 * b : 2 * b + 2] = out[c, 2 * b : 2 * b + 2] + add
    arrive(d_y)
    for y in range(2):
        j = 0 if y == 0 else CJ - 1
        for c in range(NS):
            for i in range(CI):
                out[c, i, j : j + 1, :] = (
                    out[c, i, j : j + 1, :] + dy_in[y, i : i + 1, c * CK : c * CK + CK]
                )

    for group in groups:
        sent(group)


def local(sizes, vel, scal, pos, mot, heat, diam, li, lj, lk, tally):
    n = heat.shape[0]
    vmem = pl.BlockSpec(memory_space=pltpu.VMEM)
    hbm = pl.BlockSpec(memory_space=pltpu.HBM)
    planes = NF * CJ + 16
    return pl.pallas_call(
        functools.partial(kernel, sizes),
        out_shape=(
            jax.ShapeDtypeStruct((NS, CI, CJ, CK), F32),
            jax.ShapeDtypeStruct((NS, n), F32),
        ),
        in_specs=[hbm] * 9 + [pl.BlockSpec(memory_space=pltpu.SMEM)],
        out_specs=(vmem, vmem),
        scratch_shapes=[
            pltpu.VMEM((NF, CI, CJ, CK), F32),
            pltpu.VMEM((3, n), F32),
            pltpu.VMEM((3, n), F32),
            pltpu.VMEM((n,), F32),
            pltpu.VMEM((n,), F32),
            pltpu.VMEM((n,), jnp.int32),
            pltpu.VMEM((n,), jnp.int32),
            pltpu.VMEM((n,), jnp.int32),
            pltpu.VMEM((8, n), F32),
            pltpu.VMEM((2, 8, n), F32),
            pltpu.VMEM((ROWS, COLS), BF16),
            pltpu.VMEM((ROWS, COLS), BF16),
            pltpu.VMEM((COLS, n), BF16),
            pltpu.VMEM((COLS, n), BF16),
            pltpu.VMEM((768, n), BF16),
            pltpu.VMEM((768, n), BF16),
            pltpu.VMEM((2, planes, 512), BF16),
            pltpu.VMEM((2, 2 * CK, n), BF16),
            pltpu.VMEM((2, 2 * CK, n), BF16),
            pltpu.VMEM((NS * CJ + 32, n), BF16),
            pltpu.VMEM((NS * CJ + 32, n), BF16),
            pltpu.VMEM((2, CJ, n), F32),
            pltpu.VMEM((2, 8, n), F32),
            pltpu.VMEM((16, n), F32),
            pltpu.VMEM((CK, n), F32),
            pltpu.VMEM((8, n), F32),
            pltpu.VMEM((8, n), F32),
            pltpu.VMEM((2, 8, n), F32),
            pltpu.VMEM((2, 8, n), F32),
            pltpu.VMEM((8, n), F32),
            pltpu.VMEM((2, 8, n), F32),
            pltpu.VMEM((NF, 128, CK), F32),
            pltpu.VMEM((2, NF, 8, CK), F32),
            pltpu.VMEM((2, 8, OWN), F32),
            pltpu.VMEM((16, OWN), F32),
            pltpu.VMEM((2, 2, 8, OWN), F32),
            pltpu.VMEM((32, NS * CK), F32),
            pltpu.VMEM((2, 8, NS * CK), F32),
            pltpu.VMEM((16, COLS), F32),
            pltpu.VMEM((16, OWN), F32),
            pltpu.VMEM((2, 2, 8, 128), F32),
            pltpu.SemaphoreType.DMA((9,)),
            pltpu.SemaphoreType.DMA((22,)),
            pltpu.SemaphoreType.DMA((22,)),
        ],
        compiler_params=pltpu.CompilerParams(
            collective_id=0, has_side_effects=True, vmem_limit_bytes=32 * 1024 * 1024
        ),
    )(*(pltpu.with_memory_space_constraint(x, pltpu.HBM) for x in (vel, scal, pos, mot, heat, diam, li, lj, lk)), tally)


def solution(mesh):
    sizes = {axis: mesh.shape[axis] for axis in ("gx", "gy", "gz")}
    flat = P(("gx", "gy", "gz"))
    wide = P(None, ("gx", "gy", "gz"))
    grid = P(None, "gx", "gy", "gz")
    return jax.shard_map(
        functools.partial(local, sizes),
        mesh=mesh,
        in_specs=(grid, grid, wide, wide) + (flat,) * 6,
        out_specs=(grid, wide),
        check_vma=False,
    )
```

```python
import functools
import itertools

import jax
import jax.numpy as jnp
from jax import lax
from jax.experimental import pallas as pl
from jax.experimental.pallas import tpu as pltpu
from jax.sharding import PartitionSpec as P

TILE = 128
NF = 6
NS = 5
CI, CJ, CK = 8, 64, 128
OWN = CI * CJ
COLS = OWN + 128
ROWS = NF * CK + 16
MESH = pl.DeviceIdType.MESH
F32 = jnp.float32
BF16 = jnp.bfloat16

step_time = 0.25
evap_rate = 1.0
heat_rate = 2.0
boiling_energy_drain = 0.3


def split(x):
    hi = x.astype(BF16)
    return hi, (x - hi.astype(F32)).astype(BF16)


def tent(offset):
    return jnp.maximum(0.0, 1.0 - jnp.abs(offset))


def iota(shape, dim):
    return lax.broadcasted_iota(jnp.int32, shape, dim)


def kernel(
    sizes,
    vel,
    scal,
    pos_hbm,
    mot_hbm,
    heat_hbm,
    diam_hbm,
    li_hbm,
    lj_hbm,
    lk_hbm,
    tally,
    out,
    state,
    fields,
    pos,
    mot,
    heat,
    diam,
    li,
    lj,
    lk,
    mine,
    theirs,
    a_hi,
    a_lo,
    s_hi,
    s_lo,
    t_hi,
    t_lo,
    e_lhs,
    l_hi,
    l_lo,
    u_hi,
    u_lo,
    x_hi,
    x_lo,
    edges,
    ws,
    ws_ends,
    wi,
    lines,
    line_ends,
    gathered,
    part_out,
    part_in,
    terms_out,
    terms_pack,
    terms_in,
    yb,
    y_out,
    z_out,
    z_in,
    yz_in,
    dy,
    dy_in,
    dz_out,
    dz_in,
    dyz_in,
    dxz_out,
    dxz_in,
    dxy_out,
    dxy_in,
    dxyz_in,
    zt,
    local_sem,
    send_sem,
    recv_sem,
):
    n = pos.shape[1]
    axes = tuple(sizes)
    me = {axis: lax.axis_index(axis) for axis in axes}
    ends = {axis: size - 1 for axis, size in sizes.items()}

    def there(steps):
        found = None
        for axis, step in steps:
            one = me[axis] < ends[axis] if step > 0 else me[axis] > 0
            found = one if found is None else jnp.logical_and(found, one)
        return found

    def peer(steps):
        return {axis: me[axis] + step for axis, step in steps}

    def back(steps):
        return tuple((axis, -step) for axis, step in steps)

    numbers = iter(range(64))

    def pack(ref, number, row):
        for b in range(n // 128):
            at = number * (n // 128) + b
            ref[at : at + 1, :] = row[:, b * 128 : b * 128 + 128]

    def unpack(ref, number):
        first = number * (n // 128)
        return jnp.concatenate([ref[first + b : first + b + 1, :] for b in range(n // 128)], axis=1)

    def both(axis, up, land0, down, land1):
        return (
            (next(numbers), ((axis, 1),), up, land0),
            (next(numbers), ((axis, -1),), down, land1),
        )

    def diagonal(axes, source, land):
        found = []
        for steps in itertools.product((1, -1), repeat=len(axes)):
            sides = tuple((1 - step) // 2 for step in steps)
            from_sides = tuple(1 - side for side in sides)
            steps = tuple(zip(axes, steps))
            found.append((next(numbers), steps, source(*from_sides), land.at[sides]))
        return tuple(found)

    def copy(transfer, steps):
        number, _, source, land = transfer
        return pltpu.make_async_remote_copy(
            src_ref=source,
            dst_ref=land,
            send_sem=send_sem.at[number],
            recv_sem=recv_sem.at[number],
            device_id=peer(steps),
            device_id_type=MESH,
        )

    def send(group):
        for transfer in group:
            pl.when(there(transfer[1]))(lambda t=transfer: copy(t, t[1]).start())

    def arrive(group):
        for transfer in group:
            steps = back(transfer[1])
            pl.when(there(steps))(lambda t=transfer, s=steps: copy(t, s).wait_recv())

    def sent(group):
        for transfer in group:
            pl.when(there(transfer[1]))(lambda t=transfer: copy(t, t[1]).wait_send())

    def blank(group):
        for _, steps, _, land in group:

            @pl.when(jnp.logical_not(there(back(steps))))
            def _():
                land[...] = jnp.zeros(land.shape, F32)

    g_pos = both("gx", mine.at[1], theirs.at[0], mine.at[0], theirs.at[1])
    g_y = both("gy", y_out.at[1], yb.at[:, 0:8], y_out.at[0], yb.at[:, 16:24])
    g_z = both("gz", z_out.at[1], z_in.at[0:8], z_out.at[0], z_in.at[8:16])
    g_yz = diagonal(("gy", "gz"), lambda y, z: z_out.at[z], yz_in)
    g_part = both("gx", part_out.at[1], part_in.at[0], part_out.at[0], part_in.at[1])
    d_terms = both("gx", terms_pack, terms_in.at[0], terms_pack, terms_in.at[1])
    d_z = both(
        "gz",
        dz_out.at[8:16, 0:OWN],
        dz_in.at[0:8],
        dz_out.at[0:8, 0:OWN],
        dz_in.at[8:16],
    )
    d_y = both("gy", dy.at[16:24], dy_in.at[0], dy.at[0:8], dy_in.at[1])
    d_yz = diagonal(
        ("gy", "gz"), lambda y, z: dz_out.at[8 * z : 8 * z + 8, OWN:COLS], dyz_in
    )
    d_xz = diagonal(("gx", "gz"), lambda x, z: dxz_out.at[8 * z : 8 * z + 8], dxz_in)

    def edge(x, y):
        first = 16 * x + 8 * y
        return slice(first, first + 8)

    d_xy = diagonal(("gx", "gy"), lambda x, y: dxy_out.at[edge(x, y), 0:128], dxy_in)
    d_xyz = diagonal(
        ("gx", "gy", "gz"), lambda x, y, z: dxy_out.at[edge(x, y), 128:256], dxyz_in
    )
    groups = (g_pos, g_y, g_z, g_yz, g_part, d_terms, d_xz, d_xy, d_xyz, d_z, d_y, d_yz)

    loads = []
    for number, (source, land) in enumerate(
        (
            (pos_hbm, pos),
            (li_hbm, li),
            (lj_hbm, lj),
            (lk_hbm, lk),
            (vel, fields.at[0:3]),
            (scal, fields.at[3:6]),
            (mot_hbm, mot),
            (heat_hbm, heat),
            (diam_hbm, diam),
        )
    ):
        loads.append(pltpu.make_async_copy(source, land, local_sem.at[number]))
        loads[-1].start()

    barrier = pltpu.get_barrier_semaphore()
    for _, steps, _, _ in g_pos + g_y + g_z + g_yz:
        pl.when(there(steps))(
            lambda s=steps: pl.semaphore_signal(
                barrier, inc=1, device_id=peer(s), device_id_type=MESH
            )
        )

    for group in groups:
        blank(group)
    yb[:, 8:16] = jnp.zeros((NF, 8, CK), F32)
    yb[:, 24:128] = jnp.zeros((NF, 104, CK), F32)
    z_out[...] = jnp.zeros(z_out.shape, F32)
    dxy_out[...] = jnp.zeros(dxy_out.shape, F32)
    zt[...] = jnp.zeros(zt.shape, F32)
    s_hi[OWN + 32 : COLS] = jnp.zeros((96, n), BF16)
    s_lo[OWN + 32 : COLS] = jnp.zeros((96, n), BF16)
    t_hi[NS * CK + 16 :] = jnp.zeros((112, n), BF16)
    t_lo[NS * CK + 16 :] = jnp.zeros((112, n), BF16)

    for load in loads[0:4]:
        load.wait()
    at = [pos[axis : axis + 1] for axis in range(3)]
    cell = [ref[...].reshape(1, n).astype(F32) for ref in (li, lj, lk)]
    reach = [tent(at[0] - (place - cell[0])) for place in (-1.0, float(CI))]
    for x in range(2):
        for number, row in enumerate((reach[x], at[1], cell[1], at[2], cell[2])):
            pack(mine.at[x], number, row)

    near = {axis: jnp.minimum(me[axis], 1) + jnp.minimum(ends[axis] - me[axis], 1) for axis in axes}
    pl.semaphore_wait(barrier, near["gx"] + near["gy"] + near["gz"] + near["gy"] * near["gz"])
    send(g_pos)

    for load in loads[4:]:
        load.wait()
    for f in range(NF):
        for i in range(CI):
            y_out[0, f, i : i + 1, :] = fields[f, i, 0:1, :]
            y_out[1, f, i : i + 1, :] = fields[f, i, CJ - 1 : CJ, :]
    send(g_y)

    for f in range(NF):
        for b in range(OWN // 128):
            block = fields[f, 2 * b : 2 * b + 2].reshape(128, CK).T
            z_out[0, f : f + 1, b * 128 : b * 128 + 128] = block[0:1]
            z_out[1, f : f + 1, b * 128 : b * 128 + 128] = block[CK - 1 : CK]
            hi, lo = split(block)
            a_hi[f * CK : f * CK + CK, b * 128 : b * 128 + 128] = hi
            a_lo[f * CK : f * CK + CK, b * 128 : b * 128 + 128] = lo
    send(g_z)
    send(g_yz)

    def ramp(rows):
        return iota((rows, n), 0).astype(F32)

    row16 = iota((16, n), 0)

    def k_weights(x, offset, cell):
        hi, lo = split(tent(offset - (ramp(CK) - cell)))
        l_hi[x, 0:CK] = hi
        l_lo[x, 0:CK] = lo
        low, high = tent(offset - (-1.0 - cell)), tent(offset - (float(CK) - cell))
        hi, lo = split(jnp.where(row16 == 0, low, jnp.where(row16 == 8, high, 0.0)))
        l_hi[x, CK:] = hi
        l_lo[x, CK:] = lo
        return low, high

    wi[...] = jnp.where(row16 < CI, tent(at[0] - (ramp(16) - cell[0])), 0.0)
    wj = tent(at[1] - (ramp(CJ) - cell[1]))
    wj_ends = (tent(at[1] - (-1.0 - cell[1])), tent(at[1] - (float(CJ) - cell[1])))
    lines[...] = tent(at[2] - (ramp(CK) - cell[2]))
    line_ends[0:1], line_ends[1:2] = k_weights(2, at[2], cell[2])
    for i in range(CI):
        hi, lo = split(wi[i : i + 1] * wj)
        s_hi[i * CJ : i * CJ + CJ] = hi
        s_lo[i * CJ : i * CJ + CJ] = lo
    for y in range(2):
        hi, lo = split(wi[...] * wj_ends[y])
        s_hi[OWN + 16 * y : OWN + 16 * y + 16] = hi
        s_lo[OWN + 16 * y : OWN + 16 * y + 16] = lo
    for x in range(2):
        hi, lo = split(reach[x] * wj)
        x_hi[x * CJ : x * CJ + CJ] = hi
        x_lo[x * CJ : x * CJ + CJ] = lo
        for y in range(2):
            edges[2 * x + y : 2 * x + y + 1] = reach[x] * wj_ends[y]

    lane16 = iota((16, 128), 1)
    arrive(g_y)
    for f in range(NF):
        hi, lo = split(yb[f].T)
        a_hi[f * CK : f * CK + CK, OWN:COLS] = hi
        a_lo[f * CK : f * CK + CK, OWN:COLS] = lo
    arrive(g_z)
    hi, lo = split(z_in[...])
    a_hi[NF * CK : ROWS, 0:OWN] = hi
    a_lo[NF * CK : ROWS, 0:OWN] = lo
    arrive(g_yz)
    corner = jnp.zeros((16, 128), F32)
    for y in range(2):
        for i in range(CI):
            at = i * CJ + (CJ - 1 if y == 0 else 0)
            first = at // 128 * 128
            block = jnp.concatenate([yz_in[y, z, :, first : first + 128] for z in range(2)], axis=0)
            to = 16 * y + i
            moved = pltpu.roll(block, (to - at) % 128, 1)
            corner = jnp.where(lane16 == to, moved, corner)
    hi, lo = split(corner)
    a_hi[NF * CK : ROWS, OWN:COLS] = hi
    a_lo[NF * CK : ROWS, OWN:COLS] = lo

    def z_block(value):
        hi, lo = split(value)
        hi, lo = hi.astype(F32), lo.astype(F32)
        return (hi + pltpu.roll(hi, 16, 1) + pltpu.roll(lo, 32, 1)).astype(BF16)

    def put_plane(x, at, rows, value, ends_value):
        hi, lo = split(value)
        e_lhs[x, at : at + rows, 0:128] = hi
        e_lhs[x, at : at + rows, 128:256] = hi
        e_lhs[x, at : at + rows, 256:384] = lo
        e_lhs[x, at : at + rows, 384:512] = z_block(ends_value)

    lane64 = iota((CJ, 128), 1)
    lane8 = iota((8, 128), 1)
    for x in range(2):
        i = 0 if x == 0 else CI - 1
        first = i * CJ // 128 * 128
        columns = jnp.concatenate(
            [z_in[:, first : first + 128], jnp.zeros((112, 128), F32)], axis=0
        ).T
        columns = columns[0:CJ] if x == 0 else columns[CJ:128]
        for f in range(NF):
            moved = columns if f == 0 else pltpu.roll(columns, 128 - f, 1)
            moved = jnp.where((lane64 == 0) | (lane64 == 8), moved, 0.0)
            put_plane(x, f * CJ, CJ, fields[f, i], moved)
        values, moves = [], []
        for y in range(2):
            values += [yb[f, 16 * y + i : 16 * y + i + 1, :] for f in range(NF)]
            values.append(jnp.zeros((2, CK), F32))
            at = i * CJ + (CJ - 1 if y == 0 else 0)
            first = at // 128 * 128
            total = jnp.zeros((8, 128), F32)
            for z in range(2):
                block = pltpu.roll(yz_in[y, z, :, first : first + 128], (8 * z - at) % 128, 1)
                total = jnp.where(lane8 == 8 * z, block, total)
            moves.append(total)
        put_plane(
            x, NF * CJ, 16, jnp.concatenate(values, axis=0), jnp.concatenate(moves, axis=0)
        )

    chunks = [slice(c * 256, c * 256 + 256) for c in range(n // 256)]

    def gather(chunk):
        left = jnp.concatenate([a_hi[...], a_hi[...], a_lo[...]], axis=1)
        right = jnp.concatenate([s_hi[:, chunk], s_lo[:, chunk], s_hi[:, chunk]], axis=0)
        value = jnp.dot(left, right, preferred_element_type=F32)
        for f in range(NF):
            total = jnp.sum(value[f * CK : f * CK + CK] * lines[:, chunk], axis=0, keepdims=True)
            for z in range(2):
                row = NF * CK + 8 * z + f
                total = total + value[row : row + 1] * line_ends[z : z + 1, chunk]
            gathered[f : f + 1, chunk] = total

    for chunk in chunks[:2]:
        gather(chunk)

    arrive(g_pos)
    for x in range(2):
        near_x, at_j, cell_j, at_k, cell_k = [unpack(theirs.at[x], q) for q in range(5)]
        ws[x] = near_x * tent(at_j - (ramp(CJ) - cell_j))
        ws_ends[x, 0:1] = near_x * tent(at_j - (-1.0 - cell_j))
        ws_ends[x, 1:2] = near_x * tent(at_j - (float(CJ) - cell_j))
        k_weights(x, at_k, cell_k)
    for x in range(2):
        for chunk in chunks:
            top, low = l_hi[x, 0:CK, chunk], l_lo[x, 0:CK, chunk]
            top_z, low_z = l_hi[x, CK:, chunk], l_lo[x, CK:, chunk]
            right = jnp.concatenate(
                [top, low, top, top_z, low_z, top_z, jnp.zeros((80, 256), BF16)], axis=0
            )
            value = jnp.dot(e_lhs[x], right, preferred_element_type=F32)
            last = NF * CJ
            total = value[last : last + 8] * ws_ends[x, 0:1, chunk]
            total = total + value[last + 8 : last + 16] * ws_ends[x, 1:2, chunk]
            weight = ws[x, :, chunk]
            for f in range(NF):
                row = jnp.sum(value[f * CJ : f * CJ + CJ] * weight, axis=0, keepdims=True)
                row = row + total[f : f + 1]
                for b in range(2):
                    put = f * (n // 128) + chunk.start // 128 + b
                    part_out[x, put : put + 1, :] = row[:, b * 128 : b * 128 + 128]
    send(g_part)

    for chunk in chunks[2:]:
        gather(chunk)

    motion = mot[...]
    warmth = heat[...].reshape(1, n)
    q = diam[...].reshape(1, n)
    live = iota((1, n), 1) // TILE < tally[0]
    arrive(g_part)
    got = [
        gathered[f : f + 1] + unpack(part_in.at[0], f) + unpack(part_in.at[1], f)
        for f in range(NF)
    ]
    gas = jnp.concatenate(got[0:3], axis=0)
    gas_heat, moisture, rho = got[3:6]
    drag = step_time / (0.5 * q)
    new_motion = (motion + drag * gas) / (1.0 + drag)
    mass = q * jnp.sqrt(q)
    vapour = jnp.exp(4.0 * (warmth - 1.0))
    decay = step_time * evap_rate * rho * (vapour - moisture)
    new_q = q - decay
    new_mass = new_q * jnp.sqrt(new_q)
    conduction = step_time * heat_rate * rho / q
    new_heat = (warmth + conduction * gas_heat) / (1.0 + conduction) - (
        boiling_energy_drain * decay / q
    )
    state[0:3] = jnp.where(live, new_motion, motion)
    state[3:4] = jnp.where(live, new_heat, warmth)
    state[4:5] = jnp.where(live, new_q, q)
    terms_out[0:3] = jnp.where(live, mass * (motion - new_motion), 0.0)
    terms_out[3:4] = jnp.where(live, mass * (warmth - new_heat), 0.0)
    terms_out[4:5] = jnp.where(live, mass - new_mass, 0.0)
    terms_out[5:8] = jnp.zeros((3, n), F32)
    for c in range(NS):
        pack(terms_pack, c, terms_out[c : c + 1])
    send(d_terms)

    def cross(left, right):
        return lax.dot_general(
            left, right, (((1,), (1,)), ((), ())), preferred_element_type=F32
        )

    tail = jnp.concatenate(
        [terms_out[...] * line_ends[0:1], terms_out[...] * line_ends[1:2]], axis=0
    )
    hi, lo = split(tail)
    t_hi[NS * CK : NS * CK + 16] = hi
    t_lo[NS * CK : NS * CK + 16] = lo
    left = jnp.concatenate([x_hi[...], x_lo[...], x_hi[...]], axis=1)
    right = jnp.concatenate(
        [jnp.concatenate([hi, hi, lo], axis=1), jnp.zeros((112, 3 * n), BF16)], axis=0
    )
    dxz_out[...] = cross(left, right).T[0:16]
    hi, lo = split(
        jnp.concatenate([terms_out[...] * edges[line : line + 1] for line in range(4)], axis=0)
    )
    left = jnp.concatenate([hi, hi, lo], axis=1)
    right = jnp.concatenate([l_hi[2], l_lo[2], l_hi[2]], axis=1)
    value = cross(left, right)
    dxy_out[:, 0:128] = value[:, 0:CK]
    dxy_out[:, 128:144] = value[:, CK : CK + 16]
    send(d_xyz)
    send(d_xy)
    send(d_xz)

    for c in range(NS):
        hi, lo = split(terms_out[c : c + 1] * lines[...])
        t_hi[c * CK : c * CK + CK] = hi
        t_lo[c * CK : c * CK + CK] = lo

    lines_used = slice(0, OWN + 32)
    for w in range(3):
        column = slice(w * 256, w * 256 + 256)
        left = jnp.concatenate(
            [s_hi[lines_used], s_lo[lines_used], s_hi[lines_used]], axis=1
        )
        right = jnp.concatenate([t_hi[column], t_hi[column], t_lo[column]], axis=1)
        value = cross(left, right)
        for h in range(2):
            c = 2 * w + h
            half = value[:, h * 128 : h * 128 + 128]
            if c < NS:
                out[c] = half[0:OWN].reshape(CI, CJ, CK)
                dy[:, c * CK : c * CK + CK] = half[OWN : OWN + 32]
            else:
                for b in range(OWN // 128):
                    dz_out[:, b * 128 : b * 128 + 128] = half[b * 128 : b * 128 + 128].T[0:16]
                rest = jnp.concatenate([half[OWN : OWN + 32], jnp.zeros((96, 128), F32)], axis=0)
                dz_out[:, OWN:COLS] = rest.T[0:16]

    send(d_z)
    send(d_yz)
    send(d_y)

    arrive(d_terms)
    for x in range(2):
        i = 0 if x == 0 else CI - 1
        weight = ws[x]
        for c in range(NS):
            hi, lo = split(unpack(terms_in.at[x], c) * weight)
            u_hi[c * CJ : c * CJ + CJ] = hi
            u_lo[c * CJ : c * CJ + CJ] = lo
        left = jnp.concatenate([u_hi[...], u_hi[...], u_lo[...]], axis=1)
        right = jnp.concatenate([l_hi[x, 0:CK], l_lo[x, 0:CK], l_hi[x, 0:CK]], axis=1)
        value = cross(left, right)
        for c in range(NS):
            out[c, i] = out[c, i] + value[c * CJ : c * CJ + CJ]

    arrive(d_z)
    arrive(d_y)
    arrive(d_yz)
    arrive(d_xz)
    arrive(d_xy)
    arrive(d_xyz)
    lane128 = iota((128, 128), 1)
    rim = (lane128 == 0) | (lane128 == CK - 1)
    for b in range(OWN // 128):
        block = dz_in[:, b * 128 : b * 128 + 128]
        for i in (2 * b, 2 * b + 1):
            for y in range(2):
                to = i * CJ % 128 + (0 if y == 0 else CJ - 1)
                at = (16 if y == 0 else 0) + i
                moved = jnp.concatenate([dyz_in[y, 0], dyz_in[y, 1]], axis=0)
                moved = pltpu.roll(moved, (to - at) % 128, 1)
                block = block + jnp.where(lane16 == to, moved, 0.0)
        if b in (0, OWN // 128 - 1):
            x = 0 if b == 0 else 1
            moved = jnp.concatenate([dxz_in[x, 0], dxz_in[x, 1]], axis=0)
            half = lane16 < CJ if x == 0 else lane16 >= CJ
            block = block + jnp.where(half, pltpu.roll(moved, CJ, 1), 0.0)
            for y in range(2):
                to = CJ * x + (0 if y == 0 else CJ - 1)
                moved = jnp.concatenate(
                    [
                        pltpu.roll(dxyz_in[x, y, z], (to - 8 * (1 - z)) % 128, 1)
                        for z in range(2)
                    ],
                    axis=0,
                )
                block = block + jnp.where(lane16 == to, moved, 0.0)
        for c in range(NS):
            zt[b, 2 * c : 2 * c + 1] = block[8 + c : 9 + c]
            zt[b, 2 * c + 1 : 2 * c + 2] = block[c : c + 1]
        columns = jnp.concatenate([zt[b], jnp.zeros((112, 128), F32)], axis=0).T
        for c in range(NS):
            add = jnp.where(rim, pltpu.roll(columns, 127 - 2 * c, 1), 0.0)
            out[c, 2 * b : 2 * b + 2] = out[c, 2 * b : 2 * b + 2] + add.reshape(2, CJ, CK)
    for y in range(2):
        j = 0 if y == 0 else CJ - 1
        for c in range(NS):
            for i in range(CI):
                add = dy_in[y, i : i + 1, c * CK : c * CK + CK]
                if i in (0, CI - 1):
                    add = add + dxy_in[0 if i == 0 else 1, y, c : c + 1, :]
                out[c, i, j : j + 1, :] = out[c, i, j : j + 1, :] + add

    for group in groups:
        sent(group)


def local(sizes, vel, scal, pos, mot, heat, diam, li, lj, lk, tally):
    n = heat.shape[0]
    vmem = pl.BlockSpec(memory_space=pltpu.VMEM)
    hbm = pl.BlockSpec(memory_space=pltpu.HBM)
    planes = NF * CJ + 16
    return pl.pallas_call(
        functools.partial(kernel, sizes),
        out_shape=(
            jax.ShapeDtypeStruct((NS, CI, CJ, CK), F32),
            jax.ShapeDtypeStruct((NS, n), F32),
        ),
        in_specs=[hbm] * 9 + [pl.BlockSpec(memory_space=pltpu.SMEM)],
        out_specs=(vmem, vmem),
        scratch_shapes=[
            pltpu.VMEM((NF, CI, CJ, CK), F32),
            pltpu.VMEM((3, n), F32),
            pltpu.VMEM((3, n), F32),
            pltpu.VMEM((n,), F32),
            pltpu.VMEM((n,), F32),
            pltpu.VMEM((n,), jnp.int32),
            pltpu.VMEM((n,), jnp.int32),
            pltpu.VMEM((n,), jnp.int32),
            pltpu.VMEM((2, 5 * n // 128, 128), F32),
            pltpu.VMEM((2, 5 * n // 128, 128), F32),
            pltpu.VMEM((ROWS, COLS), BF16),
            pltpu.VMEM((ROWS, COLS), BF16),
            pltpu.VMEM((COLS, n), BF16),
            pltpu.VMEM((COLS, n), BF16),
            pltpu.VMEM((768, n), BF16),
            pltpu.VMEM((768, n), BF16),
            pltpu.VMEM((2, planes, 512), BF16),
            pltpu.VMEM((3, CK + 16, n), BF16),
            pltpu.VMEM((3, CK + 16, n), BF16),
            pltpu.VMEM((NS * CJ, n), BF16),
            pltpu.VMEM((NS * CJ, n), BF16),
            pltpu.VMEM((2 * CJ, n), BF16),
            pltpu.VMEM((2 * CJ, n), BF16),
            pltpu.VMEM((8, n), F32),
            pltpu.VMEM((2, CJ, n), F32),
            pltpu.VMEM((2, 8, n), F32),
            pltpu.VMEM((16, n), F32),
            pltpu.VMEM((CK, n), F32),
            pltpu.VMEM((8, n), F32),
            pltpu.VMEM((8, n), F32),
            pltpu.VMEM((2, NF * n // 128, 128), F32),
            pltpu.VMEM((2, NF * n // 128, 128), F32),
            pltpu.VMEM((8, n), F32),
            pltpu.VMEM((NS * n // 128, 128), F32),
            pltpu.VMEM((2, NS * n // 128, 128), F32),
            pltpu.VMEM((NF, 128, CK), F32),
            pltpu.VMEM((2, NF, 8, CK), F32),
            pltpu.VMEM((2, 8, OWN), F32),
            pltpu.VMEM((16, OWN), F32),
            pltpu.VMEM((2, 2, 8, OWN), F32),
            pltpu.VMEM((32, NS * CK), F32),
            pltpu.VMEM((2, 8, NS * CK), F32),
            pltpu.VMEM((16, COLS), F32),
            pltpu.VMEM((16, OWN), F32),
            pltpu.VMEM((2, 2, 8, 128), F32),
            pltpu.VMEM((16, 128), F32),
            pltpu.VMEM((2, 2, 8, 128), F32),
            pltpu.VMEM((32, 256), F32),
            pltpu.VMEM((2, 2, 8, 128), F32),
            pltpu.VMEM((2, 2, 2, 8, 128), F32),
            pltpu.VMEM((OWN // 128, 16, 128), F32),
            pltpu.SemaphoreType.DMA((9,)),
            pltpu.SemaphoreType.DMA((38,)),
            pltpu.SemaphoreType.DMA((38,)),
        ],
        compiler_params=pltpu.CompilerParams(
            collective_id=0, has_side_effects=True, vmem_limit_bytes=32 * 1024 * 1024
        ),
    )(*(pltpu.with_memory_space_constraint(x, pltpu.HBM) for x in (vel, scal, pos, mot, heat, diam, li, lj, lk)), tally)


def solution(mesh):
    sizes = {axis: mesh.shape[axis] for axis in ("gx", "gy", "gz")}
    flat = P(("gx", "gy", "gz"))
    wide = P(None, ("gx", "gy", "gz"))
    grid = P(None, "gx", "gy", "gz")
    return jax.shard_map(
        functools.partial(local, sizes),
        mesh=mesh,
        in_specs=(grid, grid, wide, wide) + (flat,) * 6,
        out_specs=(grid, wide),
        check_vma=False,
    )
```

```python
import functools
import itertools

import jax
import jax.numpy as jnp
from jax import lax
from jax.experimental import pallas as pl
from jax.experimental.pallas import tpu as pltpu
from jax.sharding import PartitionSpec as P

TILE = 128
NF = 6
NS = 5
CI, CJ, CK = 8, 64, 128
OWN = CI * CJ
COLS = OWN + 128
ROWS = NF * CK + 16
MESH = pl.DeviceIdType.MESH
F32 = jnp.float32
BF16 = jnp.bfloat16

step_time = 0.25
evap_rate = 1.0
heat_rate = 2.0
boiling_energy_drain = 0.3


def split(x):
    hi = x.astype(BF16)
    return hi, (x - hi.astype(F32)).astype(BF16)


def tent(offset):
    return jnp.maximum(0.0, 1.0 - jnp.abs(offset))


def iota(shape, dim):
    return lax.broadcasted_iota(jnp.int32, shape, dim)


def kernel(
    sizes,
    vel,
    scal,
    pos_hbm,
    mot_hbm,
    heat_hbm,
    diam_hbm,
    li_hbm,
    lj_hbm,
    lk_hbm,
    tally,
    out,
    state,
    zt,
    rows,
    fields,
    pos,
    mot,
    heat,
    diam,
    li,
    lj,
    lk,
    mine,
    theirs,
    a_hi,
    a_lo,
    s_hi,
    s_lo,
    t_hi,
    t_lo,
    e_lhs,
    l_hi,
    l_lo,
    u_hi,
    u_lo,
    x_hi,
    x_lo,
    edges,
    ws,
    ws_ends,
    wi,
    lines,
    line_ends,
    gathered,
    part_out,
    part_in,
    terms_out,
    terms_pack,
    terms_in,
    yb,
    y_out,
    z_out,
    z_in,
    yz_in,
    dy,
    dy_in,
    dz_out,
    dz_in,
    dyz_in,
    dxz_out,
    dxz_in,
    dxy_out,
    dxy_in,
    dxyz_in,
    local_sem,
    send_sem,
    recv_sem,
):
    n = pos.shape[1]
    axes = tuple(sizes)
    me = {axis: lax.axis_index(axis) for axis in axes}
    ends = {axis: size - 1 for axis, size in sizes.items()}

    def there(steps):
        found = None
        for axis, step in steps:
            one = me[axis] < ends[axis] if step > 0 else me[axis] > 0
            found = one if found is None else jnp.logical_and(found, one)
        return found

    def peer(steps):
        return {axis: me[axis] + step for axis, step in steps}

    def back(steps):
        return tuple((axis, -step) for axis, step in steps)

    numbers = iter(range(64))

    def pack(ref, number, row):
        for b in range(n // 128):
            at = number * (n // 128) + b
            ref[at : at + 1, :] = row[:, b * 128 : b * 128 + 128]

    def unpack(ref, number):
        first = number * (n // 128)
        return jnp.concatenate([ref[first + b : first + b + 1, :] for b in range(n // 128)], axis=1)

    def both(axis, up, land0, down, land1):
        return (
            (next(numbers), ((axis, 1),), up, land0),
            (next(numbers), ((axis, -1),), down, land1),
        )

    def diagonal(axes, source, land):
        found = []
        for steps in itertools.product((1, -1), repeat=len(axes)):
            sides = tuple((1 - step) // 2 for step in steps)
            from_sides = tuple(1 - side for side in sides)
            steps = tuple(zip(axes, steps))
            found.append((next(numbers), steps, source(*from_sides), land.at[sides]))
        return tuple(found)

    def copy(transfer, steps):
        number, _, source, land = transfer
        return pltpu.make_async_remote_copy(
            src_ref=source,
            dst_ref=land,
            send_sem=send_sem.at[number],
            recv_sem=recv_sem.at[number],
            device_id=peer(steps),
            device_id_type=MESH,
        )

    def send(group):
        for transfer in group:
            pl.when(there(transfer[1]))(lambda t=transfer: copy(t, t[1]).start())

    def arrive(group):
        for transfer in group:
            steps = back(transfer[1])
            pl.when(there(steps))(lambda t=transfer, s=steps: copy(t, s).wait_recv())

    def sent(group):
        for transfer in group:
            pl.when(there(transfer[1]))(lambda t=transfer: copy(t, t[1]).wait_send())

    def blank(group):
        for _, steps, _, land in group:

            @pl.when(jnp.logical_not(there(back(steps))))
            def _():
                land[...] = jnp.zeros(land.shape, F32)

    g_pos = both("gx", mine.at[1], theirs.at[0], mine.at[0], theirs.at[1])
    g_y = both("gy", y_out.at[1], yb.at[:, 0:8], y_out.at[0], yb.at[:, 16:24])
    g_z = both("gz", z_out.at[1], z_in.at[0:8], z_out.at[0], z_in.at[8:16])
    g_yz = diagonal(("gy", "gz"), lambda y, z: z_out.at[z], yz_in)
    g_part = both("gx", part_out.at[1], part_in.at[0], part_out.at[0], part_in.at[1])
    d_terms = both("gx", terms_pack, terms_in.at[0], terms_pack, terms_in.at[1])
    d_z = both(
        "gz",
        dz_out.at[8:16, 0:OWN],
        dz_in.at[0:8],
        dz_out.at[0:8, 0:OWN],
        dz_in.at[8:16],
    )
    d_y = both("gy", dy.at[16:24], dy_in.at[0], dy.at[0:8], dy_in.at[1])
    d_yz = diagonal(
        ("gy", "gz"), lambda y, z: dz_out.at[8 * z : 8 * z + 8, OWN:COLS], dyz_in
    )
    d_xz = diagonal(("gx", "gz"), lambda x, z: dxz_out.at[8 * z : 8 * z + 8], dxz_in)

    def edge(x, y):
        first = 16 * x + 8 * y
        return slice(first, first + 8)

    d_xy = diagonal(("gx", "gy"), lambda x, y: dxy_out.at[edge(x, y), 0:128], dxy_in)
    d_xyz = diagonal(
        ("gx", "gy", "gz"), lambda x, y, z: dxy_out.at[edge(x, y), 128:256], dxyz_in
    )
    groups = (g_pos, g_y, g_z, g_yz, g_part, d_terms, d_xz, d_xy, d_xyz, d_z, d_y, d_yz)

    barrier = pltpu.get_barrier_semaphore()
    for _, steps, _, _ in g_pos + g_y + g_z + g_yz:
        pl.when(there(steps))(
            lambda s=steps: pl.semaphore_signal(
                barrier, inc=1, device_id=peer(s), device_id_type=MESH
            )
        )

    loads = []
    for number, (source, land) in enumerate(
        (
            (pos_hbm, pos),
            (li_hbm, li),
            (lj_hbm, lj),
            (lk_hbm, lk),
            (vel, fields.at[0:3]),
            (scal, fields.at[3:6]),
            (mot_hbm, mot),
            (heat_hbm, heat),
            (diam_hbm, diam),
        )
    ):
        loads.append(pltpu.make_async_copy(source, land, local_sem.at[number]))
        loads[-1].start()

    for group in groups:
        blank(group)
    yb[:, 8:16] = jnp.zeros((NF, 8, CK), F32)
    yb[:, 24:128] = jnp.zeros((NF, 104, CK), F32)
    z_out[...] = jnp.zeros(z_out.shape, F32)
    dxy_out[...] = jnp.zeros(dxy_out.shape, F32)
    zt[:, 10:16] = jnp.zeros((OWN // 128, 6, 128), F32)
    s_hi[OWN + 32 : COLS] = jnp.zeros((96, n), BF16)
    s_lo[OWN + 32 : COLS] = jnp.zeros((96, n), BF16)
    t_hi[NS * CK + 16 :] = jnp.zeros((112, n), BF16)
    t_lo[NS * CK + 16 :] = jnp.zeros((112, n), BF16)

    for load in loads[0:4]:
        load.wait()
    at = [pos[axis : axis + 1] for axis in range(3)]
    cell = [ref[...].reshape(1, n).astype(F32) for ref in (li, lj, lk)]
    reach = [tent(at[0] - (place - cell[0])) for place in (-1.0, float(CI))]
    for x in range(2):
        for number, row in enumerate((reach[x], at[1], cell[1], at[2], cell[2])):
            pack(mine.at[x], number, row)

    for load in loads[4:]:
        load.wait()
    for f in range(NF):
        for i in range(CI):
            y_out[0, f, i : i + 1, :] = fields[f, i, 0:1, :]
            y_out[1, f, i : i + 1, :] = fields[f, i, CJ - 1 : CJ, :]
    for f in range(NF):
        for b in range(OWN // 128):
            block = fields[f, 2 * b : 2 * b + 2].reshape(128, CK).T
            z_out[0, f : f + 1, b * 128 : b * 128 + 128] = block[0:1]
            z_out[1, f : f + 1, b * 128 : b * 128 + 128] = block[CK - 1 : CK]
            hi, lo = split(block)
            a_hi[f * CK : f * CK + CK, b * 128 : b * 128 + 128] = hi
            a_lo[f * CK : f * CK + CK, b * 128 : b * 128 + 128] = lo
    near = {axis: jnp.minimum(me[axis], 1) + jnp.minimum(ends[axis] - me[axis], 1) for axis in axes}
    pl.semaphore_wait(barrier, near["gx"] + near["gy"] + near["gz"] + near["gy"] * near["gz"])
    send(g_pos)

    send(g_y)
    send(g_z)
    send(g_yz)

    def ramp(rows):
        return iota((rows, n), 0).astype(F32)

    row16 = iota((16, n), 0)

    def k_weights(x, offset, cell):
        hi, lo = split(tent(offset - (ramp(CK) - cell)))
        l_hi[x, 0:CK] = hi
        l_lo[x, 0:CK] = lo
        low, high = tent(offset - (-1.0 - cell)), tent(offset - (float(CK) - cell))
        hi, lo = split(jnp.where(row16 == 0, low, jnp.where(row16 == 8, high, 0.0)))
        l_hi[x, CK:] = hi
        l_lo[x, CK:] = lo
        return low, high

    wi[...] = jnp.where(row16 < CI, tent(at[0] - (ramp(16) - cell[0])), 0.0)
    wj = tent(at[1] - (ramp(CJ) - cell[1]))
    wj_ends = (tent(at[1] - (-1.0 - cell[1])), tent(at[1] - (float(CJ) - cell[1])))
    lines[...] = tent(at[2] - (ramp(CK) - cell[2]))
    line_ends[0:1], line_ends[1:2] = k_weights(2, at[2], cell[2])
    for i in range(CI):
        hi, lo = split(wi[i : i + 1] * wj)
        s_hi[i * CJ : i * CJ + CJ] = hi
        s_lo[i * CJ : i * CJ + CJ] = lo
    for y in range(2):
        hi, lo = split(wi[...] * wj_ends[y])
        s_hi[OWN + 16 * y : OWN + 16 * y + 16] = hi
        s_lo[OWN + 16 * y : OWN + 16 * y + 16] = lo
    for x in range(2):
        hi, lo = split(reach[x] * wj)
        x_hi[x * CJ : x * CJ + CJ] = hi
        x_lo[x * CJ : x * CJ + CJ] = lo
        for y in range(2):
            edges[2 * x + y : 2 * x + y + 1] = reach[x] * wj_ends[y]

    lane16 = iota((16, 128), 1)
    arrive(g_y)
    for f in range(NF):
        hi, lo = split(yb[f].T)
        a_hi[f * CK : f * CK + CK, OWN:COLS] = hi
        a_lo[f * CK : f * CK + CK, OWN:COLS] = lo
    arrive(g_z)
    hi, lo = split(z_in[...])
    a_hi[NF * CK : ROWS, 0:OWN] = hi
    a_lo[NF * CK : ROWS, 0:OWN] = lo
    arrive(g_yz)
    corner = jnp.zeros((16, 128), F32)
    for y in range(2):
        for i in range(CI):
            at = i * CJ + (CJ - 1 if y == 0 else 0)
            first = at // 128 * 128
            block = jnp.concatenate([yz_in[y, z, :, first : first + 128] for z in range(2)], axis=0)
            to = 16 * y + i
            moved = pltpu.roll(block, (to - at) % 128, 1)
            corner = jnp.where(lane16 == to, moved, corner)
    hi, lo = split(corner)
    a_hi[NF * CK : ROWS, OWN:COLS] = hi
    a_lo[NF * CK : ROWS, OWN:COLS] = lo

    def z_block(value):
        hi, lo = split(value)
        hi, lo = hi.astype(F32), lo.astype(F32)
        return (hi + pltpu.roll(hi, 16, 1) + pltpu.roll(lo, 32, 1)).astype(BF16)

    def put_plane(x, at, rows, value, ends_value):
        hi, lo = split(value)
        e_lhs[x, at : at + rows, 0:128] = hi
        e_lhs[x, at : at + rows, 128:256] = hi
        e_lhs[x, at : at + rows, 256:384] = lo
        e_lhs[x, at : at + rows, 384:512] = z_block(ends_value)

    lane64 = iota((CJ, 128), 1)
    lane8 = iota((8, 128), 1)
    for x in range(2):
        i = 0 if x == 0 else CI - 1
        first = i * CJ // 128 * 128
        columns = jnp.concatenate(
            [z_in[:, first : first + 128], jnp.zeros((112, 128), F32)], axis=0
        ).T
        columns = columns[0:CJ] if x == 0 else columns[CJ:128]
        for f in range(NF):
            moved = columns if f == 0 else pltpu.roll(columns, 128 - f, 1)
            moved = jnp.where((lane64 == 0) | (lane64 == 8), moved, 0.0)
            put_plane(x, f * CJ, CJ, fields[f, i], moved)
        values, moves = [], []
        for y in range(2):
            values += [yb[f, 16 * y + i : 16 * y + i + 1, :] for f in range(NF)]
            values.append(jnp.zeros((2, CK), F32))
            at = i * CJ + (CJ - 1 if y == 0 else 0)
            first = at // 128 * 128
            total = jnp.zeros((8, 128), F32)
            for z in range(2):
                block = pltpu.roll(yz_in[y, z, :, first : first + 128], (8 * z - at) % 128, 1)
                total = jnp.where(lane8 == 8 * z, block, total)
            moves.append(total)
        put_plane(
            x, NF * CJ, 16, jnp.concatenate(values, axis=0), jnp.concatenate(moves, axis=0)
        )

    chunks = [slice(c * 256, c * 256 + 256) for c in range(n // 256)]

    def gather(chunk):
        left = jnp.concatenate([a_hi[...], a_hi[...], a_lo[...]], axis=1)
        right = jnp.concatenate([s_hi[:, chunk], s_lo[:, chunk], s_hi[:, chunk]], axis=0)
        value = jnp.dot(left, right, preferred_element_type=F32)
        for f in range(NF):
            total = jnp.sum(value[f * CK : f * CK + CK] * lines[:, chunk], axis=0, keepdims=True)
            for z in range(2):
                row = NF * CK + 8 * z + f
                total = total + value[row : row + 1] * line_ends[z : z + 1, chunk]
            gathered[f : f + 1, chunk] = total

    for chunk in chunks[:2]:
        gather(chunk)

    arrive(g_pos)
    for x in range(2):
        near_x, at_j, cell_j, at_k, cell_k = [unpack(theirs.at[x], q) for q in range(5)]
        ws[x] = near_x * tent(at_j - (ramp(CJ) - cell_j))
        ws_ends[x, 0:1] = near_x * tent(at_j - (-1.0 - cell_j))
        ws_ends[x, 1:2] = near_x * tent(at_j - (float(CJ) - cell_j))
        k_weights(x, at_k, cell_k)
    for x in range(2):
        for chunk in chunks:
            top, low = l_hi[x, 0:CK, chunk], l_lo[x, 0:CK, chunk]
            top_z, low_z = l_hi[x, CK:, chunk], l_lo[x, CK:, chunk]
            right = jnp.concatenate(
                [top, low, top, top_z, low_z, top_z, jnp.zeros((80, 256), BF16)], axis=0
            )
            value = jnp.dot(e_lhs[x], right, preferred_element_type=F32)
            last = NF * CJ
            total = value[last : last + 8] * ws_ends[x, 0:1, chunk]
            total = total + value[last + 8 : last + 16] * ws_ends[x, 1:2, chunk]
            weight = ws[x, :, chunk]
            for f in range(NF):
                row = jnp.sum(value[f * CJ : f * CJ + CJ] * weight, axis=0, keepdims=True)
                row = row + total[f : f + 1]
                for b in range(2):
                    put = f * (n // 128) + chunk.start // 128 + b
                    part_out[x, put : put + 1, :] = row[:, b * 128 : b * 128 + 128]
    send(g_part)

    for chunk in chunks[2:]:
        gather(chunk)

    motion = mot[...]
    warmth = heat[...].reshape(1, n)
    q = diam[...].reshape(1, n)
    live = iota((1, n), 1) // TILE < tally[0]
    arrive(g_part)
    got = [
        gathered[f : f + 1] + unpack(part_in.at[0], f) + unpack(part_in.at[1], f)
        for f in range(NF)
    ]
    gas = jnp.concatenate(got[0:3], axis=0)
    gas_heat, moisture, rho = got[3:6]
    drag = step_time / (0.5 * q)
    new_motion = (motion + drag * gas) / (1.0 + drag)
    mass = q * jnp.sqrt(q)
    vapour = jnp.exp(4.0 * (warmth - 1.0))
    decay = step_time * evap_rate * rho * (vapour - moisture)
    new_q = q - decay
    new_mass = new_q * jnp.sqrt(new_q)
    conduction = step_time * heat_rate * rho / q
    new_heat = (warmth + conduction * gas_heat) / (1.0 + conduction) - (
        boiling_energy_drain * decay / q
    )
    state[0:3] = jnp.where(live, new_motion, motion)
    state[3:4] = jnp.where(live, new_heat, warmth)
    state[4:5] = jnp.where(live, new_q, q)
    terms_out[0:3] = jnp.where(live, mass * (motion - new_motion), 0.0)
    terms_out[3:4] = jnp.where(live, mass * (warmth - new_heat), 0.0)
    terms_out[4:5] = jnp.where(live, mass - new_mass, 0.0)
    terms_out[5:8] = jnp.zeros((3, n), F32)
    for c in range(NS):
        pack(terms_pack, c, terms_out[c : c + 1])
    send(d_terms)

    def cross(left, right):
        return lax.dot_general(
            left, right, (((1,), (1,)), ((), ())), preferred_element_type=F32
        )

    tail = jnp.concatenate(
        [terms_out[...] * line_ends[0:1], terms_out[...] * line_ends[1:2]], axis=0
    )
    hi, lo = split(tail)
    t_hi[NS * CK : NS * CK + 16] = hi
    t_lo[NS * CK : NS * CK + 16] = lo
    left = jnp.concatenate([x_hi[...], x_lo[...], x_hi[...]], axis=1)
    right = jnp.concatenate(
        [jnp.concatenate([hi, hi, lo], axis=1), jnp.zeros((112, 3 * n), BF16)], axis=0
    )
    dxz_out[...] = cross(left, right).T[0:16]
    hi, lo = split(
        jnp.concatenate([terms_out[...] * edges[line : line + 1] for line in range(4)], axis=0)
    )
    left = jnp.concatenate([hi, hi, lo], axis=1)
    right = jnp.concatenate([l_hi[2], l_lo[2], l_hi[2]], axis=1)
    value = cross(left, right)
    dxy_out[:, 0:128] = value[:, 0:CK]
    dxy_out[:, 128:144] = value[:, CK : CK + 16]
    send(d_xyz)
    send(d_xy)
    send(d_xz)

    for c in range(NS):
        hi, lo = split(terms_out[c : c + 1] * lines[...])
        t_hi[c * CK : c * CK + CK] = hi
        t_lo[c * CK : c * CK + CK] = lo

    lines_used = slice(0, OWN + 32)
    for w in range(3):
        column = slice(w * 256, w * 256 + 256)
        left = jnp.concatenate(
            [s_hi[lines_used], s_lo[lines_used], s_hi[lines_used]], axis=1
        )
        right = jnp.concatenate([t_hi[column], t_hi[column], t_lo[column]], axis=1)
        value = cross(left, right)
        for h in range(2):
            c = 2 * w + h
            half = value[:, h * 128 : h * 128 + 128]
            if c < NS:
                out[c] = half[0:OWN].reshape(CI, CJ, CK)
                dy[:, c * CK : c * CK + CK] = half[OWN : OWN + 32]
            else:
                for b in range(OWN // 128):
                    dz_out[:, b * 128 : b * 128 + 128] = half[b * 128 : b * 128 + 128].T[0:16]
                rest = jnp.concatenate([half[OWN : OWN + 32], jnp.zeros((96, 128), F32)], axis=0)
                dz_out[:, OWN:COLS] = rest.T[0:16]

    send(d_z)
    send(d_yz)
    send(d_y)

    for group in (g_pos, g_y, g_z, g_yz, g_part):
        sent(group)
    arrive(d_terms)
    for x in range(2):
        i = 0 if x == 0 else CI - 1
        weight = ws[x]
        for c in range(NS):
            hi, lo = split(unpack(terms_in.at[x], c) * weight)
            u_hi[x, c * CJ : c * CJ + CJ] = hi
            u_lo[x, c * CJ : c * CJ + CJ] = lo
        left = jnp.concatenate([u_hi[x], u_hi[x], u_lo[x]], axis=1)
        right = jnp.concatenate([l_hi[x, 0:CK], l_lo[x, 0:CK], l_hi[x, 0:CK]], axis=1)
        value = cross(left, right)
        for c in range(NS):
            out[c, i] = out[c, i] + value[c * CJ : c * CJ + CJ]

    for group in (d_terms, d_xz, d_xy, d_xyz):
        sent(group)
    arrive(d_z)
    arrive(d_y)
    arrive(d_yz)
    arrive(d_xz)
    arrive(d_xy)
    arrive(d_xyz)
    for b in range(OWN // 128):
        block = dz_in[:, b * 128 : b * 128 + 128]
        for i in (2 * b, 2 * b + 1):
            for y in range(2):
                to = i * CJ % 128 + (0 if y == 0 else CJ - 1)
                at = (16 if y == 0 else 0) + i
                moved = jnp.concatenate([dyz_in[y, 0], dyz_in[y, 1]], axis=0)
                moved = pltpu.roll(moved, (to - at) % 128, 1)
                block = block + jnp.where(lane16 == to, moved, 0.0)
        if b in (0, OWN // 128 - 1):
            x = 0 if b == 0 else 1
            moved = jnp.concatenate([dxz_in[x, 0], dxz_in[x, 1]], axis=0)
            half = lane16 < CJ if x == 0 else lane16 >= CJ
            block = block + jnp.where(half, pltpu.roll(moved, CJ, 1), 0.0)
            for y in range(2):
                to = CJ * x + (0 if y == 0 else CJ - 1)
                moved = jnp.concatenate(
                    [
                        pltpu.roll(dxyz_in[x, y, z], (to - 8 * (1 - z)) % 128, 1)
                        for z in range(2)
                    ],
                    axis=0,
                )
                block = block + jnp.where(lane16 == to, moved, 0.0)
        for c in range(NS):
            zt[b, 2 * c : 2 * c + 1] = block[8 + c : 9 + c]
            zt[b, 2 * c + 1 : 2 * c + 2] = block[c : c + 1]
    rows[...] = dy_in[...]
    for x in range(2):
        i = 0 if x == 0 else CI - 1
        for y in range(2):
            for c in range(NS):
                at = slice(c * CK, c * CK + CK)
                rows[y, i : i + 1, at] = rows[y, i : i + 1, at] + dxy_in[x, y, c : c + 1, :]

    for group in (d_z, d_y, d_yz):
        sent(group)


def deliver(part, state, zt, rows, out, state_out, whole, sem):
    state_copy = pltpu.make_async_copy(state, state_out, sem.at[NS])
    state_copy.start()
    lane = iota((128, 128), 1)
    rim = (lane == 0) | (lane == CK - 1)
    blocks = range(OWN // 128)
    columns = [
        jnp.concatenate([zt[b], jnp.zeros((112, 128), F32)], axis=0).T for b in blocks
    ]
    copies = []
    for c in range(NS):
        for b in blocks:
            add = jnp.where(rim, pltpu.roll(columns[b], 127 - 2 * c, 1), 0.0)
            whole[c, 2 * b : 2 * b + 2] = part[c, 2 * b : 2 * b + 2] + add.reshape(2, CJ, CK)
        for y in range(2):
            j = 0 if y == 0 else CJ - 1
            for i in range(CI):
                whole[c, i, j : j + 1, :] = (
                    whole[c, i, j : j + 1, :] + rows[y, i : i + 1, c * CK : c * CK + CK]
                )
        copies.append(pltpu.make_async_copy(whole.at[c], out.at[c], sem.at[c]))
        copies[-1].start()
    for copy in copies + [state_copy]:
        copy.wait()


def local(sizes, vel, scal, pos, mot, heat, diam, li, lj, lk, tally):
    n = heat.shape[0]
    vmem = pl.BlockSpec(memory_space=pltpu.VMEM)
    hbm = pl.BlockSpec(memory_space=pltpu.HBM)
    planes = NF * CJ + 16
    parts = pl.pallas_call(
        functools.partial(kernel, sizes),
        out_shape=(
            jax.ShapeDtypeStruct((NS, CI, CJ, CK), F32),
            jax.ShapeDtypeStruct((NS, n), F32),
            jax.ShapeDtypeStruct((OWN // 128, 16, 128), F32),
            jax.ShapeDtypeStruct((2, 8, NS * CK), F32),
        ),
        in_specs=[hbm] * 9 + [pl.BlockSpec(memory_space=pltpu.SMEM)],
        out_specs=(vmem,) * 4,
        scratch_shapes=[
            pltpu.VMEM((NF, CI, CJ, CK), F32),
            pltpu.VMEM((3, n), F32),
            pltpu.VMEM((3, n), F32),
            pltpu.VMEM((n,), F32),
            pltpu.VMEM((n,), F32),
            pltpu.VMEM((n,), jnp.int32),
            pltpu.VMEM((n,), jnp.int32),
            pltpu.VMEM((n,), jnp.int32),
            pltpu.VMEM((2, 5 * n // 128, 128), F32),
            pltpu.VMEM((2, 5 * n // 128, 128), F32),
            pltpu.VMEM((ROWS, COLS), BF16),
            pltpu.VMEM((ROWS, COLS), BF16),
            pltpu.VMEM((COLS, n), BF16),
            pltpu.VMEM((COLS, n), BF16),
            pltpu.VMEM((768, n), BF16),
            pltpu.VMEM((768, n), BF16),
            pltpu.VMEM((2, planes, 512), BF16),
            pltpu.VMEM((3, CK + 16, n), BF16),
            pltpu.VMEM((3, CK + 16, n), BF16),
            pltpu.VMEM((2, NS * CJ, n), BF16),
            pltpu.VMEM((2, NS * CJ, n), BF16),
            pltpu.VMEM((2 * CJ, n), BF16),
            pltpu.VMEM((2 * CJ, n), BF16),
            pltpu.VMEM((8, n), F32),
            pltpu.VMEM((2, CJ, n), F32),
            pltpu.VMEM((2, 8, n), F32),
            pltpu.VMEM((16, n), F32),
            pltpu.VMEM((CK, n), F32),
            pltpu.VMEM((8, n), F32),
            pltpu.VMEM((8, n), F32),
            pltpu.VMEM((2, NF * n // 128, 128), F32),
            pltpu.VMEM((2, NF * n // 128, 128), F32),
            pltpu.VMEM((8, n), F32),
            pltpu.VMEM((NS * n // 128, 128), F32),
            pltpu.VMEM((2, NS * n // 128, 128), F32),
            pltpu.VMEM((NF, 128, CK), F32),
            pltpu.VMEM((2, NF, 8, CK), F32),
            pltpu.VMEM((2, 8, OWN), F32),
            pltpu.VMEM((16, OWN), F32),
            pltpu.VMEM((2, 2, 8, OWN), F32),
            pltpu.VMEM((32, NS * CK), F32),
            pltpu.VMEM((2, 8, NS * CK), F32),
            pltpu.VMEM((16, COLS), F32),
            pltpu.VMEM((16, OWN), F32),
            pltpu.VMEM((2, 2, 8, 128), F32),
            pltpu.VMEM((16, 128), F32),
            pltpu.VMEM((2, 2, 8, 128), F32),
            pltpu.VMEM((32, 256), F32),
            pltpu.VMEM((2, 2, 8, 128), F32),
            pltpu.VMEM((2, 2, 2, 8, 128), F32),
            pltpu.SemaphoreType.DMA((9,)),
            pltpu.SemaphoreType.DMA((38,)),
            pltpu.SemaphoreType.DMA((38,)),
        ],
        compiler_params=pltpu.CompilerParams(
            collective_id=0, has_side_effects=True, vmem_limit_bytes=32 * 1024 * 1024
        ),
    )(*(pltpu.with_memory_space_constraint(x, pltpu.HBM) for x in (vel, scal, pos, mot, heat, diam, li, lj, lk)), tally)
    return pl.pallas_call(
        deliver,
        out_shape=tuple(jax.ShapeDtypeStruct(part.shape, F32) for part in parts[:2]),
        in_specs=[vmem] * 4,
        out_specs=(hbm, hbm),
        scratch_shapes=[
            pltpu.VMEM((NS, CI, CJ, CK), F32),
            pltpu.SemaphoreType.DMA((NS + 1,)),
        ],
        compiler_params=pltpu.CompilerParams(vmem_limit_bytes=4 * 1024 * 1024),
    )(*parts)


def solution(mesh):
    sizes = {axis: mesh.shape[axis] for axis in ("gx", "gy", "gz")}
    flat = P(("gx", "gy", "gz"))
    wide = P(None, ("gx", "gy", "gz"))
    grid = P(None, "gx", "gy", "gz")
    return jax.shard_map(
        functools.partial(local, sizes),
        mesh=mesh,
        in_specs=(grid, grid, wide, wide) + (flat,) * 6,
        out_specs=(grid, wide),
        check_vma=False,
    )
```

```python
import functools
import itertools

import jax
import jax.numpy as jnp
from jax import lax
from jax.experimental import pallas as pl
from jax.experimental.pallas import tpu as pltpu
from jax.sharding import PartitionSpec as P

TILE = 128
NF = 6
NS = 5
CI, CJ, CK = 8, 64, 128
OWN = CI * CJ
COLS = OWN + 128
ROWS = NF * CK + 16
PARTS = 1
MESH = pl.DeviceIdType.MESH
F32 = jnp.float32
BF16 = jnp.bfloat16

step_time = 0.25
evap_rate = 1.0
heat_rate = 2.0
boiling_energy_drain = 0.3


def split(x):
    hi = x.astype(BF16)
    return hi, (x - hi.astype(F32)).astype(BF16)


def tent(offset):
    return jnp.maximum(0.0, 1.0 - jnp.abs(offset))


def iota(shape, dim):
    return lax.broadcasted_iota(jnp.int32, shape, dim)


def kernel(
    sizes,
    vel,
    scal,
    pos_hbm,
    mot_hbm,
    heat_hbm,
    diam_hbm,
    li_hbm,
    lj_hbm,
    lk_hbm,
    tally,
    out,
    state,
    zt,
    rows,
    fields,
    pos,
    mot,
    heat,
    diam,
    li,
    lj,
    lk,
    mine,
    theirs,
    a_hi,
    a_lo,
    s_hi,
    s_lo,
    e_lhs,
    l_hi,
    l_lo,
    x_hi,
    x_lo,
    edges,
    ws,
    ws_ends,
    wi,
    lines,
    line_ends,
    gathered,
    part_out,
    part_in,
    terms_out,
    terms_pack,
    terms_in,
    yb,
    y_out,
    z_out,
    z_in,
    yz_in,
    dy,
    dy_in,
    dz_out,
    dz_in,
    dyz_in,
    dxz_out,
    dxz_in,
    dxy_out,
    dxy_in,
    dxyz_in,
    send_sem,
    recv_sem,
):
    n = pos.shape[1]
    width = n // PARTS
    parts = [slice(h * width, h * width + width) for h in range(PARTS)]
    per_row = width // 128
    axes = tuple(sizes)
    me = {axis: lax.axis_index(axis) for axis in axes}
    ends = {axis: size - 1 for axis, size in sizes.items()}

    def there(steps):
        found = None
        for axis, step in steps:
            one = me[axis] < ends[axis] if step > 0 else me[axis] > 0
            found = one if found is None else jnp.logical_and(found, one)
        return found

    def peer(steps):
        return {axis: me[axis] + step for axis, step in steps}

    def back(steps):
        return tuple((axis, -step) for axis, step in steps)

    numbers = iter(range(64))

    def pack(ref, number, row, first=0):
        for b in range(row.shape[1] // 128):
            at = number * per_row + first + b
            ref[at : at + 1, :] = row[:, b * 128 : b * 128 + 128]

    def unpack(ref, number):
        first = number * per_row
        return jnp.concatenate([ref[first + b : first + b + 1, :] for b in range(per_row)], axis=1)

    def numbered(first, again):
        send_number = iter(range(first, 64))
        if again is not None:
            taken = [transfer[0][1] for transfer in again]
            return zip(send_number, taken)
        return zip(send_number, numbers)

    def both(first, axis, up, land0, down, land1, again=None):
        pair = numbered(first, again)
        return (
            (next(pair), ((axis, 1),), up, land0),
            (next(pair), ((axis, -1),), down, land1),
        )

    def diagonal(first, axes, source, land):
        found = []
        pair = numbered(first, None)
        for steps in itertools.product((1, -1), repeat=len(axes)):
            sides = tuple((1 - step) // 2 for step in steps)
            from_sides = tuple(1 - side for side in sides)
            steps = tuple(zip(axes, steps))
            found.append((next(pair), steps, source(*from_sides), land.at[sides]))
        return tuple(found)

    def copy(transfer, steps):
        number, _, source, land = transfer
        return pltpu.make_async_remote_copy(
            src_ref=source,
            dst_ref=land,
            send_sem=send_sem.at[number[0]],
            recv_sem=recv_sem.at[number[1]],
            device_id=peer(steps),
            device_id_type=MESH,
        )

    def send(group):
        for transfer in group:
            pl.when(there(transfer[1]))(lambda t=transfer: copy(t, t[1]).start())

    def arrive(group):
        for transfer in group:
            steps = back(transfer[1])
            pl.when(there(steps))(lambda t=transfer, s=steps: copy(t, s).wait_recv())

    def sent(group):
        for transfer in group:
            pl.when(there(transfer[1]))(lambda t=transfer: copy(t, t[1]).wait_send())

    def blank(group):
        for _, steps, _, land in group:

            @pl.when(jnp.logical_not(there(back(steps))))
            def _():
                land[...] = jnp.zeros(land.shape, F32)

    g_pos = [
        both(2 * h, "gx", mine.at[1, h], theirs.at[0, h], mine.at[0, h], theirs.at[1, h])
        for h in range(PARTS)
    ]
    first = 2 * PARTS
    g_y = both(first, "gy", y_out.at[1], yb.at[:, 0:8], y_out.at[0], yb.at[:, 16:24])
    g_z = both(first + 2, "gz", z_out.at[1], z_in.at[0:8], z_out.at[0], z_in.at[8:16])
    g_yz = diagonal(first + 4, ("gy", "gz"), lambda y, z: z_out.at[z], yz_in)
    g_part = [
        both(
            first + 20 + 2 * h,
            "gx",
            part_out.at[1, h],
            part_in.at[0, h],
            part_out.at[0, h],
            part_in.at[1, h],
        )
        for h in range(PARTS)
    ]
    d_terms = [
        both(
            2 * h,
            "gx",
            terms_pack.at[h],
            terms_in.at[0, h],
            terms_pack.at[h],
            terms_in.at[1, h],
            again=g_pos[h],
        )
        for h in range(PARTS)
    ]
    d_z = both(
        first + 16,
        "gz",
        dz_out.at[8:16, 0:OWN],
        dz_in.at[0:8],
        dz_out.at[0:8, 0:OWN],
        dz_in.at[8:16],
    )
    d_y = both(first + 18, "gy", dy.at[16:24], dy_in.at[0], dy.at[0:8], dy_in.at[1])
    d_yz = diagonal(
        first + 20, ("gy", "gz"), lambda y, z: dz_out.at[8 * z : 8 * z + 8, OWN:COLS], dyz_in
    )
    d_xz = diagonal(first, ("gx", "gz"), lambda x, z: dxz_out.at[8 * z : 8 * z + 8], dxz_in)

    def edge(x, y):
        first = 16 * x + 8 * y
        return slice(first, first + 8)

    d_xy = diagonal(first + 4, ("gx", "gy"), lambda x, y: dxy_out.at[edge(x, y), 0:128], dxy_in)
    d_xyz = diagonal(
        first + 8, ("gx", "gy", "gz"), lambda x, y, z: dxy_out.at[edge(x, y), 128:256], dxyz_in
    )
    groups = (g_y, g_z, g_yz, d_xz, d_xy, d_xyz, d_z, d_y, d_yz)
    groups += tuple(g_pos) + tuple(g_part) + tuple(d_terms)

    barrier = pltpu.get_barrier_semaphore()
    for _, steps, _, _ in g_pos[0] + g_y + g_z + g_yz:
        pl.when(there(steps))(
            lambda s=steps: pl.semaphore_signal(
                barrier, inc=1, device_id=peer(s), device_id_type=MESH
            )
        )

    loads = []
    for number, (source, land) in enumerate(
        (
            (pos_hbm, pos),
            (li_hbm, li),
            (lj_hbm, lj),
            (lk_hbm, lk),
            (vel, fields.at[0:3]),
            (scal, fields.at[3:6]),
            (mot_hbm, mot),
            (heat_hbm, heat),
            (diam_hbm, diam),
        )
    ):
        loads.append(pltpu.make_async_copy(source, land, send_sem.at[first + 8 + number]))
        loads[-1].start()

    for group in groups:
        blank(group)
    yb[:, 8:16] = jnp.zeros((NF, 8, CK), F32)
    yb[:, 24:128] = jnp.zeros((NF, 104, CK), F32)
    z_out[...] = jnp.zeros(z_out.shape, F32)
    dxy_out[...] = jnp.zeros(dxy_out.shape, F32)
    zt[:, 10:16] = jnp.zeros((OWN // 128, 6, 128), F32)
    s_hi[OWN + 32 : COLS] = jnp.zeros((96, n), BF16)
    s_lo[OWN + 32 : COLS] = jnp.zeros((96, n), BF16)

    for load in loads[0:4]:
        load.wait()
    at = [pos[axis : axis + 1] for axis in range(3)]
    cell = [ref[...].reshape(1, n).astype(F32) for ref in (li, lj, lk)]
    reach = [tent(at[0] - (place - cell[0])) for place in (-1.0, float(CI))]
    for x in range(2):
        for number, row in enumerate((reach[x], at[1], cell[1], at[2], cell[2])):
            for h, part in enumerate(parts):
                pack(mine.at[x, h], number, row[:, part])

    for load in loads[4:]:
        load.wait()
    for f in range(NF):
        for i in range(CI):
            y_out[0, f, i : i + 1, :] = fields[f, i, 0:1, :]
            y_out[1, f, i : i + 1, :] = fields[f, i, CJ - 1 : CJ, :]
    for f in range(NF):
        for b in range(OWN // 128):
            block = fields[f, 2 * b : 2 * b + 2].reshape(128, CK).T
            z_out[0, f : f + 1, b * 128 : b * 128 + 128] = block[0:1]
            z_out[1, f : f + 1, b * 128 : b * 128 + 128] = block[CK - 1 : CK]
            hi, lo = split(block)
            a_hi[f * CK : f * CK + CK, b * 128 : b * 128 + 128] = hi
            a_lo[f * CK : f * CK + CK, b * 128 : b * 128 + 128] = lo
    near = {axis: jnp.minimum(me[axis], 1) + jnp.minimum(ends[axis] - me[axis], 1) for axis in axes}
    pl.semaphore_wait(barrier, near["gx"] + near["gy"] + near["gz"] + near["gy"] * near["gz"])
    for h in range(PARTS):
        send(g_pos[h])
    send(g_y)
    send(g_z)
    send(g_yz)

    def ramp(rows, columns=n):
        return iota((rows, columns), 0).astype(F32)

    row16 = iota((16, n), 0)

    def k_weights(x, part, offset, cell):
        rows = iota((16, offset.shape[1]), 0)
        hi, lo = split(tent(offset - (ramp(CK, offset.shape[1]) - cell)))
        l_hi[x, 0:CK, part] = hi
        l_lo[x, 0:CK, part] = lo
        low, high = tent(offset - (-1.0 - cell)), tent(offset - (float(CK) - cell))
        hi, lo = split(jnp.where(rows == 0, low, jnp.where(rows == 8, high, 0.0)))
        l_hi[x, CK:, part] = hi
        l_lo[x, CK:, part] = lo
        return low, high

    wi[...] = jnp.where(row16 < CI, tent(at[0] - (ramp(16) - cell[0])), 0.0)
    wj = tent(at[1] - (ramp(CJ) - cell[1]))
    wj_ends = (tent(at[1] - (-1.0 - cell[1])), tent(at[1] - (float(CJ) - cell[1])))
    lines[...] = tent(at[2] - (ramp(CK) - cell[2]))
    line_ends[0:1], line_ends[1:2] = k_weights(2, slice(0, n), at[2], cell[2])
    for i in range(CI):
        hi, lo = split(wi[i : i + 1] * wj)
        s_hi[i * CJ : i * CJ + CJ] = hi
        s_lo[i * CJ : i * CJ + CJ] = lo
    for y in range(2):
        hi, lo = split(wi[...] * wj_ends[y])
        s_hi[OWN + 16 * y : OWN + 16 * y + 16] = hi
        s_lo[OWN + 16 * y : OWN + 16 * y + 16] = lo
    for x in range(2):
        hi, lo = split(reach[x] * wj)
        x_hi[x * CJ : x * CJ + CJ] = hi
        x_lo[x * CJ : x * CJ + CJ] = lo
        for y in range(2):
            edges[2 * x + y : 2 * x + y + 1] = reach[x] * wj_ends[y]

    lane16 = iota((16, 128), 1)
    arrive(g_y)
    for f in range(NF):
        hi, lo = split(yb[f].T)
        a_hi[f * CK : f * CK + CK, OWN:COLS] = hi
        a_lo[f * CK : f * CK + CK, OWN:COLS] = lo
    arrive(g_z)
    hi, lo = split(z_in[...])
    a_hi[NF * CK : ROWS, 0:OWN] = hi
    a_lo[NF * CK : ROWS, 0:OWN] = lo
    arrive(g_yz)
    corner = jnp.zeros((16, 128), F32)
    for y in range(2):
        for i in range(CI):
            at = i * CJ + (CJ - 1 if y == 0 else 0)
            first = at // 128 * 128
            block = jnp.concatenate([yz_in[y, z, :, first : first + 128] for z in range(2)], axis=0)
            to = 16 * y + i
            moved = pltpu.roll(block, (to - at) % 128, 1)
            corner = jnp.where(lane16 == to, moved, corner)
    hi, lo = split(corner)
    a_hi[NF * CK : ROWS, OWN:COLS] = hi
    a_lo[NF * CK : ROWS, OWN:COLS] = lo

    def z_block(value):
        hi, lo = split(value)
        hi, lo = hi.astype(F32), lo.astype(F32)
        return (hi + pltpu.roll(hi, 16, 1) + pltpu.roll(lo, 32, 1)).astype(BF16)

    def put_plane(x, at, rows, value, ends_value):
        hi, lo = split(value)
        e_lhs[x, at : at + rows, 0:128] = hi
        e_lhs[x, at : at + rows, 128:256] = hi
        e_lhs[x, at : at + rows, 256:384] = lo
        e_lhs[x, at : at + rows, 384:512] = z_block(ends_value)

    lane64 = iota((CJ, 128), 1)
    lane8 = iota((8, 128), 1)
    for x in range(2):
        i = 0 if x == 0 else CI - 1
        first = i * CJ // 128 * 128
        columns = jnp.concatenate(
            [z_in[:, first : first + 128], jnp.zeros((112, 128), F32)], axis=0
        ).T
        columns = columns[0:CJ] if x == 0 else columns[CJ:128]
        for f in range(NF):
            moved = columns if f == 0 else pltpu.roll(columns, 128 - f, 1)
            moved = jnp.where((lane64 == 0) | (lane64 == 8), moved, 0.0)
            put_plane(x, f * CJ, CJ, fields[f, i], moved)
        values, moves = [], []
        for y in range(2):
            values += [yb[f, 16 * y + i : 16 * y + i + 1, :] for f in range(NF)]
            values.append(jnp.zeros((2, CK), F32))
            at = i * CJ + (CJ - 1 if y == 0 else 0)
            first = at // 128 * 128
            total = jnp.zeros((8, 128), F32)
            for z in range(2):
                block = pltpu.roll(yz_in[y, z, :, first : first + 128], (8 * z - at) % 128, 1)
                total = jnp.where(lane8 == 8 * z, block, total)
            moves.append(total)
        put_plane(
            x, NF * CJ, 16, jnp.concatenate(values, axis=0), jnp.concatenate(moves, axis=0)
        )

    chunks = [slice(c * 256, c * 256 + 256) for c in range(n // 256)]

    def gather(chunk):
        left = jnp.concatenate([a_hi[...], a_hi[...], a_lo[...]], axis=1)
        right = jnp.concatenate([s_hi[:, chunk], s_lo[:, chunk], s_hi[:, chunk]], axis=0)
        value = jnp.dot(left, right, preferred_element_type=F32)
        for f in range(NF):
            total = jnp.sum(value[f * CK : f * CK + CK] * lines[:, chunk], axis=0, keepdims=True)
            for z in range(2):
                row = NF * CK + 8 * z + f
                total = total + value[row : row + 1] * line_ends[z : z + 1, chunk]
            gathered[f : f + 1, chunk] = total

    for chunk in chunks[:2]:
        gather(chunk)

    for h, part in enumerate(parts):
        arrive(g_pos[h])
        for x in range(2):
            near_x, at_j, cell_j, at_k, cell_k = [unpack(theirs.at[x, h], q) for q in range(5)]
            ws[x, :, part] = near_x * tent(at_j - (ramp(CJ, width) - cell_j))
            ws_ends[x, 0:1, part] = near_x * tent(at_j - (-1.0 - cell_j))
            ws_ends[x, 1:2, part] = near_x * tent(at_j - (float(CJ) - cell_j))
            k_weights(x, part, at_k, cell_k)
        for x in range(2):
            for start in range(part.start, part.stop, 256):
                chunk = slice(start, start + 256)
                top, low = l_hi[x, 0:CK, chunk], l_lo[x, 0:CK, chunk]
                top_z, low_z = l_hi[x, CK:, chunk], l_lo[x, CK:, chunk]
                right = jnp.concatenate(
                    [top, low, top, top_z, low_z, top_z, jnp.zeros((80, 256), BF16)], axis=0
                )
                value = jnp.dot(e_lhs[x], right, preferred_element_type=F32)
                last = NF * CJ
                total = value[last : last + 8] * ws_ends[x, 0:1, chunk]
                total = total + value[last + 8 : last + 16] * ws_ends[x, 1:2, chunk]
                weight = ws[x, :, chunk]
                for f in range(NF):
                    row = jnp.sum(value[f * CJ : f * CJ + CJ] * weight, axis=0, keepdims=True)
                    row = row + total[f : f + 1]
                    pack(part_out.at[x, h], f, row, (start - part.start) // 128)
        send(g_part[h])

    for chunk in chunks[2:]:
        gather(chunk)

    for group in (*g_pos, g_y, g_z, g_yz):
        sent(group)

    terms_out[5:8] = jnp.zeros((3, n), F32)
    for h, part in enumerate(parts):
        motion = mot[:, part]
        warmth = heat[part].reshape(1, width)
        q = diam[part].reshape(1, width)
        live = (iota((1, width), 1) + h * width) // TILE < tally[0]
        arrive(g_part[h])
        got = [
            gathered[f : f + 1, part]
            + unpack(part_in.at[0, h], f)
            + unpack(part_in.at[1, h], f)
            for f in range(NF)
        ]
        gas = jnp.concatenate(got[0:3], axis=0)
        gas_heat, moisture, rho = got[3:6]
        drag = step_time / (0.5 * q)
        new_motion = (motion + drag * gas) / (1.0 + drag)
        mass = q * jnp.sqrt(q)
        vapour = jnp.exp(4.0 * (warmth - 1.0))
        decay = step_time * evap_rate * rho * (vapour - moisture)
        new_q = q - decay
        new_mass = new_q * jnp.sqrt(new_q)
        conduction = step_time * heat_rate * rho / q
        new_heat = (warmth + conduction * gas_heat) / (1.0 + conduction) - (
            boiling_energy_drain * decay / q
        )
        state[0:3, part] = jnp.where(live, new_motion, motion)
        state[3:4, part] = jnp.where(live, new_heat, warmth)
        state[4:5, part] = jnp.where(live, new_q, q)
        pushes = jnp.where(live, mass * (motion - new_motion), 0.0)
        terms = [pushes[c : c + 1] for c in range(3)]
        terms.append(jnp.where(live, mass * (warmth - new_heat), 0.0))
        terms.append(jnp.where(live, mass - new_mass, 0.0))
        for c in range(NS):
            terms_out[c : c + 1, part] = terms[c]
            pack(terms_pack.at[h], c, terms[c])
        send(d_terms[h])

    def cross(left, right):
        return lax.dot_general(
            left, right, (((1,), (1,)), ((), ())), preferred_element_type=F32
        )

    tail = jnp.concatenate(
        [terms_out[...] * line_ends[0:1], terms_out[...] * line_ends[1:2]], axis=0
    )
    hi, lo = split(tail)
    tail = jnp.concatenate([hi, hi, lo], axis=1)
    tail = jnp.concatenate([tail, jnp.zeros((112, 3 * n), BF16)], axis=0)
    left = jnp.concatenate([x_hi[...], x_lo[...], x_hi[...]], axis=1)
    dxz_out[...] = cross(left, tail).T[0:16]
    hi, lo = split(
        jnp.concatenate([terms_out[...] * edges[line : line + 1] for line in range(4)], axis=0)
    )
    left = jnp.concatenate([hi, hi, lo], axis=1)
    right = jnp.concatenate([l_hi[2], l_lo[2], l_hi[2]], axis=1)
    value = cross(left, right)
    dxy_out[:, 0:128] = value[:, 0:CK]
    dxy_out[:, 128:144] = value[:, CK : CK + 16]
    send(d_xyz)
    send(d_xy)
    send(d_xz)

    lines_used = slice(0, OWN + 32)
    for w in (2, 0, 1):
        left = jnp.concatenate(
            [s_hi[lines_used], s_lo[lines_used], s_hi[lines_used]], axis=1
        )
        right = []
        for c in (2 * w, 2 * w + 1):
            if c < NS:
                hi, lo = split(terms_out[c : c + 1] * lines[...])
                right.append(jnp.concatenate([hi, hi, lo], axis=1))
            else:
                right.append(tail)
        right = jnp.concatenate(right, axis=0)
        if w < 2:
            value = cross(left, right)
        else:
            value = jnp.concatenate(
                [cross(left[0:272], right), cross(left[272:], right)], axis=0
            )
        for h in range(2):
            c = 2 * w + h
            half = value[:, h * 128 : h * 128 + 128]
            if c < NS:
                out[c] = half[0:OWN].reshape(CI, CJ, CK)
                dy[:, c * CK : c * CK + CK] = half[OWN : OWN + 32]
            else:
                for b in range(OWN // 128):
                    dz_out[:, b * 128 : b * 128 + 128] = half[b * 128 : b * 128 + 128].T[0:16]
                rest = jnp.concatenate([half[OWN : OWN + 32], jnp.zeros((96, 128), F32)], axis=0)
                dz_out[:, OWN:COLS] = rest.T[0:16]

    for group in g_part:
        sent(group)
    send(d_z)
    send(d_yz)
    send(d_y)

    for h, part in enumerate(parts):
        arrive(d_terms[h])
        for x in range(2):
            i = 0 if x == 0 else CI - 1
            weight = ws[x, :, part]
            left = []
            for c in range(NS):
                hi, lo = split(unpack(terms_in.at[x, h], c) * weight)
                left.append(jnp.concatenate([hi, hi, lo], axis=1))
            left = jnp.concatenate(left, axis=0)
            hi, lo = l_hi[x, 0:CK, part], l_lo[x, 0:CK, part]
            right = jnp.concatenate([hi, lo, hi], axis=1)
            value = cross(left, right)
            for c in range(NS):
                out[c, i] = out[c, i] + value[c * CJ : c * CJ + CJ]

    for group in (*d_terms, d_xz, d_xy, d_xyz):
        sent(group)
    arrive(d_z)
    arrive(d_y)
    arrive(d_yz)
    arrive(d_xz)
    arrive(d_xy)
    arrive(d_xyz)
    for b in range(OWN // 128):
        block = dz_in[:, b * 128 : b * 128 + 128]
        for i in (2 * b, 2 * b + 1):
            for y in range(2):
                to = i * CJ % 128 + (0 if y == 0 else CJ - 1)
                at = (16 if y == 0 else 0) + i
                moved = jnp.concatenate([dyz_in[y, 0], dyz_in[y, 1]], axis=0)
                moved = pltpu.roll(moved, (to - at) % 128, 1)
                block = block + jnp.where(lane16 == to, moved, 0.0)
        if b in (0, OWN // 128 - 1):
            x = 0 if b == 0 else 1
            moved = jnp.concatenate([dxz_in[x, 0], dxz_in[x, 1]], axis=0)
            half = lane16 < CJ if x == 0 else lane16 >= CJ
            block = block + jnp.where(half, pltpu.roll(moved, CJ, 1), 0.0)
            for y in range(2):
                to = CJ * x + (0 if y == 0 else CJ - 1)
                moved = jnp.concatenate(
                    [
                        pltpu.roll(dxyz_in[x, y, z], (to - 8 * (1 - z)) % 128, 1)
                        for z in range(2)
                    ],
                    axis=0,
                )
                block = block + jnp.where(lane16 == to, moved, 0.0)
        for c in range(NS):
            zt[b, 2 * c : 2 * c + 1] = block[8 + c : 9 + c]
            zt[b, 2 * c + 1 : 2 * c + 2] = block[c : c + 1]
    rows[...] = dy_in[...]
    for x in range(2):
        i = 0 if x == 0 else CI - 1
        for y in range(2):
            for c in range(NS):
                at = slice(c * CK, c * CK + CK)
                rows[y, i : i + 1, at] = rows[y, i : i + 1, at] + dxy_in[x, y, c : c + 1, :]

    for group in (d_z, d_y, d_yz):
        sent(group)


def deliver(part, state, zt, rows, out, state_out, whole, sem):
    state_copy = pltpu.make_async_copy(state, state_out, sem.at[NS])
    state_copy.start()
    lane = iota((128, 128), 1)
    rim = (lane == 0) | (lane == CK - 1)
    blocks = range(OWN // 128)
    columns = [
        jnp.concatenate([zt[b], jnp.zeros((112, 128), F32)], axis=0).T for b in blocks
    ]
    copies = []
    for c in range(NS):
        for b in blocks:
            add = jnp.where(rim, pltpu.roll(columns[b], 127 - 2 * c, 1), 0.0)
            whole[c, 2 * b : 2 * b + 2] = part[c, 2 * b : 2 * b + 2] + add.reshape(2, CJ, CK)
        for y in range(2):
            j = 0 if y == 0 else CJ - 1
            for i in range(CI):
                whole[c, i, j : j + 1, :] = (
                    whole[c, i, j : j + 1, :] + rows[y, i : i + 1, c * CK : c * CK + CK]
                )
        copies.append(pltpu.make_async_copy(whole.at[c], out.at[c], sem.at[c]))
        copies[-1].start()
    for copy in copies + [state_copy]:
        copy.wait()


def local(sizes, vel, scal, pos, mot, heat, diam, li, lj, lk, tally):
    n = heat.shape[0]
    vmem = pl.BlockSpec(memory_space=pltpu.VMEM)
    hbm = pl.BlockSpec(memory_space=pltpu.HBM)
    planes = NF * CJ + 16
    parts = pl.pallas_call(
        functools.partial(kernel, sizes),
        out_shape=(
            jax.ShapeDtypeStruct((NS, CI, CJ, CK), F32),
            jax.ShapeDtypeStruct((NS, n), F32),
            jax.ShapeDtypeStruct((OWN // 128, 16, 128), F32),
            jax.ShapeDtypeStruct((2, 8, NS * CK), F32),
        ),
        in_specs=[hbm] * 9 + [pl.BlockSpec(memory_space=pltpu.SMEM)],
        out_specs=(vmem,) * 4,
        scratch_shapes=[
            pltpu.VMEM((NF, CI, CJ, CK), F32),
            pltpu.VMEM((3, n), F32),
            pltpu.VMEM((3, n), F32),
            pltpu.VMEM((n,), F32),
            pltpu.VMEM((n,), F32),
            pltpu.VMEM((n,), jnp.int32),
            pltpu.VMEM((n,), jnp.int32),
            pltpu.VMEM((n,), jnp.int32),
            pltpu.VMEM((2, PARTS, 5 * n // PARTS // 128, 128), F32),
            pltpu.VMEM((2, PARTS, 5 * n // PARTS // 128, 128), F32),
            pltpu.VMEM((ROWS, COLS), BF16),
            pltpu.VMEM((ROWS, COLS), BF16),
            pltpu.VMEM((COLS, n), BF16),
            pltpu.VMEM((COLS, n), BF16),
            pltpu.VMEM((2, planes, 512), BF16),
            pltpu.VMEM((3, CK + 16, n), BF16),
            pltpu.VMEM((3, CK + 16, n), BF16),
            pltpu.VMEM((2 * CJ, n), BF16),
            pltpu.VMEM((2 * CJ, n), BF16),
            pltpu.VMEM((8, n), F32),
            pltpu.VMEM((2, CJ, n), F32),
            pltpu.VMEM((2, 8, n), F32),
            pltpu.VMEM((16, n), F32),
            pltpu.VMEM((CK, n), F32),
            pltpu.VMEM((8, n), F32),
            pltpu.VMEM((8, n), F32),
            pltpu.VMEM((2, PARTS, NF * n // PARTS // 128, 128), F32),
            pltpu.VMEM((2, PARTS, NF * n // PARTS // 128, 128), F32),
            pltpu.VMEM((8, n), F32),
            pltpu.VMEM((PARTS, NS * n // PARTS // 128, 128), F32),
            pltpu.VMEM((2, PARTS, NS * n // PARTS // 128, 128), F32),
            pltpu.VMEM((NF, 128, CK), F32),
            pltpu.VMEM((2, NF, 8, CK), F32),
            pltpu.VMEM((2, 8, OWN), F32),
            pltpu.VMEM((16, OWN), F32),
            pltpu.VMEM((2, 2, 8, OWN), F32),
            pltpu.VMEM((32, NS * CK), F32),
            pltpu.VMEM((2, 8, NS * CK), F32),
            pltpu.VMEM((16, COLS), F32),
            pltpu.VMEM((16, OWN), F32),
            pltpu.VMEM((2, 2, 8, 128), F32),
            pltpu.VMEM((16, 128), F32),
            pltpu.VMEM((2, 2, 8, 128), F32),
            pltpu.VMEM((32, 256), F32),
            pltpu.VMEM((2, 2, 8, 128), F32),
            pltpu.VMEM((2, 2, 2, 8, 128), F32),
            pltpu.SemaphoreType.DMA((2 * PARTS + 20 + max(4, 2 * PARTS),)),
            pltpu.SemaphoreType.DMA((32 + 4 * PARTS,)),
        ],
        compiler_params=pltpu.CompilerParams(
            collective_id=0, has_side_effects=True, vmem_limit_bytes=32 * 1024 * 1024
        ),
    )(*(pltpu.with_memory_space_constraint(x, pltpu.HBM) for x in (vel, scal, pos, mot, heat, diam, li, lj, lk)), tally)
    return pl.pallas_call(
        deliver,
        out_shape=tuple(jax.ShapeDtypeStruct(part.shape, F32) for part in parts[:2]),
        in_specs=[vmem] * 4,
        out_specs=(hbm, hbm),
        scratch_shapes=[
            pltpu.VMEM((NS, CI, CJ, CK), F32),
            pltpu.SemaphoreType.DMA((NS + 1,)),
        ],
        compiler_params=pltpu.CompilerParams(vmem_limit_bytes=4 * 1024 * 1024),
    )(*parts)


def solution(mesh):
    sizes = {axis: mesh.shape[axis] for axis in ("gx", "gy", "gz")}
    flat = P(("gx", "gy", "gz"))
    wide = P(None, ("gx", "gy", "gz"))
    grid = P(None, "gx", "gy", "gz")
    return jax.shard_map(
        functools.partial(local, sizes),
        mesh=mesh,
        in_specs=(grid, grid, wide, wide) + (flat,) * 6,
        out_specs=(grid, wide),
        check_vma=False,
    )
```

```python
import functools
import itertools

import jax
import jax.numpy as jnp
from jax import lax
from jax.experimental import pallas as pl
from jax.experimental.pallas import tpu as pltpu
from jax.sharding import PartitionSpec as P

TILE = 128
NF = 6
NS = 5
CI, CJ, CK = 8, 64, 128
OWN = CI * CJ
COLS = OWN + 128
ROWS = NF * CK + 16
PARTS = 2
MESH = pl.DeviceIdType.MESH
F32 = jnp.float32
BF16 = jnp.bfloat16

step_time = 0.25
evap_rate = 1.0
heat_rate = 2.0
boiling_energy_drain = 0.3


def split(x):
    hi = x.astype(BF16)
    return hi, (x - hi.astype(F32)).astype(BF16)


def tent(offset):
    return jnp.maximum(0.0, 1.0 - jnp.abs(offset))


def iota(shape, dim):
    return lax.broadcasted_iota(jnp.int32, shape, dim)


def kernel(
    sizes,
    vel,
    scal,
    pos_hbm,
    mot_hbm,
    heat_hbm,
    diam_hbm,
    li_hbm,
    lj_hbm,
    lk_hbm,
    tally_hbm,
    out,
    state,
    zt,
    rows,
    fields,
    pos,
    mot,
    heat,
    diam,
    li,
    lj,
    lk,
    tally,
    mine,
    theirs,
    a_hi,
    a_lo,
    s_hi,
    s_lo,
    e_lhs,
    l_hi,
    l_lo,
    x_hi,
    x_lo,
    edges,
    ws,
    ws_ends,
    wi,
    lines,
    line_ends,
    gathered,
    part_out,
    part_in,
    terms_out,
    terms_pack,
    terms_in,
    yb,
    y_out,
    z_out,
    z_in,
    yz_in,
    dy,
    dy_in,
    dz_out,
    dz_in,
    dyz_in,
    dxz_out,
    dxz_in,
    dxy_out,
    dxy_in,
    dxyz_in,
    send_sem,
    recv_sem,
):
    n = pos.shape[1]
    width = n // PARTS
    parts = [slice(h * width, h * width + width) for h in range(PARTS)]
    per_row = width // 128
    axes = tuple(sizes)
    me = {axis: lax.axis_index(axis) for axis in axes}
    ends = {axis: size - 1 for axis, size in sizes.items()}

    def there(steps):
        found = None
        for axis, step in steps:
            one = me[axis] < ends[axis] if step > 0 else me[axis] > 0
            found = one if found is None else jnp.logical_and(found, one)
        return found

    def peer(steps):
        return {axis: me[axis] + step for axis, step in steps}

    def back(steps):
        return tuple((axis, -step) for axis, step in steps)

    numbers = iter(range(64))

    def pack(ref, number, row, first=0):
        for b in range(row.shape[1] // 128):
            at = number * per_row + first + b
            ref[at : at + 1, :] = row[:, b * 128 : b * 128 + 128]

    def unpack(ref, number):
        first = number * per_row
        return jnp.concatenate([ref[first + b : first + b + 1, :] for b in range(per_row)], axis=1)

    def numbered(first, again):
        send_number = iter(range(first, 64))
        if again is not None:
            taken = [transfer[0][1] for transfer in again]
            return zip(send_number, taken)
        return zip(send_number, numbers)

    def both(first, axis, up, land0, down, land1, again=None):
        pair = numbered(first, again)
        return (
            (next(pair), ((axis, 1),), up, land0),
            (next(pair), ((axis, -1),), down, land1),
        )

    def diagonal(first, axes, source, land):
        found = []
        pair = numbered(first, None)
        for steps in itertools.product((1, -1), repeat=len(axes)):
            sides = tuple((1 - step) // 2 for step in steps)
            from_sides = tuple(1 - side for side in sides)
            steps = tuple(zip(axes, steps))
            found.append((next(pair), steps, source(*from_sides), land.at[sides]))
        return tuple(found)

    def copy(transfer, steps):
        number, _, source, land = transfer
        return pltpu.make_async_remote_copy(
            src_ref=source,
            dst_ref=land,
            send_sem=send_sem.at[number[0]],
            recv_sem=recv_sem.at[number[1]],
            device_id=peer(steps),
            device_id_type=MESH,
        )

    def send(group):
        for transfer in group:
            pl.when(there(transfer[1]))(lambda t=transfer: copy(t, t[1]).start())

    def arrive(group):
        for transfer in group:
            steps = back(transfer[1])
            pl.when(there(steps))(lambda t=transfer, s=steps: copy(t, s).wait_recv())

    def sent(group):
        for transfer in group:
            pl.when(there(transfer[1]))(lambda t=transfer: copy(t, t[1]).wait_send())

    def blank(group):
        for _, steps, _, land in group:

            @pl.when(jnp.logical_not(there(back(steps))))
            def _():
                land[...] = jnp.zeros(land.shape, F32)

    g_pos = [
        both(2 * h, "gx", mine.at[1, h], theirs.at[0, h], mine.at[0, h], theirs.at[1, h])
        for h in range(PARTS)
    ]
    first = 2 * PARTS
    g_y = both(first, "gy", y_out.at[1], yb.at[:, 0:8], y_out.at[0], yb.at[:, 16:24])
    g_z = both(first + 2, "gz", z_out.at[1], z_in.at[0:8], z_out.at[0], z_in.at[8:16])
    g_yz = diagonal(first + 4, ("gy", "gz"), lambda y, z: z_out.at[z], yz_in)
    g_part = [
        both(
            first + 20 + 2 * h,
            "gx",
            part_out.at[1, h],
            part_in.at[0, h],
            part_out.at[0, h],
            part_in.at[1, h],
        )
        for h in range(PARTS)
    ]
    d_terms = [
        both(
            2 * h,
            "gx",
            terms_pack.at[h],
            terms_in.at[0, h],
            terms_pack.at[h],
            terms_in.at[1, h],
            again=g_pos[h],
        )
        for h in range(PARTS)
    ]
    d_z = both(
        first + 16,
        "gz",
        dz_out.at[8:16, 0:OWN],
        dz_in.at[0:8],
        dz_out.at[0:8, 0:OWN],
        dz_in.at[8:16],
    )
    d_y = both(first + 18, "gy", dy.at[16:24], dy_in.at[0], dy.at[0:8], dy_in.at[1])
    d_yz = diagonal(
        first + 20, ("gy", "gz"), lambda y, z: dz_out.at[8 * z : 8 * z + 8, OWN:COLS], dyz_in
    )
    d_xz = diagonal(first, ("gx", "gz"), lambda x, z: dxz_out.at[8 * z : 8 * z + 8], dxz_in)

    def edge(x, y):
        first = 16 * x + 8 * y
        return slice(first, first + 8)

    d_xy = diagonal(first + 4, ("gx", "gy"), lambda x, y: dxy_out.at[edge(x, y), 0:128], dxy_in)
    d_xyz = diagonal(
        first + 8, ("gx", "gy", "gz"), lambda x, y, z: dxy_out.at[edge(x, y), 128:256], dxyz_in
    )
    groups = (g_y, g_z, g_yz, d_xz, d_xy, d_xyz, d_z, d_y, d_yz)
    groups += tuple(g_pos) + tuple(g_part) + tuple(d_terms)

    barrier = pltpu.get_barrier_semaphore()
    for _, steps, _, _ in g_pos[0] + g_y + g_z + g_yz:
        pl.when(there(steps))(
            lambda s=steps: pl.semaphore_signal(
                barrier, inc=1, device_id=peer(s), device_id_type=MESH
            )
        )

    loads = []
    for number, (source, land) in enumerate(
        (
            (pos_hbm, pos),
            (li_hbm, li),
            (lj_hbm, lj),
            (lk_hbm, lk),
            (vel, fields.at[0:3]),
            (scal, fields.at[3:6]),
            (mot_hbm, mot),
            (heat_hbm, heat),
            (diam_hbm, diam),
            (tally_hbm, tally),
        )
    ):
        loads.append(pltpu.make_async_copy(source, land, send_sem.at[first + 8 + number]))
        loads[-1].start()

    for group in groups:
        blank(group)
    yb[:, 8:16] = jnp.zeros((NF, 8, CK), F32)
    yb[:, 24:128] = jnp.zeros((NF, 104, CK), F32)
    z_out[...] = jnp.zeros(z_out.shape, F32)
    dxy_out[...] = jnp.zeros(dxy_out.shape, F32)
    zt[:, 10:16] = jnp.zeros((OWN // 128, 6, 128), F32)
    s_hi[OWN + 32 : COLS] = jnp.zeros((96, n), BF16)
    s_lo[OWN + 32 : COLS] = jnp.zeros((96, n), BF16)

    for load in loads[0:4]:
        load.wait()
    at = [pos[axis : axis + 1] for axis in range(3)]
    cell = [ref[...].reshape(1, n).astype(F32) for ref in (li, lj, lk)]
    reach = [tent(at[0] - (place - cell[0])) for place in (-1.0, float(CI))]
    for x in range(2):
        for number, row in enumerate((reach[x], at[1], cell[1], at[2], cell[2])):
            for h, part in enumerate(parts):
                pack(mine.at[x, h], number, row[:, part])

    for load in loads[4:]:
        load.wait()
    for f in range(NF):
        for i in range(CI):
            y_out[0, f, i : i + 1, :] = fields[f, i, 0:1, :]
            y_out[1, f, i : i + 1, :] = fields[f, i, CJ - 1 : CJ, :]
    for f in range(NF):
        for b in range(OWN // 128):
            block = fields[f, 2 * b : 2 * b + 2].reshape(128, CK).T
            z_out[0, f : f + 1, b * 128 : b * 128 + 128] = block[0:1]
            z_out[1, f : f + 1, b * 128 : b * 128 + 128] = block[CK - 1 : CK]
            hi, lo = split(block)
            a_hi[f * CK : f * CK + CK, b * 128 : b * 128 + 128] = hi
            a_lo[f * CK : f * CK + CK, b * 128 : b * 128 + 128] = lo
    near = {axis: jnp.minimum(me[axis], 1) + jnp.minimum(ends[axis] - me[axis], 1) for axis in axes}
    pl.semaphore_wait(barrier, near["gx"] + near["gy"] + near["gz"] + near["gy"] * near["gz"])
    for h in range(PARTS):
        send(g_pos[h])
    send(g_y)
    send(g_z)
    send(g_yz)

    def ramp(rows, columns=n):
        return iota((rows, columns), 0).astype(F32)

    row16 = iota((16, n), 0)

    def k_weights(x, part, offset, cell):
        rows = iota((16, offset.shape[1]), 0)
        hi, lo = split(tent(offset - (ramp(CK, offset.shape[1]) - cell)))
        l_hi[x, 0:CK, part] = hi
        l_lo[x, 0:CK, part] = lo
        low, high = tent(offset - (-1.0 - cell)), tent(offset - (float(CK) - cell))
        hi, lo = split(jnp.where(rows == 0, low, jnp.where(rows == 8, high, 0.0)))
        l_hi[x, CK:, part] = hi
        l_lo[x, CK:, part] = lo
        return low, high

    wi[...] = jnp.where(row16 < CI, tent(at[0] - (ramp(16) - cell[0])), 0.0)
    wj = tent(at[1] - (ramp(CJ) - cell[1]))
    wj_ends = (tent(at[1] - (-1.0 - cell[1])), tent(at[1] - (float(CJ) - cell[1])))
    lines[...] = tent(at[2] - (ramp(CK) - cell[2]))
    line_ends[0:1], line_ends[1:2] = k_weights(2, slice(0, n), at[2], cell[2])
    for i in range(CI):
        hi, lo = split(wi[i : i + 1] * wj)
        s_hi[i * CJ : i * CJ + CJ] = hi
        s_lo[i * CJ : i * CJ + CJ] = lo
    for y in range(2):
        hi, lo = split(wi[...] * wj_ends[y])
        s_hi[OWN + 16 * y : OWN + 16 * y + 16] = hi
        s_lo[OWN + 16 * y : OWN + 16 * y + 16] = lo
    for x in range(2):
        hi, lo = split(reach[x] * wj)
        x_hi[x * CJ : x * CJ + CJ] = hi
        x_lo[x * CJ : x * CJ + CJ] = lo
        for y in range(2):
            edges[2 * x + y : 2 * x + y + 1] = reach[x] * wj_ends[y]

    lane16 = iota((16, 128), 1)
    arrive(g_y)
    for f in range(NF):
        hi, lo = split(yb[f].T)
        a_hi[f * CK : f * CK + CK, OWN:COLS] = hi
        a_lo[f * CK : f * CK + CK, OWN:COLS] = lo
    arrive(g_z)
    hi, lo = split(z_in[...])
    a_hi[NF * CK : ROWS, 0:OWN] = hi
    a_lo[NF * CK : ROWS, 0:OWN] = lo
    arrive(g_yz)
    corner = jnp.zeros((16, 128), F32)
    for y in range(2):
        for i in range(CI):
            at = i * CJ + (CJ - 1 if y == 0 else 0)
            first = at // 128 * 128
            block = jnp.concatenate([yz_in[y, z, :, first : first + 128] for z in range(2)], axis=0)
            to = 16 * y + i
            moved = pltpu.roll(block, (to - at) % 128, 1)
            corner = jnp.where(lane16 == to, moved, corner)
    hi, lo = split(corner)
    a_hi[NF * CK : ROWS, OWN:COLS] = hi
    a_lo[NF * CK : ROWS, OWN:COLS] = lo

    def z_block(value):
        hi, lo = split(value)
        hi, lo = hi.astype(F32), lo.astype(F32)
        return (hi + pltpu.roll(hi, 16, 1) + pltpu.roll(lo, 32, 1)).astype(BF16)

    def put_plane(x, at, rows, value, ends_value):
        hi, lo = split(value)
        e_lhs[x, at : at + rows, 0:128] = hi
        e_lhs[x, at : at + rows, 128:256] = hi
        e_lhs[x, at : at + rows, 256:384] = lo
        e_lhs[x, at : at + rows, 384:512] = z_block(ends_value)

    lane64 = iota((CJ, 128), 1)
    lane8 = iota((8, 128), 1)
    for x in range(2):
        i = 0 if x == 0 else CI - 1
        first = i * CJ // 128 * 128
        columns = jnp.concatenate(
            [z_in[:, first : first + 128], jnp.zeros((112, 128), F32)], axis=0
        ).T
        columns = columns[0:CJ] if x == 0 else columns[CJ:128]
        for f in range(NF):
            moved = columns if f == 0 else pltpu.roll(columns, 128 - f, 1)
            moved = jnp.where((lane64 == 0) | (lane64 == 8), moved, 0.0)
            put_plane(x, f * CJ, CJ, fields[f, i], moved)
        values, moves = [], []
        for y in range(2):
            values += [yb[f, 16 * y + i : 16 * y + i + 1, :] for f in range(NF)]
            values.append(jnp.zeros((2, CK), F32))
            at = i * CJ + (CJ - 1 if y == 0 else 0)
            first = at // 128 * 128
            total = jnp.zeros((8, 128), F32)
            for z in range(2):
                block = pltpu.roll(yz_in[y, z, :, first : first + 128], (8 * z - at) % 128, 1)
                total = jnp.where(lane8 == 8 * z, block, total)
            moves.append(total)
        put_plane(
            x, NF * CJ, 16, jnp.concatenate(values, axis=0), jnp.concatenate(moves, axis=0)
        )

    chunks = [slice(c * 256, c * 256 + 256) for c in range(n // 256)]

    def gather(chunk):
        left = jnp.concatenate([a_hi[...], a_hi[...], a_lo[...]], axis=1)
        right = jnp.concatenate([s_hi[:, chunk], s_lo[:, chunk], s_hi[:, chunk]], axis=0)
        value = jnp.dot(left, right, preferred_element_type=F32)
        for f in range(NF):
            total = jnp.sum(value[f * CK : f * CK + CK] * lines[:, chunk], axis=0, keepdims=True)
            for z in range(2):
                row = NF * CK + 8 * z + f
                total = total + value[row : row + 1] * line_ends[z : z + 1, chunk]
            gathered[f : f + 1, chunk] = total

    for chunk in chunks[:2]:
        gather(chunk)

    for h, part in enumerate(parts):
        arrive(g_pos[h])
        for x in range(2):
            near_x, at_j, cell_j, at_k, cell_k = [unpack(theirs.at[x, h], q) for q in range(5)]
            ws[x, :, part] = near_x * tent(at_j - (ramp(CJ, width) - cell_j))
            ws_ends[x, 0:1, part] = near_x * tent(at_j - (-1.0 - cell_j))
            ws_ends[x, 1:2, part] = near_x * tent(at_j - (float(CJ) - cell_j))
            k_weights(x, part, at_k, cell_k)
        for x in range(2):
            for start in range(part.start, part.stop, 256):
                chunk = slice(start, start + 256)
                top, low = l_hi[x, 0:CK, chunk], l_lo[x, 0:CK, chunk]
                top_z, low_z = l_hi[x, CK:, chunk], l_lo[x, CK:, chunk]
                right = jnp.concatenate(
                    [top, low, top, top_z, low_z, top_z, jnp.zeros((80, 256), BF16)], axis=0
                )
                value = jnp.dot(e_lhs[x], right, preferred_element_type=F32)
                last = NF * CJ
                total = value[last : last + 8] * ws_ends[x, 0:1, chunk]
                total = total + value[last + 8 : last + 16] * ws_ends[x, 1:2, chunk]
                weight = ws[x, :, chunk]
                for f in range(NF):
                    row = jnp.sum(value[f * CJ : f * CJ + CJ] * weight, axis=0, keepdims=True)
                    row = row + total[f : f + 1]
                    pack(part_out.at[x, h], f, row, (start - part.start) // 128)
        send(g_part[h])

    for chunk in chunks[2:]:
        gather(chunk)

    for group in (*g_pos, g_y, g_z, g_yz):
        sent(group)

    terms_out[5:8] = jnp.zeros((3, n), F32)
    for h, part in enumerate(parts):
        motion = mot[:, part]
        warmth = heat[part].reshape(1, width)
        q = diam[part].reshape(1, width)
        live = (iota((1, width), 1) + h * width) // TILE < tally[0]
        arrive(g_part[h])
        got = [
            gathered[f : f + 1, part]
            + unpack(part_in.at[0, h], f)
            + unpack(part_in.at[1, h], f)
            for f in range(NF)
        ]
        gas = jnp.concatenate(got[0:3], axis=0)
        gas_heat, moisture, rho = got[3:6]
        drag = step_time / (0.5 * q)
        new_motion = (motion + drag * gas) / (1.0 + drag)
        mass = q * jnp.sqrt(q)
        vapour = jnp.exp(4.0 * (warmth - 1.0))
        decay = step_time * evap_rate * rho * (vapour - moisture)
        new_q = q - decay
        new_mass = new_q * jnp.sqrt(new_q)
        conduction = step_time * heat_rate * rho / q
        new_heat = (warmth + conduction * gas_heat) / (1.0 + conduction) - (
            boiling_energy_drain * decay / q
        )
        state[0:3, part] = jnp.where(live, new_motion, motion)
        state[3:4, part] = jnp.where(live, new_heat, warmth)
        state[4:5, part] = jnp.where(live, new_q, q)
        pushes = jnp.where(live, mass * (motion - new_motion), 0.0)
        terms = [pushes[c : c + 1] for c in range(3)]
        terms.append(jnp.where(live, mass * (warmth - new_heat), 0.0))
        terms.append(jnp.where(live, mass - new_mass, 0.0))
        for c in range(NS):
            terms_out[c : c + 1, part] = terms[c]
            pack(terms_pack.at[h], c, terms[c])
        send(d_terms[h])

    def cross(left, right):
        return lax.dot_general(
            left, right, (((1,), (1,)), ((), ())), preferred_element_type=F32
        )

    tail = jnp.concatenate(
        [terms_out[...] * line_ends[0:1], terms_out[...] * line_ends[1:2]], axis=0
    )
    hi, lo = split(tail)
    tail = jnp.concatenate([hi, hi, lo], axis=1)
    tail = jnp.concatenate([tail, jnp.zeros((112, 3 * n), BF16)], axis=0)
    left = jnp.concatenate([x_hi[...], x_lo[...], x_hi[...]], axis=1)
    dxz_out[...] = cross(left, tail).T[0:16]
    hi, lo = split(
        jnp.concatenate([terms_out[...] * edges[line : line + 1] for line in range(4)], axis=0)
    )
    left = jnp.concatenate([hi, hi, lo], axis=1)
    right = jnp.concatenate([l_hi[2], l_lo[2], l_hi[2]], axis=1)
    value = cross(left, right)
    dxy_out[:, 0:128] = value[:, 0:CK]
    dxy_out[:, 128:144] = value[:, CK : CK + 16]
    send(d_xyz)
    send(d_xy)
    send(d_xz)

    lines_used = slice(0, OWN + 32)
    for w in (2, 0, 1):
        left = jnp.concatenate(
            [s_hi[lines_used], s_lo[lines_used], s_hi[lines_used]], axis=1
        )
        right = []
        for c in (2 * w, 2 * w + 1):
            if c < NS:
                hi, lo = split(terms_out[c : c + 1] * lines[...])
                right.append(jnp.concatenate([hi, hi, lo], axis=1))
            else:
                right.append(tail)
        right = jnp.concatenate(right, axis=0)
        if w < 2:
            value = cross(left, right)
        else:
            value = jnp.concatenate(
                [cross(left[0:272], right), cross(left[272:], right)], axis=0
            )
        for h in range(2):
            c = 2 * w + h
            half = value[:, h * 128 : h * 128 + 128]
            if c < NS:
                out[c] = half[0:OWN].reshape(CI, CJ, CK)
                dy[:, c * CK : c * CK + CK] = half[OWN : OWN + 32]
            else:
                for b in range(OWN // 128):
                    dz_out[:, b * 128 : b * 128 + 128] = half[b * 128 : b * 128 + 128].T[0:16]
                rest = jnp.concatenate([half[OWN : OWN + 32], jnp.zeros((96, 128), F32)], axis=0)
                dz_out[:, OWN:COLS] = rest.T[0:16]

    for group in g_part:
        sent(group)
    send(d_z)
    send(d_yz)
    send(d_y)

    for h, part in enumerate(parts):
        arrive(d_terms[h])
        for x in range(2):
            i = 0 if x == 0 else CI - 1
            weight = ws[x, :, part]
            left = []
            for c in range(NS):
                hi, lo = split(unpack(terms_in.at[x, h], c) * weight)
                left.append(jnp.concatenate([hi, hi, lo], axis=1))
            left = jnp.concatenate(left, axis=0)
            hi, lo = l_hi[x, 0:CK, part], l_lo[x, 0:CK, part]
            right = jnp.concatenate([hi, lo, hi], axis=1)
            value = cross(left, right)
            for c in range(NS):
                out[c, i] = out[c, i] + value[c * CJ : c * CJ + CJ]

    for group in (*d_terms, d_xz, d_xy, d_xyz):
        sent(group)
    arrive(d_z)
    arrive(d_y)
    arrive(d_yz)
    arrive(d_xz)
    arrive(d_xy)
    arrive(d_xyz)
    for b in range(OWN // 128):
        block = dz_in[:, b * 128 : b * 128 + 128]
        for i in (2 * b, 2 * b + 1):
            for y in range(2):
                to = i * CJ % 128 + (0 if y == 0 else CJ - 1)
                at = (16 if y == 0 else 0) + i
                moved = jnp.concatenate([dyz_in[y, 0], dyz_in[y, 1]], axis=0)
                moved = pltpu.roll(moved, (to - at) % 128, 1)
                block = block + jnp.where(lane16 == to, moved, 0.0)
        if b in (0, OWN // 128 - 1):
            x = 0 if b == 0 else 1
            moved = jnp.concatenate([dxz_in[x, 0], dxz_in[x, 1]], axis=0)
            half = lane16 < CJ if x == 0 else lane16 >= CJ
            block = block + jnp.where(half, pltpu.roll(moved, CJ, 1), 0.0)
            for y in range(2):
                to = CJ * x + (0 if y == 0 else CJ - 1)
                moved = jnp.concatenate(
                    [
                        pltpu.roll(dxyz_in[x, y, z], (to - 8 * (1 - z)) % 128, 1)
                        for z in range(2)
                    ],
                    axis=0,
                )
                block = block + jnp.where(lane16 == to, moved, 0.0)
        for c in range(NS):
            zt[b, 2 * c : 2 * c + 1] = block[8 + c : 9 + c]
            zt[b, 2 * c + 1 : 2 * c + 2] = block[c : c + 1]
    rows[...] = dy_in[...]
    for x in range(2):
        i = 0 if x == 0 else CI - 1
        for y in range(2):
            for c in range(NS):
                at = slice(c * CK, c * CK + CK)
                rows[y, i : i + 1, at] = rows[y, i : i + 1, at] + dxy_in[x, y, c : c + 1, :]

    for group in (d_z, d_y, d_yz):
        sent(group)


def deliver(part, state, zt, rows, out, state_out, whole, sem):
    state_copy = pltpu.make_async_copy(state, state_out, sem.at[NS])
    state_copy.start()
    lane = iota((128, 128), 1)
    rim = (lane == 0) | (lane == CK - 1)
    blocks = range(OWN // 128)
    columns = [
        jnp.concatenate([zt[b], jnp.zeros((112, 128), F32)], axis=0).T for b in blocks
    ]
    copies = []
    for c in range(NS):
        for b in blocks:
            add = jnp.where(rim, pltpu.roll(columns[b], 127 - 2 * c, 1), 0.0)
            whole[c, 2 * b : 2 * b + 2] = part[c, 2 * b : 2 * b + 2] + add.reshape(2, CJ, CK)
        for y in range(2):
            j = 0 if y == 0 else CJ - 1
            for i in range(CI):
                whole[c, i, j : j + 1, :] = (
                    whole[c, i, j : j + 1, :] + rows[y, i : i + 1, c * CK : c * CK + CK]
                )
        copies.append(pltpu.make_async_copy(whole.at[c], out.at[c], sem.at[c]))
        copies[-1].start()
    for copy in copies + [state_copy]:
        copy.wait()


def local(sizes, vel, scal, pos, mot, heat, diam, li, lj, lk, tally):
    n = heat.shape[0]
    vmem = pl.BlockSpec(memory_space=pltpu.VMEM)
    hbm = pl.BlockSpec(memory_space=pltpu.HBM)
    planes = NF * CJ + 16
    parts = pl.pallas_call(
        functools.partial(kernel, sizes),
        out_shape=(
            jax.ShapeDtypeStruct((NS, CI, CJ, CK), F32),
            jax.ShapeDtypeStruct((NS, n), F32),
            jax.ShapeDtypeStruct((OWN // 128, 16, 128), F32),
            jax.ShapeDtypeStruct((2, 8, NS * CK), F32),
        ),
        in_specs=[hbm] * 9 + [pl.BlockSpec(memory_space=pl.ANY)],
        out_specs=(vmem,) * 4,
        scratch_shapes=[
            pltpu.VMEM((NF, CI, CJ, CK), F32),
            pltpu.VMEM((3, n), F32),
            pltpu.VMEM((3, n), F32),
            pltpu.VMEM((n,), F32),
            pltpu.VMEM((n,), F32),
            pltpu.VMEM((n,), jnp.int32),
            pltpu.VMEM((n,), jnp.int32),
            pltpu.VMEM((n,), jnp.int32),
            pltpu.SMEM((1,), jnp.int32),
            pltpu.VMEM((2, PARTS, 5 * n // PARTS // 128, 128), F32),
            pltpu.VMEM((2, PARTS, 5 * n // PARTS // 128, 128), F32),
            pltpu.VMEM((ROWS, COLS), BF16),
            pltpu.VMEM((ROWS, COLS), BF16),
            pltpu.VMEM((COLS, n), BF16),
            pltpu.VMEM((COLS, n), BF16),
            pltpu.VMEM((2, planes, 512), BF16),
            pltpu.VMEM((3, CK + 16, n), BF16),
            pltpu.VMEM((3, CK + 16, n), BF16),
            pltpu.VMEM((2 * CJ, n), BF16),
            pltpu.VMEM((2 * CJ, n), BF16),
            pltpu.VMEM((8, n), F32),
            pltpu.VMEM((2, CJ, n), F32),
            pltpu.VMEM((2, 8, n), F32),
            pltpu.VMEM((16, n), F32),
            pltpu.VMEM((CK, n), F32),
            pltpu.VMEM((8, n), F32),
            pltpu.VMEM((8, n), F32),
            pltpu.VMEM((2, PARTS, NF * n // PARTS // 128, 128), F32),
            pltpu.VMEM((2, PARTS, NF * n // PARTS // 128, 128), F32),
            pltpu.VMEM((8, n), F32),
            pltpu.VMEM((PARTS, NS * n // PARTS // 128, 128), F32),
            pltpu.VMEM((2, PARTS, NS * n // PARTS // 128, 128), F32),
            pltpu.VMEM((NF, 128, CK), F32),
            pltpu.VMEM((2, NF, 8, CK), F32),
            pltpu.VMEM((2, 8, OWN), F32),
            pltpu.VMEM((16, OWN), F32),
            pltpu.VMEM((2, 2, 8, OWN), F32),
            pltpu.VMEM((32, NS * CK), F32),
            pltpu.VMEM((2, 8, NS * CK), F32),
            pltpu.VMEM((16, COLS), F32),
            pltpu.VMEM((16, OWN), F32),
            pltpu.VMEM((2, 2, 8, 128), F32),
            pltpu.VMEM((16, 128), F32),
            pltpu.VMEM((2, 2, 8, 128), F32),
            pltpu.VMEM((32, 256), F32),
            pltpu.VMEM((2, 2, 8, 128), F32),
            pltpu.VMEM((2, 2, 2, 8, 128), F32),
            pltpu.SemaphoreType.DMA((2 * PARTS + 20 + max(4, 2 * PARTS),)),
            pltpu.SemaphoreType.DMA((32 + 4 * PARTS,)),
        ],
        compiler_params=pltpu.CompilerParams(
            collective_id=0, has_side_effects=True, vmem_limit_bytes=32 * 1024 * 1024
        ),
    )(*(pltpu.with_memory_space_constraint(x, pltpu.HBM) for x in (vel, scal, pos, mot, heat, diam, li, lj, lk)), tally)
    return pl.pallas_call(
        deliver,
        out_shape=tuple(jax.ShapeDtypeStruct(part.shape, F32) for part in parts[:2]),
        in_specs=[vmem] * 4,
        out_specs=(hbm, hbm),
        scratch_shapes=[
            pltpu.VMEM((NS, CI, CJ, CK), F32),
            pltpu.SemaphoreType.DMA((NS + 1,)),
        ],
        compiler_params=pltpu.CompilerParams(vmem_limit_bytes=4 * 1024 * 1024),
    )(*parts)


def solution(mesh):
    sizes = {axis: mesh.shape[axis] for axis in ("gx", "gy", "gz")}
    flat = P(("gx", "gy", "gz"))
    wide = P(None, ("gx", "gy", "gz"))
    grid = P(None, "gx", "gy", "gz")
    return jax.shard_map(
        functools.partial(local, sizes),
        mesh=mesh,
        in_specs=(grid, grid, wide, wide) + (flat,) * 6,
        out_specs=(grid, wide),
        check_vma=False,
    )
```

```python
import functools
import itertools

import jax
import jax.numpy as jnp
from jax import lax
from jax.experimental import pallas as pl
from jax.experimental.pallas import tpu as pltpu
from jax.sharding import PartitionSpec as P

TILE = 128
NF = 6
NS = 5
CI, CJ, CK = 8, 64, 128
OWN = CI * CJ
COLS = OWN + 128
ROWS = NF * CK + 16
PARTS = 2
MESH = pl.DeviceIdType.MESH
F32 = jnp.float32
BF16 = jnp.bfloat16

step_time = 0.25
evap_rate = 1.0
heat_rate = 2.0
boiling_energy_drain = 0.3


def split(x):
    hi = x.astype(BF16)
    return hi, (x - hi.astype(F32)).astype(BF16)


def tent(offset):
    return jnp.maximum(0.0, 1.0 - jnp.abs(offset))


def iota(shape, dim):
    return lax.broadcasted_iota(jnp.int32, shape, dim)


def kernel(
    sizes,
    vel,
    scal,
    pos_hbm,
    mot_hbm,
    heat_hbm,
    diam_hbm,
    li_hbm,
    lj_hbm,
    lk_hbm,
    tally_hbm,
    out,
    state,
    zt,
    rows,
    fields,
    pos,
    mot,
    heat,
    diam,
    li,
    lj,
    lk,
    tally,
    mine,
    theirs,
    a_hi,
    a_lo,
    s_hi,
    s_lo,
    e_lhs,
    l_hi,
    l_lo,
    x_hi,
    x_lo,
    edges,
    ws,
    ws_ends,
    wi,
    lines,
    line_ends,
    gathered,
    part_out,
    part_in,
    terms_out,
    terms_pack,
    terms_in,
    yb,
    y_out,
    z_out,
    z_in,
    yz_in,
    dy,
    dy_in,
    dz_out,
    dz_in,
    dyz_in,
    dxz_out,
    dxz_in,
    dxy_out,
    dxy_in,
    dxyz_in,
    send_sem,
    recv_sem,
):
    n = pos.shape[1]
    width = n // PARTS
    parts = [slice(h * width, h * width + width) for h in range(PARTS)]
    per_row = width // 128
    axes = tuple(sizes)
    me = {axis: lax.axis_index(axis) for axis in axes}
    ends = {axis: size - 1 for axis, size in sizes.items()}

    def there(steps):
        found = None
        for axis, step in steps:
            one = me[axis] < ends[axis] if step > 0 else me[axis] > 0
            found = one if found is None else jnp.logical_and(found, one)
        return found

    def peer(steps):
        return {axis: me[axis] + step for axis, step in steps}

    def back(steps):
        return tuple((axis, -step) for axis, step in steps)

    numbers = iter(range(64))

    def pack(ref, number, row, first=0):
        for b in range(row.shape[1] // 128):
            at = number * per_row + first + b
            ref[at : at + 1, :] = row[:, b * 128 : b * 128 + 128]

    def unpack(ref, number):
        first = number * per_row
        return jnp.concatenate([ref[first + b : first + b + 1, :] for b in range(per_row)], axis=1)

    def numbered(first, again):
        send_number = iter(range(first, 64))
        if again is not None:
            taken = [transfer[0][1] for transfer in again]
            return zip(send_number, taken)
        return zip(send_number, numbers)

    def both(first, axis, up, land0, down, land1, again=None):
        pair = numbered(first, again)
        return (
            (next(pair), ((axis, 1),), up, land0),
            (next(pair), ((axis, -1),), down, land1),
        )

    def diagonal(first, axes, source, land):
        found = []
        pair = numbered(first, None)
        for steps in itertools.product((1, -1), repeat=len(axes)):
            sides = tuple((1 - step) // 2 for step in steps)
            from_sides = tuple(1 - side for side in sides)
            steps = tuple(zip(axes, steps))
            found.append((next(pair), steps, source(*from_sides), land.at[sides]))
        return tuple(found)

    def copy(transfer, steps):
        number, _, source, land = transfer
        return pltpu.make_async_remote_copy(
            src_ref=source,
            dst_ref=land,
            send_sem=send_sem.at[number[0]],
            recv_sem=recv_sem.at[number[1]],
            device_id=peer(steps),
            device_id_type=MESH,
        )

    def send(group):
        for transfer in group:
            pl.when(there(transfer[1]))(lambda t=transfer: copy(t, t[1]).start())

    def arrive(group):
        for transfer in group:
            steps = back(transfer[1])
            pl.when(there(steps))(lambda t=transfer, s=steps: copy(t, s).wait_recv())

    def sent(group):
        for transfer in group:
            pl.when(there(transfer[1]))(lambda t=transfer: copy(t, t[1]).wait_send())

    def blank(group):
        for _, steps, _, land in group:

            @pl.when(jnp.logical_not(there(back(steps))))
            def _():
                land[...] = jnp.zeros(land.shape, F32)

    g_pos = [
        both(2 * h, "gx", mine.at[1, h], theirs.at[0, h], mine.at[0, h], theirs.at[1, h])
        for h in range(PARTS)
    ]
    first = 2 * PARTS
    g_y = both(first, "gy", y_out.at[1], yb.at[:, 0:8], y_out.at[0], yb.at[:, 16:24])
    g_z = both(first + 2, "gz", z_out.at[1], z_in.at[0:8], z_out.at[0], z_in.at[8:16])
    g_yz = diagonal(first + 4, ("gy", "gz"), lambda y, z: z_out.at[z], yz_in)
    g_part = [
        both(
            first + 20 + 2 * h,
            "gx",
            part_out.at[1, h],
            part_in.at[0, h],
            part_out.at[0, h],
            part_in.at[1, h],
        )
        for h in range(PARTS)
    ]
    d_terms = [
        both(
            2 * h,
            "gx",
            terms_pack.at[h],
            terms_in.at[0, h],
            terms_pack.at[h],
            terms_in.at[1, h],
            again=g_pos[h],
        )
        for h in range(PARTS)
    ]
    d_z = both(
        first + 16,
        "gz",
        dz_out.at[8:16, 0:OWN],
        dz_in.at[0:8],
        dz_out.at[0:8, 0:OWN],
        dz_in.at[8:16],
    )
    d_y = both(first + 18, "gy", dy.at[16:24], dy_in.at[0], dy.at[0:8], dy_in.at[1])
    d_yz = diagonal(
        first + 20, ("gy", "gz"), lambda y, z: dz_out.at[8 * z : 8 * z + 8, OWN:COLS], dyz_in
    )
    d_xz = diagonal(first, ("gx", "gz"), lambda x, z: dxz_out.at[8 * z : 8 * z + 8], dxz_in)

    def edge(x, y):
        first = 16 * x + 8 * y
        return slice(first, first + 8)

    d_xy = diagonal(first + 4, ("gx", "gy"), lambda x, y: dxy_out.at[edge(x, y), 0:128], dxy_in)
    d_xyz = diagonal(
        first + 8, ("gx", "gy", "gz"), lambda x, y, z: dxy_out.at[edge(x, y), 128:256], dxyz_in
    )
    groups = (g_y, g_z, g_yz, d_xz, d_xy, d_xyz, d_z, d_y, d_yz)
    groups += tuple(g_pos) + tuple(g_part) + tuple(d_terms)

    barrier = pltpu.get_barrier_semaphore()
    for _, steps, _, _ in g_pos[0] + g_y + g_z + g_yz:
        pl.when(there(steps))(
            lambda s=steps: pl.semaphore_signal(
                barrier, inc=1, device_id=peer(s), device_id_type=MESH
            )
        )

    loads = []
    for number, (source, land) in enumerate(
        (
            (pos_hbm, pos),
            (li_hbm, li),
            (lj_hbm, lj),
            (lk_hbm, lk),
            (vel, fields.at[0:3]),
            (scal, fields.at[3:6]),
            (mot_hbm, mot),
            (heat_hbm, heat),
            (diam_hbm, diam),
            (tally_hbm, tally),
        )
    ):
        loads.append(pltpu.make_async_copy(source, land, send_sem.at[first + 8 + number]))
        loads[-1].start()

    for group in groups:
        blank(group)
    yb[:, 8:16] = jnp.zeros((NF, 8, CK), F32)
    yb[:, 24:128] = jnp.zeros((NF, 104, CK), F32)
    z_out[...] = jnp.zeros(z_out.shape, F32)
    dxy_out[...] = jnp.zeros(dxy_out.shape, F32)
    zt[:, 10:16] = jnp.zeros((OWN // 128, 6, 128), F32)
    s_hi[OWN + 32 : COLS] = jnp.zeros((96, n), BF16)
    s_lo[OWN + 32 : COLS] = jnp.zeros((96, n), BF16)

    for load in loads[0:4]:
        load.wait()
    at = [pos[axis : axis + 1] for axis in range(3)]
    cell = [ref[...].reshape(1, n).astype(F32) for ref in (li, lj, lk)]
    reach = [tent(at[0] - (place - cell[0])) for place in (-1.0, float(CI))]
    for x in range(2):
        for number, row in enumerate((reach[x], at[1], cell[1], at[2], cell[2])):
            for h, part in enumerate(parts):
                pack(mine.at[x, h], number, row[:, part])

    for load in loads[4:]:
        load.wait()
    for f in range(NF):
        for i in range(CI):
            y_out[0, f, i : i + 1, :] = fields[f, i, 0:1, :]
            y_out[1, f, i : i + 1, :] = fields[f, i, CJ - 1 : CJ, :]
    for f in range(NF):
        for b in range(OWN // 128):
            block = fields[f, 2 * b : 2 * b + 2].reshape(128, CK).T
            z_out[0, f : f + 1, b * 128 : b * 128 + 128] = block[0:1]
            z_out[1, f : f + 1, b * 128 : b * 128 + 128] = block[CK - 1 : CK]
            hi, lo = split(block)
            a_hi[f * CK : f * CK + CK, b * 128 : b * 128 + 128] = hi
            a_lo[f * CK : f * CK + CK, b * 128 : b * 128 + 128] = lo
    near = {axis: jnp.minimum(me[axis], 1) + jnp.minimum(ends[axis] - me[axis], 1) for axis in axes}
    pl.semaphore_wait(barrier, near["gx"] + near["gy"] + near["gz"] + near["gy"] * near["gz"])
    for h in range(PARTS):
        send(g_pos[h])
    send(g_y)
    send(g_z)
    send(g_yz)

    def ramp(rows, columns=n):
        return iota((rows, columns), 0).astype(F32)

    row16 = iota((16, n), 0)

    def k_weights(x, part, offset, cell):
        rows = iota((16, offset.shape[1]), 0)
        hi, lo = split(tent(offset - (ramp(CK, offset.shape[1]) - cell)))
        l_hi[x, 0:CK, part] = hi
        l_lo[x, 0:CK, part] = lo
        low, high = tent(offset - (-1.0 - cell)), tent(offset - (float(CK) - cell))
        hi, lo = split(jnp.where(rows == 0, low, jnp.where(rows == 8, high, 0.0)))
        l_hi[x, CK:, part] = hi
        l_lo[x, CK:, part] = lo
        return low, high

    wi[...] = jnp.where(row16 < CI, tent(at[0] - (ramp(16) - cell[0])), 0.0)
    wj = tent(at[1] - (ramp(CJ) - cell[1]))
    wj_ends = (tent(at[1] - (-1.0 - cell[1])), tent(at[1] - (float(CJ) - cell[1])))
    lines[...] = tent(at[2] - (ramp(CK) - cell[2]))
    line_ends[0:1], line_ends[1:2] = k_weights(2, slice(0, n), at[2], cell[2])
    for i in range(CI):
        hi, lo = split(wi[i : i + 1] * wj)
        s_hi[i * CJ : i * CJ + CJ] = hi
        s_lo[i * CJ : i * CJ + CJ] = lo
    for y in range(2):
        hi, lo = split(wi[...] * wj_ends[y])
        s_hi[OWN + 16 * y : OWN + 16 * y + 16] = hi
        s_lo[OWN + 16 * y : OWN + 16 * y + 16] = lo
    for x in range(2):
        hi, lo = split(reach[x] * wj)
        x_hi[x * CJ : x * CJ + CJ] = hi
        x_lo[x * CJ : x * CJ + CJ] = lo
        for y in range(2):
            edges[2 * x + y : 2 * x + y + 1] = reach[x] * wj_ends[y]

    lane16 = iota((16, 128), 1)
    arrive(g_y)
    for f in range(NF):
        hi, lo = split(yb[f].T)
        a_hi[f * CK : f * CK + CK, OWN:COLS] = hi
        a_lo[f * CK : f * CK + CK, OWN:COLS] = lo
    arrive(g_z)
    hi, lo = split(z_in[...])
    a_hi[NF * CK : ROWS, 0:OWN] = hi
    a_lo[NF * CK : ROWS, 0:OWN] = lo
    arrive(g_yz)
    corner = jnp.zeros((16, 128), F32)
    for y in range(2):
        for i in range(CI):
            at = i * CJ + (CJ - 1 if y == 0 else 0)
            first = at // 128 * 128
            block = jnp.concatenate([yz_in[y, z, :, first : first + 128] for z in range(2)], axis=0)
            to = 16 * y + i
            moved = pltpu.roll(block, (to - at) % 128, 1)
            corner = jnp.where(lane16 == to, moved, corner)
    hi, lo = split(corner)
    a_hi[NF * CK : ROWS, OWN:COLS] = hi
    a_lo[NF * CK : ROWS, OWN:COLS] = lo

    def z_block(value):
        hi, lo = split(value)
        hi, lo = hi.astype(F32), lo.astype(F32)
        return (hi + pltpu.roll(hi, 16, 1) + pltpu.roll(lo, 32, 1)).astype(BF16)

    def put_plane(x, at, rows, value, ends_value):
        hi, lo = split(value)
        e_lhs[x, at : at + rows, 0:128] = hi
        e_lhs[x, at : at + rows, 128:256] = hi
        e_lhs[x, at : at + rows, 256:384] = lo
        e_lhs[x, at : at + rows, 384:512] = z_block(ends_value)

    lane64 = iota((CJ, 128), 1)
    lane8 = iota((8, 128), 1)
    for x in range(2):
        i = 0 if x == 0 else CI - 1
        first = i * CJ // 128 * 128
        columns = jnp.concatenate(
            [z_in[:, first : first + 128], jnp.zeros((112, 128), F32)], axis=0
        ).T
        columns = columns[0:CJ] if x == 0 else columns[CJ:128]
        for f in range(NF):
            moved = columns if f == 0 else pltpu.roll(columns, 128 - f, 1)
            moved = jnp.where((lane64 == 0) | (lane64 == 8), moved, 0.0)
            put_plane(x, f * CJ, CJ, fields[f, i], moved)
        values, moves = [], []
        for y in range(2):
            values += [yb[f, 16 * y + i : 16 * y + i + 1, :] for f in range(NF)]
            values.append(jnp.zeros((2, CK), F32))
            at = i * CJ + (CJ - 1 if y == 0 else 0)
            first = at // 128 * 128
            total = jnp.zeros((8, 128), F32)
            for z in range(2):
                block = pltpu.roll(yz_in[y, z, :, first : first + 128], (8 * z - at) % 128, 1)
                total = jnp.where(lane8 == 8 * z, block, total)
            moves.append(total)
        put_plane(
            x, NF * CJ, 16, jnp.concatenate(values, axis=0), jnp.concatenate(moves, axis=0)
        )

    chunks = [slice(c * 256, c * 256 + 256) for c in range(n // 256)]

    def gather(chunk):
        left = jnp.concatenate([a_hi[...], a_hi[...], a_lo[...]], axis=1)
        right = jnp.concatenate([s_hi[:, chunk], s_lo[:, chunk], s_hi[:, chunk]], axis=0)
        value = jnp.dot(left, right, preferred_element_type=F32)
        for f in range(NF):
            total = jnp.sum(value[f * CK : f * CK + CK] * lines[:, chunk], axis=0, keepdims=True)
            for z in range(2):
                row = NF * CK + 8 * z + f
                total = total + value[row : row + 1] * line_ends[z : z + 1, chunk]
            gathered[f : f + 1, chunk] = total

    for h, part in enumerate(parts):
        arrive(g_pos[h])
        for x in range(2):
            near_x, at_j, cell_j, at_k, cell_k = [unpack(theirs.at[x, h], q) for q in range(5)]
            ws[x, :, part] = near_x * tent(at_j - (ramp(CJ, width) - cell_j))
            ws_ends[x, 0:1, part] = near_x * tent(at_j - (-1.0 - cell_j))
            ws_ends[x, 1:2, part] = near_x * tent(at_j - (float(CJ) - cell_j))
            k_weights(x, part, at_k, cell_k)
        for x in range(2):
            for start in range(part.start, part.stop, 256):
                chunk = slice(start, start + 256)
                top, low = l_hi[x, 0:CK, chunk], l_lo[x, 0:CK, chunk]
                top_z, low_z = l_hi[x, CK:, chunk], l_lo[x, CK:, chunk]
                right = jnp.concatenate(
                    [top, low, top, top_z, low_z, top_z, jnp.zeros((80, 256), BF16)], axis=0
                )
                value = jnp.dot(e_lhs[x], right, preferred_element_type=F32)
                last = NF * CJ
                total = value[last : last + 8] * ws_ends[x, 0:1, chunk]
                total = total + value[last + 8 : last + 16] * ws_ends[x, 1:2, chunk]
                weight = ws[x, :, chunk]
                for f in range(NF):
                    row = jnp.sum(value[f * CJ : f * CJ + CJ] * weight, axis=0, keepdims=True)
                    row = row + total[f : f + 1]
                    pack(part_out.at[x, h], f, row, (start - part.start) // 128)
        send(g_part[h])

    for chunk in chunks:
        gather(chunk)

    for group in (*g_pos, g_y, g_z, g_yz):
        sent(group)

    terms_out[5:8] = jnp.zeros((3, n), F32)
    for h, part in enumerate(parts):
        motion = mot[:, part]
        warmth = heat[part].reshape(1, width)
        q = diam[part].reshape(1, width)
        live = (iota((1, width), 1) + h * width) // TILE < tally[0]
        arrive(g_part[h])
        got = [
            gathered[f : f + 1, part]
            + unpack(part_in.at[0, h], f)
            + unpack(part_in.at[1, h], f)
            for f in range(NF)
        ]
        gas = jnp.concatenate(got[0:3], axis=0)
        gas_heat, moisture, rho = got[3:6]
        drag = step_time / (0.5 * q)
        new_motion = (motion + drag * gas) / (1.0 + drag)
        mass = q * jnp.sqrt(q)
        vapour = jnp.exp(4.0 * (warmth - 1.0))
        decay = step_time * evap_rate * rho * (vapour - moisture)
        new_q = q - decay
        new_mass = new_q * jnp.sqrt(new_q)
        conduction = step_time * heat_rate * rho / q
        new_heat = (warmth + conduction * gas_heat) / (1.0 + conduction) - (
            boiling_energy_drain * decay / q
        )
        state[0:3, part] = jnp.where(live, new_motion, motion)
        state[3:4, part] = jnp.where(live, new_heat, warmth)
        state[4:5, part] = jnp.where(live, new_q, q)
        pushes = jnp.where(live, mass * (motion - new_motion), 0.0)
        terms = [pushes[c : c + 1] for c in range(3)]
        terms.append(jnp.where(live, mass * (warmth - new_heat), 0.0))
        terms.append(jnp.where(live, mass - new_mass, 0.0))
        for c in range(NS):
            terms_out[c : c + 1, part] = terms[c]
            pack(terms_pack.at[h], c, terms[c])
        send(d_terms[h])

    def cross(left, right):
        return lax.dot_general(
            left, right, (((1,), (1,)), ((), ())), preferred_element_type=F32
        )

    tail = jnp.concatenate(
        [terms_out[...] * line_ends[0:1], terms_out[...] * line_ends[1:2]], axis=0
    )
    hi, lo = split(tail)
    tail = jnp.concatenate([hi, hi, lo], axis=1)
    tail = jnp.concatenate([tail, jnp.zeros((112, 3 * n), BF16)], axis=0)
    left = jnp.concatenate([x_hi[...], x_lo[...], x_hi[...]], axis=1)
    dxz_out[...] = cross(left, tail).T[0:16]
    hi, lo = split(
        jnp.concatenate([terms_out[...] * edges[line : line + 1] for line in range(4)], axis=0)
    )
    left = jnp.concatenate([hi, hi, lo], axis=1)
    right = jnp.concatenate([l_hi[2], l_lo[2], l_hi[2]], axis=1)
    value = cross(left, right)
    dxy_out[:, 0:128] = value[:, 0:CK]
    dxy_out[:, 128:144] = value[:, CK : CK + 16]
    send(d_xyz)
    send(d_xy)
    send(d_xz)

    lines_used = slice(0, OWN + 32)
    for w in (2, 0, 1):
        left = jnp.concatenate(
            [s_hi[lines_used], s_lo[lines_used], s_hi[lines_used]], axis=1
        )
        right = []
        for c in (2 * w, 2 * w + 1):
            if c < NS:
                hi, lo = split(terms_out[c : c + 1] * lines[...])
                right.append(jnp.concatenate([hi, hi, lo], axis=1))
            else:
                right.append(tail)
        right = jnp.concatenate(right, axis=0)
        if w < 2:
            value = cross(left, right)
        else:
            value = jnp.concatenate(
                [cross(left[0:272], right), cross(left[272:], right)], axis=0
            )
        for h in range(2):
            c = 2 * w + h
            half = value[:, h * 128 : h * 128 + 128]
            if c < NS:
                out[c] = half[0:OWN].reshape(CI, CJ, CK)
                dy[:, c * CK : c * CK + CK] = half[OWN : OWN + 32]
            else:
                for b in range(OWN // 128):
                    dz_out[:, b * 128 : b * 128 + 128] = half[b * 128 : b * 128 + 128].T[0:16]
                rest = jnp.concatenate([half[OWN : OWN + 32], jnp.zeros((96, 128), F32)], axis=0)
                dz_out[:, OWN:COLS] = rest.T[0:16]

    for group in g_part:
        sent(group)
    send(d_z)
    send(d_yz)
    send(d_y)

    for h, part in enumerate(parts):
        arrive(d_terms[h])
        for x in range(2):
            i = 0 if x == 0 else CI - 1
            weight = ws[x, :, part]
            left = []
            for c in range(NS):
                hi, lo = split(unpack(terms_in.at[x, h], c) * weight)
                left.append(jnp.concatenate([hi, hi, lo], axis=1))
            left = jnp.concatenate(left, axis=0)
            hi, lo = l_hi[x, 0:CK, part], l_lo[x, 0:CK, part]
            right = jnp.concatenate([hi, lo, hi], axis=1)
            value = cross(left, right)
            for c in range(NS):
                out[c, i] = out[c, i] + value[c * CJ : c * CJ + CJ]

    for group in (*d_terms, d_xz, d_xy, d_xyz):
        sent(group)
    arrive(d_z)
    arrive(d_y)
    arrive(d_yz)
    arrive(d_xz)
    arrive(d_xy)
    arrive(d_xyz)
    for b in range(OWN // 128):
        block = dz_in[:, b * 128 : b * 128 + 128]
        for i in (2 * b, 2 * b + 1):
            for y in range(2):
                to = i * CJ % 128 + (0 if y == 0 else CJ - 1)
                at = (16 if y == 0 else 0) + i
                moved = jnp.concatenate([dyz_in[y, 0], dyz_in[y, 1]], axis=0)
                moved = pltpu.roll(moved, (to - at) % 128, 1)
                block = block + jnp.where(lane16 == to, moved, 0.0)
        if b in (0, OWN // 128 - 1):
            x = 0 if b == 0 else 1
            moved = jnp.concatenate([dxz_in[x, 0], dxz_in[x, 1]], axis=0)
            half = lane16 < CJ if x == 0 else lane16 >= CJ
            block = block + jnp.where(half, pltpu.roll(moved, CJ, 1), 0.0)
            for y in range(2):
                to = CJ * x + (0 if y == 0 else CJ - 1)
                moved = jnp.concatenate(
                    [
                        pltpu.roll(dxyz_in[x, y, z], (to - 8 * (1 - z)) % 128, 1)
                        for z in range(2)
                    ],
                    axis=0,
                )
                block = block + jnp.where(lane16 == to, moved, 0.0)
        for c in range(NS):
            zt[b, 2 * c : 2 * c + 1] = block[8 + c : 9 + c]
            zt[b, 2 * c + 1 : 2 * c + 2] = block[c : c + 1]
    rows[...] = dy_in[...]
    for x in range(2):
        i = 0 if x == 0 else CI - 1
        for y in range(2):
            for c in range(NS):
                at = slice(c * CK, c * CK + CK)
                rows[y, i : i + 1, at] = rows[y, i : i + 1, at] + dxy_in[x, y, c : c + 1, :]

    for group in (d_z, d_y, d_yz):
        sent(group)


def deliver(part, state, zt, rows, out, state_out, whole, sem):
    state_copy = pltpu.make_async_copy(state, state_out, sem.at[NS])
    state_copy.start()
    lane = iota((128, 128), 1)
    rim = (lane == 0) | (lane == CK - 1)
    blocks = range(OWN // 128)
    columns = [
        jnp.concatenate([zt[b], jnp.zeros((112, 128), F32)], axis=0).T for b in blocks
    ]
    copies = []
    for c in range(NS):
        for b in blocks:
            add = jnp.where(rim, pltpu.roll(columns[b], 127 - 2 * c, 1), 0.0)
            whole[c, 2 * b : 2 * b + 2] = part[c, 2 * b : 2 * b + 2] + add.reshape(2, CJ, CK)
        for y in range(2):
            j = 0 if y == 0 else CJ - 1
            for i in range(CI):
                whole[c, i, j : j + 1, :] = (
                    whole[c, i, j : j + 1, :] + rows[y, i : i + 1, c * CK : c * CK + CK]
                )
        copies.append(pltpu.make_async_copy(whole.at[c], out.at[c], sem.at[c]))
        copies[-1].start()
    for copy in copies + [state_copy]:
        copy.wait()


def local(sizes, vel, scal, pos, mot, heat, diam, li, lj, lk, tally):
    n = heat.shape[0]
    vmem = pl.BlockSpec(memory_space=pltpu.VMEM)
    hbm = pl.BlockSpec(memory_space=pltpu.HBM)
    planes = NF * CJ + 16
    parts = pl.pallas_call(
        functools.partial(kernel, sizes),
        out_shape=(
            jax.ShapeDtypeStruct((NS, CI, CJ, CK), F32),
            jax.ShapeDtypeStruct((NS, n), F32),
            jax.ShapeDtypeStruct((OWN // 128, 16, 128), F32),
            jax.ShapeDtypeStruct((2, 8, NS * CK), F32),
        ),
        in_specs=[hbm] * 9 + [pl.BlockSpec(memory_space=pl.ANY)],
        out_specs=(vmem,) * 4,
        scratch_shapes=[
            pltpu.VMEM((NF, CI, CJ, CK), F32),
            pltpu.VMEM((3, n), F32),
            pltpu.VMEM((3, n), F32),
            pltpu.VMEM((n,), F32),
            pltpu.VMEM((n,), F32),
            pltpu.VMEM((n,), jnp.int32),
            pltpu.VMEM((n,), jnp.int32),
            pltpu.VMEM((n,), jnp.int32),
            pltpu.SMEM((1,), jnp.int32),
            pltpu.VMEM((2, PARTS, 5 * n // PARTS // 128, 128), F32),
            pltpu.VMEM((2, PARTS, 5 * n // PARTS // 128, 128), F32),
            pltpu.VMEM((ROWS, COLS), BF16),
            pltpu.VMEM((ROWS, COLS), BF16),
            pltpu.VMEM((COLS, n), BF16),
            pltpu.VMEM((COLS, n), BF16),
            pltpu.VMEM((2, planes, 512), BF16),
            pltpu.VMEM((3, CK + 16, n), BF16),
            pltpu.VMEM((3, CK + 16, n), BF16),
            pltpu.VMEM((2 * CJ, n), BF16),
            pltpu.VMEM((2 * CJ, n), BF16),
            pltpu.VMEM((8, n), F32),
            pltpu.VMEM((2, CJ, n), F32),
            pltpu.VMEM((2, 8, n), F32),
            pltpu.VMEM((16, n), F32),
            pltpu.VMEM((CK, n), F32),
            pltpu.VMEM((8, n), F32),
            pltpu.VMEM((8, n), F32),
            pltpu.VMEM((2, PARTS, NF * n // PARTS // 128, 128), F32),
            pltpu.VMEM((2, PARTS, NF * n // PARTS // 128, 128), F32),
            pltpu.VMEM((8, n), F32),
            pltpu.VMEM((PARTS, NS * n // PARTS // 128, 128), F32),
            pltpu.VMEM((2, PARTS, NS * n // PARTS // 128, 128), F32),
            pltpu.VMEM((NF, 128, CK), F32),
            pltpu.VMEM((2, NF, 8, CK), F32),
            pltpu.VMEM((2, 8, OWN), F32),
            pltpu.VMEM((16, OWN), F32),
            pltpu.VMEM((2, 2, 8, OWN), F32),
            pltpu.VMEM((32, NS * CK), F32),
            pltpu.VMEM((2, 8, NS * CK), F32),
            pltpu.VMEM((16, COLS), F32),
            pltpu.VMEM((16, OWN), F32),
            pltpu.VMEM((2, 2, 8, 128), F32),
            pltpu.VMEM((16, 128), F32),
            pltpu.VMEM((2, 2, 8, 128), F32),
            pltpu.VMEM((32, 256), F32),
            pltpu.VMEM((2, 2, 8, 128), F32),
            pltpu.VMEM((2, 2, 2, 8, 128), F32),
            pltpu.SemaphoreType.DMA((2 * PARTS + 20 + max(4, 2 * PARTS),)),
            pltpu.SemaphoreType.DMA((32 + 4 * PARTS,)),
        ],
        compiler_params=pltpu.CompilerParams(
            collective_id=0, has_side_effects=True, vmem_limit_bytes=32 * 1024 * 1024
        ),
    )(*(pltpu.with_memory_space_constraint(x, pltpu.HBM) for x in (vel, scal, pos, mot, heat, diam, li, lj, lk)), tally)
    return pl.pallas_call(
        deliver,
        out_shape=tuple(jax.ShapeDtypeStruct(part.shape, F32) for part in parts[:2]),
        in_specs=[vmem] * 4,
        out_specs=(hbm, hbm),
        scratch_shapes=[
            pltpu.VMEM((NS, CI, CJ, CK), F32),
            pltpu.SemaphoreType.DMA((NS + 1,)),
        ],
        compiler_params=pltpu.CompilerParams(vmem_limit_bytes=4 * 1024 * 1024),
    )(*parts)


def solution(mesh):
    sizes = {axis: mesh.shape[axis] for axis in ("gx", "gy", "gz")}
    flat = P(("gx", "gy", "gz"))
    wide = P(None, ("gx", "gy", "gz"))
    grid = P(None, "gx", "gy", "gz")
    return jax.shard_map(
        functools.partial(local, sizes),
        mesh=mesh,
        in_specs=(grid, grid, wide, wide) + (flat,) * 6,
        out_specs=(grid, wide),
        check_vma=False,
    )
```
